128 devices in a mesh: req: 32 (over x, z, core), seq: 4 (over y).
Axes of the slice: x: 4, y: 4, z: 4, core: 2. Of those that a mesh axis runs over, the one named last changes fastest.
Arguments:
- pool_states: float32 [416, 64, 64, 128], P('req', 'seq'), may hold values from -6 to 6
- inner_window: bfloat16 [416, 3, 4096], P('req', None, 'seq'), may hold values from -6 to 6
- state_window: bfloat16 [416, 3, 256], P('req', None, 'seq'), may hold values from -6 to 6
- move_plan: int32 [416, 2], P('req'), may hold values from 0 to 31, as said below
- active_mask: int32 [416], P('req'), may hold values 0 or 1
- inputs_inner: bfloat16 [32, 2048, 4096], P('req', 'seq'), may hold values from -6 to 6
- inputs_state: bfloat16 [32, 2048, 256], P('req', 'seq'), may hold values from -6 to 6
- gate_rows: bfloat16 [32, 2048, 4096], P('req', 'seq'), may hold values from -6 to 6
- step_raw: bfloat16 [32, 2048, 64], P('req', 'seq'), may hold values from -8 to 60
- lengths: int32 [32], P('req'), may hold values from 4 to 2048
- conv_weight: float32 [4, 4352], replicated, may hold values from -3 to 3
- conv_bias: float32 [4352], replicated, may hold values from -3 to 3
- step_bias: float32 [64], replicated, may hold values from -3.3 to -2.7
- decay_log: float32 [64], replicated, may hold values from -10 to 0
- skip_weight: float32 [64], replicated, may hold values from 0.5 to 1.5
- norm_weight: float32 [4096], replicated, may hold values from 0.25 to 1.75
Outputs:
- new_states: float32 [416, 64, 64, 128], P('req', 'seq')
- new_inner_window: bfloat16 [416, 3, 4096], P('req', None, 'seq')
- new_state_window: bfloat16 [416, 3, 256], P('req', None, 'seq')
- mixer_out: bfloat16 [32, 2048, 4096], P('req', 'seq')
The draws below stay inside these ranges and needn't reach their ends.
Inputs may be any that keep to these rules, and one draw needn't show every extreme that they name: `move_plan`: every pair of a destination index along req and a slot 0 .. 12 is named exactly once; the rows of one device name one destination at most 1 times, and some destination exactly 1 times.
All inputs are finite; a program needn't handle non-finite values. No bound on the sum of `active_mask` on one device may be relied on, other than what follows from the above.
Results may differ from the reference program's by a relative error of at most 0.0087.
Values may be sent and summed in bfloat16 or wider, within the bound.
A program may use at most 192 MiB of HBM per device.

```python
import jax
import jax.numpy as jnp
from jax import lax

HEAD_COUNT = 64
HEAD_DIM = 64
STATE_DIM = 128
KERNEL = 4
BLOCK_LEN = 256
SLOTS_DEV = 13
PREFILLS = 1
INNER_DIM = 4096
CHANNELS = 4352
CAPACITY = 1
PROMPT_SPAN = 2048
PROMPT_TOTAL = 32
POOL_SLOTS = 416


def draw_move_plan(key, part):
    peer_count = POOL_SLOTS // SLOTS_DEV
    sampler_seeds = jax.random.split(jax.random.fold_in(key, 11), 5)
    outer_order = jax.random.permutation(sampler_seeds[0], peer_count)
    inner_order = jax.random.permutation(sampler_seeds[1], peer_count)
    slot_order = jax.random.permutation(sampler_seeds[2], SLOTS_DEV)
    rotation = jax.random.randint(sampler_seeds[3], (), 0, peer_count)
    offsets = ((jnp.arange(SLOTS_DEV) // CAPACITY + rotation) % peer_count)[slot_order]
    devices = jnp.arange(peer_count)
    target_device = outer_order[(inner_order[devices][:, None] + offsets[None, :]) % peer_count]

    def slot_table(table_key):
        return jax.random.permutation(table_key, SLOTS_DEV)
    slot_tables = jax.vmap(slot_table)(jax.random.split(sampler_seeds[4], peer_count))
    target_slot = slot_tables[target_device, jnp.arange(SLOTS_DEV)[None, :]]
    return jnp.stack([target_device, target_slot], axis=-1).reshape(POOL_SLOTS, 2).astype(jnp.int32)


def draw_step_raw(key, part):
    sampler_seeds = jax.random.split(jax.random.fold_in(key, 23), 4)
    blocks = PROMPT_SPAN // BLOCK_LEN
    offset_steps = jax.random.uniform(sampler_seeds[0], (PROMPT_TOTAL, blocks, 1, HEAD_COUNT), minval=-0.8, maxval=0.8)
    offset_steps = jnp.broadcast_to(offset_steps, (PROMPT_TOTAL, blocks, BLOCK_LEN, HEAD_COUNT)).reshape(PROMPT_TOTAL, PROMPT_SPAN, HEAD_COUNT)
    jitter_addend = 0.7 * jax.random.normal(sampler_seeds[1], (PROMPT_TOTAL, PROMPT_SPAN, HEAD_COUNT))
    arrival_tallies = jax.random.uniform(sampler_seeds[2], (PROMPT_TOTAL, PROMPT_SPAN, 1)) < 3.0 / PROMPT_SPAN
    level_entries = jax.random.uniform(sampler_seeds[3], (PROMPT_TOTAL, PROMPT_SPAN, HEAD_COUNT), minval=34.0, maxval=46.0)
    payload_array = offset_steps + jitter_addend + jnp.where(arrival_tallies, level_entries, 0.0)
    return jnp.clip(payload_array, -8.0, 60.0).astype(jnp.float32).astype(jnp.bfloat16)


def draw_decay_log(key, part):
    sampler_seeds = jax.random.split(jax.random.fold_in(key, 37), 3)
    slow_low = jnp.log(0.5 / (0.05 * PROMPT_SPAN))
    slow_high = jnp.log(2.0 / (0.05 * PROMPT_SPAN))
    fast_share = 0.5
    slow_part = jax.random.uniform(sampler_seeds[0], (HEAD_COUNT,), minval=slow_low, maxval=slow_high)
    fast_part = jax.random.uniform(sampler_seeds[1], (HEAD_COUNT,), minval=jnp.log(0.3), maxval=jnp.log(0.67))
    fast_pick = jax.random.uniform(sampler_seeds[2], (HEAD_COUNT,)) < fast_share
    return jnp.where(fast_pick, fast_part, slow_part).astype(jnp.float32)


def plant(drawn, stream_key, low, largest):
    longest = drawn.shape.index(max(drawn.shape))
    spots = []
    for shift in (0, 1):
        where = [jax.random.randint(jax.random.fold_in(stream_key, axis), (), 0, length) for axis, length in enumerate(drawn.shape)]
        where[longest] = (where[longest] + shift) % drawn.shape[longest]
        spots.append(tuple(where))
    return drawn.at[spots[0]].set(low).at[spots[1]].set(largest)


def block_scale(own_key, shape, shards, least, high):
    level = 1.0
    for dim, blocks in shards:
        draws = jax.random.uniform(jax.random.fold_in(jax.random.fold_in(own_key, 6), dim), (blocks,), jnp.float32, least / len(shards), high / len(shards))
        level = level * jnp.repeat(jnp.exp(draws), shape[dim] // blocks).reshape((-1,) + (1,) * (len(shape) - 1 - dim))
    return level


def normal_values(own_key, dims, width, limit, pieces=(), kind=jnp.bfloat16):
    entries = jax.random.normal(own_key, dims, jnp.float32) * width
    if len(pieces) > 0:
        entries = block_scale(own_key, dims, pieces, -0.22, 0.18) * entries
    return jnp.clip(entries, min=-limit, max=limit).astype(kind)


def setup_inputs(seed: int = 0) -> dict:
    streams_of = jax.random.split(jax.random.key(seed), 17)
    pool_states = normal_values(streams_of[0], (POOL_SLOTS, HEAD_COUNT, HEAD_DIM, STATE_DIM), 1.0, 6.0, ((0, 32), (1, 4)), jnp.float32)
    inner_window = normal_values(streams_of[1], (POOL_SLOTS, KERNEL - 1, INNER_DIM), 1.0, 6.0, ((0, 32), (2, 4)))
    state_window = normal_values(streams_of[2], (POOL_SLOTS, KERNEL - 1, 2 * STATE_DIM), 1.0, 6.0, ((0, 32), (2, 4)))
    move_plan = draw_move_plan(jax.random.fold_in(streams_of[16], 71), 0)
    active_mask = plant((jax.random.randint(streams_of[4], (POOL_SLOTS,), 0, 4) < 3).astype(jnp.int32), jax.random.fold_in(streams_of[4], 1), 0, 1)
    inputs_inner = normal_values(streams_of[5], (PROMPT_TOTAL, PROMPT_SPAN, INNER_DIM), 1.0, 6.0, ((0, 32), (1, 4)))
    inputs_state = normal_values(streams_of[6], (PROMPT_TOTAL, PROMPT_SPAN, 2 * STATE_DIM), 1.0, 6.0, ((0, 32), (1, 4)))
    gate_rows = normal_values(streams_of[7], (PROMPT_TOTAL, PROMPT_SPAN, INNER_DIM), 1.0, 6.0, ((0, 32), (1, 4)))
    step_raw = draw_step_raw(jax.random.fold_in(streams_of[16], 71), 0)
    lengths = plant(jax.random.randint(streams_of[9], (PROMPT_TOTAL,), KERNEL, PROMPT_SPAN + 1), jax.random.fold_in(streams_of[9], 1), KERNEL, PROMPT_SPAN).astype(jnp.int32)
    conv_weight = normal_values(streams_of[10], (KERNEL, CHANNELS), KERNEL ** -0.5, 3.0, (), jnp.float32)
    conv_bias = normal_values(streams_of[11], (CHANNELS,), 0.5, 3.0, (), jnp.float32)
    step_bias = jnp.clip(jax.random.uniform(streams_of[12], (HEAD_COUNT,), jnp.float32, -3.3, -2.7), -3.3, -2.7)
    decay_log = draw_decay_log(jax.random.fold_in(streams_of[16], 71), 0)
    skip_weight = jnp.clip(jax.random.uniform(streams_of[14], (HEAD_COUNT,), jnp.float32, 0.5, 1.5), 0.5, 1.5)
    norm_weight = jnp.clip(1.0 + 0.15 * jax.random.normal(streams_of[15], (INNER_DIM,), jnp.float32), 0.25, 1.75)
    return dict(pool_states=pool_states, inner_window=inner_window, state_window=state_window, move_plan=move_plan, active_mask=active_mask, inputs_inner=inputs_inner, inputs_state=inputs_state, gate_rows=gate_rows, step_raw=step_raw, lengths=lengths, conv_weight=conv_weight, conv_bias=conv_bias, step_bias=step_bias, decay_log=decay_log, skip_weight=skip_weight, norm_weight=norm_weight)


EPSILON = 1e-05

def conv_silu(window, new_rows, weight, bias_values):
    extended = jnp.concatenate([window, new_rows], axis=1).astype(jnp.float32)
    length = new_rows.shape[1]
    running = jnp.zeros(new_rows.shape, jnp.float32) + bias_values
    for offset in range(weight.shape[0]):
        running = running + weight[offset] * extended[:, offset:offset + length]
    return jax.nn.silu(running).astype(jnp.bfloat16)

def block_local(value_rows, write_rows, read_rows, step_rows, decay_rates):
    log_decay = step_rows * decay_rates
    running_log = jnp.cumsum(log_decay, axis=0)
    scores = jnp.dot(read_rows, write_rows.T, preferred_element_type=jnp.float32)
    log_heads = running_log.T
    log_gaps = log_heads[:, :, None] - log_heads[:, None, :]
    positions = jnp.arange(running_log.shape[0])
    causal = positions[:, None] >= positions[None, :]
    decays = jnp.where(causal, jnp.exp(jnp.where(causal, log_gaps, 0.0)), 0.0)
    weights = (scores[None] * decays * step_rows.T[:, None, :]).astype(jnp.bfloat16)
    intra_part = jnp.einsum('hts,shp->thp', weights.astype(jnp.float32), value_rows.astype(jnp.float32))
    to_end = jnp.exp(running_log[-1:] - running_log) * step_rows
    scaled = (to_end[:, :, None] * value_rows.astype(jnp.float32)).astype(jnp.bfloat16)
    block_state = jnp.einsum('shp,sn->hpn', scaled.astype(jnp.float32), write_rows.astype(jnp.float32))
    return (intra_part, block_state, running_log)

def gated_norm(payload_array, gate_part, norm_weight):
    gated_rows = payload_array.astype(jnp.float32) * jax.nn.silu(gate_part.astype(jnp.float32))
    norm_scale = lax.rsqrt(lax.optimization_barrier(jnp.mean(gated_rows * gated_rows, axis=-1, keepdims=True)) + EPSILON)
    return (gated_rows * norm_scale * norm_weight).astype(jnp.bfloat16)

def reference(pool_states, inner_window, state_window, move_plan, active_mask, inputs_inner, inputs_state, gate_rows, step_raw, lengths, conv_weight, conv_bias, step_bias, decay_log, skip_weight, norm_weight):
    keep_flag = active_mask.astype(jnp.float32)
    targets = (move_plan[:, 0] * SLOTS_DEV + move_plan[:, 1]).astype(jnp.int32)
    moved_states = jnp.zeros_like(pool_states).at[targets].set(pool_states * keep_flag[:, None, None, None])
    moved_inner = jnp.zeros_like(inner_window).at[targets].set((inner_window.astype(jnp.float32) * keep_flag[:, None, None]).astype(jnp.bfloat16))
    moved_outer = jnp.zeros_like(state_window).at[targets].set((state_window.astype(jnp.float32) * keep_flag[:, None, None]).astype(jnp.bfloat16))
    sequence_index = jnp.arange(PROMPT_TOTAL).astype(jnp.int32)
    slot_index = (sequence_index // PREFILLS * SLOTS_DEV + sequence_index % PREFILLS).astype(jnp.int32)
    decay_rates = -jnp.exp(decay_log)
    block_count = PROMPT_SPAN // BLOCK_LEN

    def split_blocks(source):
        return source.reshape((block_count, BLOCK_LEN) + source.shape[1:])

    def one_block(members):
        return block_local(members[0], members[1], members[2], members[3], decay_rates)

    def advance(carried, members):
        block_state, running_log, read_block = members
        inter_part = jnp.einsum('qn,hpn->qhp', read_block.astype(jnp.float32), carried, precision=lax.Precision.HIGHEST) * jnp.exp(running_log)[:, :, None]
        updated = jnp.exp(running_log[-1])[:, None, None] * carried + block_state
        return (updated, inter_part)

    def prefill_one(members):
        initial, head_inner, head_outer, inner_rows, outer_rows, gate_part, step_part, length_one = members
        raw_rows = jnp.concatenate([inner_rows, outer_rows], axis=1)
        window = jnp.concatenate([head_inner, head_outer], axis=1)
        mixed_rows = conv_silu(window[None], raw_rows[None], conv_weight, conv_bias)[0]
        value_rows = mixed_rows[:, :INNER_DIM].reshape(PROMPT_SPAN, HEAD_COUNT, HEAD_DIM)
        write_rows = mixed_rows[:, INNER_DIM:INNER_DIM + STATE_DIM]
        read_rows = mixed_rows[:, INNER_DIM + STATE_DIM:]
        valid_rows = (jnp.arange(PROMPT_SPAN).astype(jnp.int32) < length_one).astype(jnp.float32)
        step_sizes = jax.nn.softplus(step_part.astype(jnp.float32) + step_bias) * valid_rows[:, None]
        intra_part, block_states, running_logs = lax.map(one_block, (split_blocks(value_rows), split_blocks(write_rows), split_blocks(read_rows), split_blocks(step_sizes)))
        final_state, inter_parts = lax.scan(advance, initial, (block_states, running_logs, split_blocks(read_rows)))
        combined = (intra_part + inter_parts).reshape(PROMPT_SPAN, HEAD_COUNT, HEAD_DIM) + skip_weight[:, None] * value_rows.astype(jnp.float32)
        y_rows = (combined * valid_rows[:, None, None]).astype(jnp.bfloat16).reshape(PROMPT_SPAN, INNER_DIM)
        mixer_rows = gated_norm(y_rows, gate_part, norm_weight)
        window_pos = (length_one - (KERNEL - 1) + jnp.arange(KERNEL - 1)).astype(jnp.int32)
        last_window = jnp.take(raw_rows, window_pos, axis=0)
        return (final_state, last_window, mixer_rows)
    final_states, last_windows, mixer_out = lax.map(prefill_one, (moved_states[slot_index], moved_inner[slot_index], moved_outer[slot_index], inputs_inner, inputs_state, gate_rows, step_raw, lengths))
    new_states = moved_states.at[slot_index].set(final_states)
    new_inner = moved_inner.at[slot_index].set(last_windows[:, :, :INNER_DIM])
    new_outer = moved_outer.at[slot_index].set(last_windows[:, :, INNER_DIM:])
    return (new_states, new_inner, new_outer, mixer_out)
```

```python
import functools

import jax
import jax.numpy as jnp
from jax import lax
from jax.experimental import pallas as pl
from jax.experimental.pallas import tpu as pltpu
from jax.sharding import PartitionSpec as P

MESH = pl.DeviceIdType.MESH
ANY = pl.BlockSpec(memory_space=pl.ANY)
VM = pl.BlockSpec(memory_space=pltpu.VMEM)
SM = pl.BlockSpec(memory_space=pltpu.SMEM)
F32 = jnp.float32
BF16 = jnp.bfloat16
I32 = jnp.int32

SLOTS = 13
HEADS = 64
INNER = 4096
SPAN = 512
CHUNK = 128
CHUNKS = SPAN // CHUNK
PAIRS = HEADS // 2
HALF = 528
LOG2E = 1.4426950408889634
EPSILON = 1e-05


def nn(a, b):
    return lax.dot_general(a, b, (((1,), (0,)), ((), ())), preferred_element_type=F32)


def nt(a, b):
    return lax.dot_general(a, b, (((1,), (1,)), ((), ())), preferred_element_type=F32)


def split3(v):
    hi = v.astype(BF16)
    rest = v - hi.astype(F32)
    mid = rest.astype(BF16)
    lo = (rest - mid.astype(F32)).astype(BF16)
    return hi, mid, lo


def silu(v):
    return v / (1.0 + jnp.exp(-v))


def softplus(v):
    u = jnp.exp(-jnp.abs(v))
    series = u * (1.0 - u * (0.5 - u * (1.0 / 3.0 - u * (0.25 - u * 0.2))))
    return jnp.maximum(v, 0.0) + jnp.where(u < 0.02, series, jnp.log(1.0 + u))


def pick_matrix(rows, pair):
    row = lax.rem(lax.broadcasted_iota(I32, (rows, 128), 0), 64)
    lane = lax.broadcasted_iota(I32, (rows, 128), 1)
    head = 2 * pair + (lane >= 64).astype(I32)
    return jnp.where(row == head, 1.0, 0.0).astype(BF16)


def conv_tile(x, taps, bias, rows):
    acc = bias + taps[3:4] * x[16 : 16 + rows]
    for k in range(3):
        acc = acc + taps[k : k + 1] * x[13 + k : 13 + k + rows]
    return silu(acc).astype(BF16)


def exchange_kernel(
    meta, lens, skip, tags, pool, win, xin, xst, step, conv_w, conv_b, step_b, decay,
    out_a, out_b, s0_all, f_in, f_st, f_dt, y_out, read_out, cum_out, pre_out, tot_out, fin_out, kept_out,
    stage, sbuf_a, sbuf_b, rel_a, rel_b, rbuf_a, rbuf_b, xbuf, xsbuf, y_buf, read_buf, cum_buf, st_buf,
    lbuf, tbuf, tagbuf, tag_s, cum3, cumt, dt2, sc_buf, wt_buf, base_buf, pay, pre_buf, fin_buf, kept_buf,
    ffin, ffst, ffdt,
    pool_sem, in_sem, out_sem, one_send, one_recv, two_send, two_recv, tag_send, tag_recv,
    halo_send, halo_recv, lend_send, lend_recv, s0_send, s0_recv, f_send, f_recv,
):
    me = lax.axis_index("req")
    my = lax.axis_index("seq")
    mx, mz, mc = me // 8, (me // 2) % 4, me % 2

    def at(dx, dz, dc):
        return ((mx + dx) % 4) * 8 + ((mz + dz) % 4) * 2 + (mc + dc) % 2

    loads = []
    for k in range(SLOTS):
        cp = pltpu.make_async_copy(pool.at[k], stage.at[k], pool_sem.at[k])
        cp.start()
        loads.append(cp)
    ins = [
        pltpu.make_async_copy(xin, xbuf.at[pl.ds(16, SPAN)], in_sem.at[0]),
        pltpu.make_async_copy(xst, xsbuf.at[pl.ds(16, SPAN)], in_sem.at[1]),
    ]
    for cp in ins:
        cp.start()

    barrier = pltpu.get_barrier_semaphore()
    for r in range(1, 32):
        peer = at(r // 8, (r // 2) % 4, r % 2)
        pl.semaphore_signal(barrier, inc=1, device_id=(peer, my), device_id_type=MESH)
    for r in range(1, 4):
        pl.semaphore_signal(barrier, inc=1, device_id=(me, (my + r) % 4), device_id_type=MESH)
    pl.semaphore_wait(barrier, 34)

    pending = []

    def send(src, dst, ssem, rsem, dev):
        cp = pltpu.make_async_remote_copy(
            src_ref=src, dst_ref=dst, send_sem=ssem, recv_sem=rsem, device_id=dev, device_id_type=MESH
        )
        cp.start()
        return cp

    halo = [
        send(xin.at[pl.ds(SPAN - 16, 16)], xbuf.at[pl.ds(0, 16)], halo_send.at[0], halo_recv.at[0], (me, (my + 1) % 4)),
        send(xst.at[pl.ds(SPAN - 16, 16)], xsbuf.at[pl.ds(0, 16)], halo_send.at[1], halo_recv.at[1], (me, (my + 1) % 4)),
    ]
    firsts = []
    for r in range(1, 4):
        dev = (me, (my + r) % 4)
        firsts.append(send(xin.at[pl.ds(0, 16)], ffin.at[my], f_send.at[r], f_recv.at[r], dev))
        firsts.append(send(xst.at[pl.ds(0, 16)], ffst.at[my], f_send.at[4 + r], f_recv.at[4 + r], dev))
        firsts.append(send(step.at[pl.ds(0, 16)], ffdt.at[my], f_send.at[8 + r], f_recv.at[8 + r], dev))

    for cp in loads:
        cp.wait()

    def fill(dest, half, put):
        slot = meta[dest, 0]
        keep = meta[dest, 1].astype(F32)
        put(0, (stage[slot, pl.ds(512 * half, 512), :] * keep).astype(BF16))
        put(512, (win[slot, pl.ds(16 * half, 16), :].astype(F32) * keep).astype(BF16))

    def fill_a(ref, lead, xd):
        def one(q, carry):
            def put(row, value):
                ref[lead, q, pl.ds(row, value.shape[0]), :] = value

            fill(xd * 8 + q, 0, put)
            return carry

        lax.fori_loop(0, 8, one, 0)

    def fill_b(ref, lead, zd):
        def one(q, carry):
            def put(row, value):
                ref[lead, q, pl.ds(row, value.shape[0]), :] = value

            fill((q // 2) * 8 + zd * 2 + q % 2, 1, put)
            return carry

        lax.fori_loop(0, 8, one, 0)

    phase_a, phase_b = {}, {}
    for d in (2, 1, 3):
        xd = (mx + d) % 4
        fill_a(sbuf_a, xd, xd)
        phase_a[d] = send(sbuf_a.at[xd], rel_a.at[mx], one_send.at[d], one_recv.at[d], (at(d, 0, 0), my))
        zd = (mz + d) % 4
        fill_b(sbuf_b, zd, zd)
        phase_b[d] = send(sbuf_b.at[zd], rel_b.at[mz], one_send.at[4 + d], one_recv.at[4 + d], (at(0, d, 0), my))
    fill_a(rel_a, mx, mx)
    fill_b(rel_b, mz, mz)

    second = []

    def forward(d):
        xs = (mx + 4 - d) % 4
        zs = (mz + 4 - d) % 4
        for e in range(1, 8):
            de, dc = e // 2, e % 2
            sem = d * 8 + e
            zt, xt, ct = (mz + de) % 4, (mx + de) % 4, (mc + dc) % 2
            second.append(
                send(rel_a.at[xs, zt * 2 + ct], rbuf_a.at[xs * 8 + mz * 2 + mc],
                     two_send.at[sem], two_recv.at[sem], (at(0, de, dc), my))
            )
            second.append(
                send(rel_b.at[zs, xt * 2 + ct], rbuf_b.at[mx * 8 + zs * 2 + mc],
                     two_send.at[32 + sem], two_recv.at[32 + sem], (at(de, 0, dc), my))
            )
        rbuf_a[xs * 8 + mz * 2 + mc] = rel_a[xs, mz * 2 + mc]
        rbuf_b[mx * 8 + zs * 2 + mc] = rel_b[zs, mx * 2 + mc]

    forward(0)

    tag_copies = []
    for r in range(1, 32):
        peer = at(r // 8, (r // 2) % 4, r % 2)
        tag_copies.append(
            send(tags.at[peer], tagbuf.at[me], tag_send.at[r], tag_recv.at[r], (peer, my))
        )
    tagbuf[me] = tags[me]

    for cp in ins:
        cp.wait()
    for cp in halo:
        cp.wait()

    @pl.when(my == 0)
    def _():
        xbuf[pl.ds(0, 16), :] = jnp.zeros((16, INNER), BF16)
        xsbuf[pl.ds(0, 16), :] = jnp.zeros((16, 256), BF16)

    st_buf[...] = jnp.zeros_like(st_buf)
    base_buf[...] = jnp.zeros_like(base_buf)
    length = lens[0]

    def chunk_body(k, carry):
        r0 = pl.multiple_of(k * CHUNK, CHUNK)
        pos = my * SPAN + r0 + lax.broadcasted_iota(I32, (CHUNK, HEADS), 0)
        live = ((pos < length) & (pos >= 3)).astype(F32)
        dt = softplus(step[pl.ds(r0, CHUNK), :].astype(F32) + step_b[0:1, :]) * live
        rate = dt * (-LOG2E * jnp.exp(decay[0:1, :]))
        rows = lax.broadcasted_iota(I32, (CHUNK, CHUNK), 0)
        cols = lax.broadcasted_iota(I32, (CHUNK, CHUNK), 1)
        tri = jnp.where(rows >= cols, 1.0, 0.0).astype(BF16)
        hi, mid, lo = split3(rate)
        cum = nn(tri, hi) + nn(tri, mid) + nn(tri, lo)
        cum3[...] = jnp.concatenate(split3(cum), axis=1)
        cumt[...] = jnp.transpose(cum)
        dth = dt.astype(BF16)
        dt2[...] = jnp.concatenate([dth, (dt - dth.astype(F32)).astype(BF16)], axis=1)
        cum_buf[pl.ds(r0, CHUNK), :] = cum + base_buf[0:1, 0:HEADS]
        base_buf[0:1, 0:HEADS] = base_buf[0:1, 0:HEADS] + cum[CHUNK - 1 : CHUNK, :]
        xs_tile = xsbuf[pl.ds(r0, CHUNK + 16), :].astype(F32)
        mixed = conv_tile(xs_tile, conv_w[:, INNER : INNER + 256], conv_b[0:1, INNER : INNER + 256], CHUNK)
        write, read = mixed[:, 0:128], mixed[:, 128:256]
        read_buf[pl.ds(r0, CHUNK), :] = read
        sc_buf[...] = jnp.where(rows >= cols, nt(read, write), 0.0)
        wt_buf[...] = jnp.transpose(write.astype(F32)).astype(BF16)

        def pair_body(i, inner):
            l0 = pl.multiple_of(i * 128, 128)
            lanes = pl.ds(l0, 128)
            x = xbuf[pl.ds(r0, CHUNK + 16), lanes].astype(F32)
            value = conv_tile(x, conv_w[:, lanes], conv_b[0:1, lanes], CHUNK)
            row = lax.rem(lax.broadcasted_iota(I32, (192, 256), 0), 64)
            lane2 = lax.broadcasted_iota(I32, (192, 256), 1)
            sel = jnp.where(row == 2 * i + (lane2 >= 128).astype(I32), 1.0, 0.0).astype(BF16)
            both = nn(cum3[...], sel)
            c1, c2 = both[:, 0:128], both[:, 128:256]
            sc = sc_buf[...]
            w1 = sc * jnp.exp2(jnp.minimum(c1 - cumt[pl.ds(2 * i, 1), :], 0.0))
            w2 = sc * jnp.exp2(jnp.minimum(c2 - cumt[pl.ds(2 * i + 1, 1), :], 0.0))
            low = lax.broadcasted_iota(I32, (CHUNK, 128), 1) < 64
            cp = jnp.where(low, c1, c2)
            vf = value.astype(F32)
            vd = vf * nn(dt2[...], pick_matrix(128, i))
            zero = jnp.zeros_like(vd)
            rhs = jnp.concatenate([jnp.where(low, vd, zero), jnp.where(low, zero, vd)], axis=0).astype(BF16)
            lhs = jnp.concatenate([w1.astype(BF16), w2.astype(BF16)], axis=1)
            state = st_buf[:, lanes]
            lane = lax.broadcasted_iota(I32, (1, 128), 1)
            skip_lane = jnp.where(lane < 64, skip[2 * i], skip[2 * i + 1])
            y = nn(lhs, rhs) + nn(read_buf[pl.ds(r0, CHUNK), :], state.astype(BF16)) * jnp.exp2(cp) + skip_lane * vf
            y_buf[pl.ds(r0, CHUNK), lanes] = y.astype(y_buf.dtype)
            last = cp[CHUNK - 1 : CHUNK, :]
            scaled = (jnp.exp2(last - cp) * vd).astype(BF16)
            st_buf[:, lanes] = jnp.exp2(last) * state + nn(wt_buf[...], scaled)
            return inner

        lax.fori_loop(0, PAIRS, pair_body, 0)
        return carry

    lax.fori_loop(0, CHUNKS, chunk_body, 0)

    cols = lax.broadcasted_iota(I32, (16, SPAN), 1)
    rows = lax.broadcasted_iota(I32, (16, SPAN), 0)
    want = length - 3 - my * SPAN
    sel_in = jnp.where((cols == want + rows) & (rows < 3), 1.0, 0.0).astype(BF16)
    sel_st = jnp.where((cols == want + rows - 3) & (rows >= 3) & (rows < 6), 1.0, 0.0).astype(BF16)
    lst = nn(sel_st, xsbuf[pl.ds(16, SPAN), :])

    def lend_body(i, carry):
        lanes = pl.ds(pl.multiple_of(i * 256, 256), 256)
        lbuf[my, pl.ds(0, 128), lanes] = st_buf[:, lanes].astype(BF16)
        first = jnp.where(i == 0, 1.0, 0.0)
        lbuf[my, pl.ds(128, 16), lanes] = (nn(sel_in, xbuf[pl.ds(16, SPAN), lanes]) + first * lst).astype(BF16)
        return carry

    lax.fori_loop(0, INNER // 256, lend_body, 0)
    tbuf[my] = base_buf[...]
    lends = []
    for r in range(1, 4):
        dev = (me, (my + r) % 4)
        lends.append(send(lbuf.at[my], lbuf.at[my], lend_send.at[r], lend_recv.at[r], dev))
        lends.append(send(tbuf.at[my], tbuf.at[my], lend_send.at[4 + r], lend_recv.at[4 + r], dev))

    outs = []

    def put_out(src, dst, i):
        cp = pltpu.make_async_copy(src, dst, out_sem.at[i])
        cp.start()
        outs.append(cp)

    put_out(y_buf, y_out, 0)
    put_out(read_buf, read_out, 1)
    put_out(cum_buf, cum_out, 2)

    for d in (1, 3, 2):
        phase_a[d].wait_recv()
        phase_b[d].wait_recv()
        forward(d)

    for cp in lends:
        cp.wait()

    tot = [tbuf[c][0:1, 0:HEADS] for c in range(4)]
    zero_row = jnp.zeros((1, HEADS), F32)
    prior_rows, suffix_rows = [], []
    for c in range(4):
        before, after = zero_row, zero_row
        for other in range(c + 1, 4):
            after = after + tot[other]
            before = before + tot[other] * jnp.where(other < my, 1.0, 0.0)
        prior_rows.append(jnp.exp2(before) * jnp.where(c < my, 1.0, 0.0))
        suffix_rows.append(jnp.exp2(after))
    prior_log = zero_row
    whole_log = zero_row
    for c in range(4):
        prior_log = prior_log + tot[c] * jnp.where(c < my, 1.0, 0.0)
        whole_log = whole_log + tot[c]
    factors = jnp.concatenate(prior_rows + suffix_rows + [jnp.exp2(whole_log)] + [zero_row] * 7, axis=0)
    factors3 = jnp.concatenate(split3(factors), axis=1)
    tot_out_rows = jnp.concatenate([prior_log, whole_log] + [zero_row] * 6, axis=0)
    base_buf[:, 0:HEADS] = tot_out_rows

    def pre_body(i, carry):
        lanes = pl.ds(pl.multiple_of(i * 128, 128), 128)
        f = nn(factors3, pick_matrix(192, i))
        acc = f[0:1] * lbuf[0, pl.ds(0, 128), lanes].astype(F32)
        for c in range(1, 4):
            acc = acc + f[c : c + 1] * lbuf[c, pl.ds(0, 128), lanes].astype(F32)
        pre_buf[:, lanes] = acc.astype(BF16)
        return carry

    lax.fori_loop(0, PAIRS, pre_body, 0)

    def fin_body(q, carry):
        i = my * 8 + q
        lanes = pl.ds(pl.multiple_of(i * 128, 128), 128)
        f = nn(factors3, pick_matrix(192, i))
        acc = f[4:5] * lbuf[0, pl.ds(0, 128), lanes].astype(F32)
        kept = lbuf[0, pl.ds(128, 16), lanes].astype(F32)
        for c in range(1, 4):
            acc = acc + f[4 + c : 5 + c] * lbuf[c, pl.ds(0, 128), lanes].astype(F32)
            kept = kept + lbuf[c, pl.ds(128, 16), lanes].astype(F32)
        fin_buf[pl.ds(pl.multiple_of(q * 128, 128), 128), :] = jnp.transpose(acc)
        kept_buf[:, pl.ds(pl.multiple_of(q * 128, 128), 128)] = kept.astype(BF16)
        return carry

    lax.fori_loop(0, 8, fin_body, 0)
    kst = lbuf[0, pl.ds(128, 16), pl.ds(0, 256)].astype(F32)
    for c in range(1, 4):
        kst = kst + lbuf[c, pl.ds(128, 16), pl.ds(0, 256)].astype(F32)
    kept_buf[:, pl.ds(1024, 256)] = kst.astype(BF16)

    for i, ref in enumerate(((pre_buf, pre_out), (base_buf, tot_out), (fin_buf, fin_out), (kept_buf, kept_out))):
        put_out(ref[0], ref[1], 3 + i)

    for cp in firsts:
        cp.wait()
    ffin_own = pltpu.make_async_copy(xin.at[pl.ds(0, 16)], ffin.at[my], in_sem.at[2])
    ffst_own = pltpu.make_async_copy(xst.at[pl.ds(0, 16)], ffst.at[my], in_sem.at[3])
    ffin_own.start()
    ffst_own.start()
    ffdt[my] = step[pl.ds(0, 16), :]
    ffin_own.wait()
    ffst_own.wait()
    put_out(ffin.at[0], f_in, 7)
    put_out(ffst.at[0], f_st, 8)
    put_out(ffdt.at[0], f_dt, 9)

    for cp in tag_copies:
        cp.wait()
    tag_load = pltpu.make_async_copy(tagbuf, tag_s, in_sem.at[4])
    tag_load.start()
    tag_load.wait()

    def source_of(j):
        acc = jnp.int32(0)
        for s in range(32):
            acc = acc + jnp.where(tag_s[s, 0, 0] == j + 1, s, 0)
        return acc

    for d in (1, 2, 3):
        phase_a[d].wait_send()
        phase_b[d].wait_send()
    for cp in second:
        cp.wait()

    src0 = source_of(0)
    pay[my, 0] = rbuf_a[src0]
    pay[my, 1] = rbuf_b[src0]
    s0s = []
    for r in range(1, 4):
        s0s.append(send(pay.at[my], pay.at[my], s0_send.at[r], s0_recv.at[r], (me, (my + r) % 4)))
    for j in range(1, SLOTS):
        src = source_of(j)
        sbuf_a[j // 8, j % 8] = rbuf_a[src]
        sbuf_b[j // 8, j % 8] = rbuf_b[src]
        put_out(sbuf_a.at[j // 8, j % 8], out_a.at[j], 10 + 2 * j)
        put_out(sbuf_b.at[j // 8, j % 8], out_b.at[j], 11 + 2 * j)
    put_out(pay.at[my, 0], out_a.at[0], 10)
    put_out(pay.at[my, 1], out_b.at[0], 11)
    for cp in s0s:
        cp.wait()
    put_out(pay, s0_all, 36)
    for cp in outs:
        cp.wait()


def exchange(meta, lens, skip, tags, pool, win, xin, xst, step, conv_w, conv_b, step_b, decay):
    dma = pltpu.SemaphoreType.DMA
    shape = jax.ShapeDtypeStruct
    out_shape = (
        shape((SLOTS, HALF, 128), BF16),
        shape((SLOTS, HALF, 128), BF16),
        shape((4, 2, HALF, 128), BF16),
        shape((16, INNER), BF16),
        shape((16, 256), BF16),
        shape((16, HEADS), BF16),
        shape((SPAN, INNER), BF16),
        shape((SPAN, 128), BF16),
        shape((SPAN, HEADS), F32),
        shape((128, INNER), BF16),
        shape((8, 128), F32),
        shape((1024, 128), F32),
        shape((16, 1280), BF16),
    )
    scratch = [
        pltpu.VMEM((SLOTS, 1024, 128), F32),
        pltpu.VMEM((4, 8, HALF, 128), BF16),
        pltpu.VMEM((4, 8, HALF, 128), BF16),
        pltpu.VMEM((4, 8, HALF, 128), BF16),
        pltpu.VMEM((4, 8, HALF, 128), BF16),
        pltpu.VMEM((32, HALF, 128), BF16),
        pltpu.VMEM((32, HALF, 128), BF16),
        pltpu.VMEM((SPAN + 16, INNER), BF16),
        pltpu.VMEM((SPAN + 16, 256), BF16),
        pltpu.VMEM((SPAN, INNER), BF16),
        pltpu.VMEM((SPAN, 128), BF16),
        pltpu.VMEM((SPAN, HEADS), F32),
        pltpu.VMEM((128, INNER), F32),
        pltpu.VMEM((4, 144, INNER), BF16),
        pltpu.VMEM((4, 8, 128), F32),
        pltpu.VMEM((32, 1, 128), I32),
        pltpu.SMEM((32, 1, 128), I32),
        pltpu.VMEM((CHUNK, 192), BF16),
        pltpu.VMEM((HEADS, CHUNK), F32),
        pltpu.VMEM((CHUNK, 128), BF16),
        pltpu.VMEM((CHUNK, CHUNK), F32),
        pltpu.VMEM((CHUNK, CHUNK), BF16),
        pltpu.VMEM((8, 128), F32),
        pltpu.VMEM((4, 2, HALF, 128), BF16),
        pltpu.VMEM((128, INNER), BF16),
        pltpu.VMEM((1024, 128), F32),
        pltpu.VMEM((16, 1280), BF16),
        pltpu.VMEM((4, 16, INNER), BF16),
        pltpu.VMEM((4, 16, 256), BF16),
        pltpu.VMEM((4, 16, HEADS), BF16),
        dma((SLOTS,)), dma((5,)), dma((37,)),
        dma((8,)), dma((8,)), dma((64,)), dma((64,)), dma((32,)), dma((32,)),
        dma((2,)), dma((2,)), dma((8,)), dma((8,)), dma((4,)), dma((4,)), dma((12,)), dma((12,)),
    ]
    return pl.pallas_call(
        exchange_kernel,
        out_shape=out_shape,
        in_specs=[SM, SM, SM, VM, ANY, VM, ANY, ANY, VM, VM, VM, VM, VM],
        out_specs=[ANY] * len(out_shape),
        scratch_shapes=scratch,
        compiler_params=pltpu.CompilerParams(
            collective_id=1, has_side_effects=True, vmem_limit_bytes=67043328
        ),
        name="exchange",
    )(meta, lens, skip, tags, pool, win, xin, xst, step, conv_w, conv_b, step_b, decay)


def mixer_kernel(
    lens, skip, y_ref, gate, read_ref, cum_ref, pre, s0_all, tot, f_in, f_st, f_dt, wfirst, wfst,
    conv_w, conv_b, step_b, decay, norm_w, out,
    gated, r0_buf, cum3, rw_buf, sc0_buf, cf3_buf, dtf3_buf, prior3,
):
    my = lax.axis_index("seq")
    k = pl.program_id(0)
    length = lens[0]

    posf = lax.broadcasted_iota(I32, (16, HEADS), 0)
    live = ((posf < length) & (posf < 3)).astype(F32)
    dt = softplus(f_dt[...].astype(F32) + step_b[0:1, :]) * live
    rate = dt * (-LOG2E * jnp.exp(decay[0:1, :]))
    c0 = rate[0:1]
    c1 = c0 + rate[1:2]
    c2 = c1 + rate[2:3]
    cumf = jnp.concatenate([c0, c1, c2] + [c2] * 13, axis=0)
    e_st = jnp.concatenate([wfst[...], f_st[...]], axis=0).astype(F32)
    mixed = conv_tile(e_st, conv_w[:, INNER : INNER + 256], conv_b[0:1, INNER : INNER + 256], 16)
    write0, read0 = mixed[:, 0:128], mixed[:, 128:256]
    sc0_buf[...] = nt(read0, write0)
    rw_buf[...] = nt(read_ref[...], write0).astype(BF16)
    cum3[...] = jnp.concatenate(split3(cum_ref[...]), axis=1)
    prior3[...] = jnp.concatenate(split3(jnp.broadcast_to(tot[0:1, 0:HEADS], (16, HEADS))), axis=1)
    cf3_buf[...] = jnp.concatenate(split3(cumf), axis=1)
    dtf3_buf[...] = jnp.concatenate(split3(dt), axis=1)
    r0_buf[...] = read0
    rowpos = my * SPAN + k * CHUNK + lax.broadcasted_iota(I32, (CHUNK, 128), 0)
    valid = (rowpos < length).astype(F32)
    head3 = rowpos < 3
    valid0 = (lax.broadcasted_iota(I32, (16, 128), 0) < length).astype(F32)

    def pair_body(i, total):
        l0 = pl.multiple_of(i * 128, 128)
        lanes = pl.ds(l0, 128)
        sel = pick_matrix(192, i)
        read = read_ref[...]
        e = jnp.exp2(nn(cum3[...], sel))
        cf = nn(cf3_buf[...], sel)
        dtf = nn(dtf3_buf[...], sel)
        x0 = jnp.concatenate([wfirst[:, lanes], f_in[:, lanes]], axis=0).astype(F32)
        v0 = conv_tile(x0, conv_w[:, lanes], conv_b[0:1, lanes], 16)
        v0f = v0.astype(F32)
        vd = v0f * dtf
        scaled = (jnp.exp2(cf[2:3] - cf) * vd).astype(BF16)
        owner = i // 8
        row = pl.multiple_of((i % 8) // 4 * HALF + (i % 4) * 128, 16)
        s0 = s0_all[owner, pl.ds(row, 128), :]
        prior = jnp.exp2(nn(prior3[...], sel)[0:1])
        a = (nt(read, s0) * jnp.exp2(cf[2:3]) + nn(rw_buf[...], scaled)) * prior + nn(read, pre_tile(i))
        lane = lax.broadcasted_iota(I32, (1, 128), 1)
        skip_lane = jnp.where(lane < 64, skip[2 * i], skip[2 * i + 1])
        y = y_ref[:, lanes].astype(F32) + e * a
        y0 = nt(r0_buf[...], s0) * jnp.exp2(cf) + skip_lane * v0f
        row16 = lax.broadcasted_iota(I32, (16, 128), 0)
        for s in range(3):
            term = sc0_buf[:, s : s + 1] * jnp.exp2(jnp.minimum(cf - cf[s : s + 1], 0.0)) * vd[s : s + 1]
            y0 = y0 + jnp.where(row16 >= s, term, 0.0)
        y0 = jnp.concatenate([y0, jnp.zeros((CHUNK - 16, 128), F32)], axis=0)
        y = jnp.where(head3, y0, y) * valid
        g = gate[:, lanes].astype(F32)
        v = y.astype(BF16).astype(F32) * silu(g)
        gated[:, lanes] = v
        return total + v * v

    def pre_tile(i):
        return pre[:, pl.ds(pl.multiple_of(i * 128, 128), 128)]

    total = lax.fori_loop(0, PAIRS, pair_body, jnp.zeros((CHUNK, 128), F32))
    scale = lax.rsqrt(jnp.sum(total, axis=1, keepdims=True) * (1.0 / INNER) + EPSILON)

    def norm_body(i, carry):
        lanes = pl.ds(pl.multiple_of(i * 128, 128), 128)
        out[:, lanes] = (gated[:, lanes] * scale * norm_w[0:1, lanes]).astype(BF16)
        return carry

    lax.fori_loop(0, PAIRS, norm_body, 0)


def mixer(lens, skip, y, gate, read, cum, pre, s0_all, tot, f_in, f_st, f_dt, wfirst, wfst,
          conv_w, conv_b, step_b, decay, norm_w):
    rows = lambda lanes: pl.BlockSpec((CHUNK, lanes), lambda k: (k, 0))
    return pl.pallas_call(
        mixer_kernel,
        grid=(CHUNKS,),
        out_shape=jax.ShapeDtypeStruct((SPAN, INNER), BF16),
        in_specs=[SM, SM, rows(INNER), rows(INNER), rows(128), rows(HEADS)] + [VM] * 13,
        out_specs=rows(INNER),
        scratch_shapes=[
            pltpu.VMEM((CHUNK, INNER), F32),
            pltpu.VMEM((16, 128), BF16),
            pltpu.VMEM((CHUNK, 192), BF16),
            pltpu.VMEM((CHUNK, 16), BF16),
            pltpu.VMEM((16, 16), F32),
            pltpu.VMEM((16, 192), BF16),
            pltpu.VMEM((16, 192), BF16),
            pltpu.VMEM((16, 192), BF16),
        ],
        compiler_params=pltpu.CompilerParams(vmem_limit_bytes=48 * 1024 * 1024),
        name="mixer",
    )(lens, skip, y, gate, read, cum, pre, s0_all, tot, f_in, f_st, f_dt, wfirst, wfst,
      conv_w, conv_b, step_b, decay, norm_w)


def place_kernel(a, b, fin, whole, states):
    j = pl.program_id(0)
    states[0, 0:512, :] = a[0, 0:512, :].astype(F32)
    states[0, 512:1024, :] = b[0, 0:512, :].astype(F32)

    @pl.when(j == 0)
    def _():
        states[0] = states[0] * whole[...] + fin[...]


def place(out_a, out_b, fin, whole):
    half = pl.BlockSpec((1, HALF, 128), lambda j: (j, 0, 0))
    return pl.pallas_call(
        place_kernel,
        grid=(SLOTS,),
        out_shape=jax.ShapeDtypeStruct((SLOTS, 1024, 128), F32),
        in_specs=[half, half, VM, VM],
        out_specs=pl.BlockSpec((1, 1024, 128), lambda j: (j, 0, 0)),
        name="place",
    )(out_a, out_b, fin, whole)


def on_device(
    pool_states, inner_window, state_window, move_plan, active_mask, inputs_inner, inputs_state, gate_rows,
    step_raw, lengths, conv_weight, conv_bias, step_bias, decay_log, skip_weight, norm_weight,
):
    my = lax.axis_index("seq")
    match = (move_plan[None, :, 0] == jnp.arange(32, dtype=I32)[:, None]).astype(I32)
    slot = jnp.sum(match * jnp.arange(SLOTS, dtype=I32)[None, :], axis=1)
    keep = jnp.sum(match * active_mask[None, :], axis=1)
    tag = jnp.sum(match * (move_plan[None, :, 1] + 1), axis=1)
    meta = jnp.stack([slot, keep], axis=1)
    tags = jnp.broadcast_to(tag[:, None, None], (32, 1, 128))
    win = jnp.concatenate(
        [
            inner_window.reshape(SLOTS, 24, 128),
            jnp.pad(state_window.reshape(SLOTS, 192), ((0, 0), (0, 64))).reshape(SLOTS, 2, 128),
            jnp.zeros((SLOTS, 6, 128), BF16),
        ],
        axis=1,
    )
    conv_b = conv_bias[None]
    step_b = step_bias[None]
    decay = decay_log[None]
    (out_a, out_b, s0_all, f_in, f_st, f_dt, y, read, cum, pre, tot, fin, kept) = exchange(
        meta, lengths, skip_weight, tags, pool_states.reshape(SLOTS, 1024, 128), win,
        inputs_inner[0], inputs_state[0], step_raw[0], conv_weight, conv_b, step_b, decay,
    )
    tail = jnp.concatenate([s0_all[:, 0, 512:528], s0_all[:, 1, 512:528]], axis=1)
    w_in = jnp.moveaxis(tail[:, 0:24].reshape(4, 3, 1024), 0, 1).reshape(3, INNER)
    w_st = jnp.moveaxis(tail[:, 24:26].reshape(4, 256)[:, :192].reshape(4, 3, 64), 0, 1).reshape(3, 256)
    wfirst = jnp.concatenate([jnp.zeros((13, INNER), BF16), w_in], axis=0)
    wfst = jnp.concatenate([jnp.zeros((13, 256), BF16), w_st], axis=0)
    mixer_out = mixer(
        lengths, skip_weight, y, gate_rows[0], read, cum, pre, s0_all.reshape(4, 2 * HALF, 128), tot, f_in, f_st, f_dt,
        wfirst, wfst, conv_weight, conv_b, step_b, decay, norm_weight[None],
    )[None]
    live = (jnp.arange(3) < lengths[0]).astype(F32)[:, None]
    dt = jax.nn.softplus(f_dt[:3].astype(F32) + step_bias) * live
    rate = dt * -jnp.exp(decay_log)
    cumf = jnp.cumsum(rate, axis=0)
    ext_in = jnp.concatenate([w_in, f_in[:3]], axis=0).astype(F32)
    ext_st = jnp.concatenate([w_st, f_st[:3]], axis=0).astype(F32)
    own_in = lax.dynamic_slice_in_dim(ext_in, my * 1024, 1024, 1)
    own_w = lax.dynamic_slice_in_dim(conv_weight, my * 1024, 1024, 1)
    own_b = lax.dynamic_slice_in_dim(conv_bias, my * 1024, 1024, 0)
    v0 = own_b + sum(own_w[k] * own_in[k : k + 3] for k in range(4))
    v0 = jax.nn.silu(v0).astype(BF16).astype(F32)
    w0 = conv_bias[INNER : INNER + 128] + sum(
        conv_weight[k, INNER : INNER + 128] * ext_st[k : k + 3, 0:128] for k in range(4)
    )
    w0 = jax.nn.silu(w0).astype(BF16).astype(F32)
    left = jnp.exp(cumf[2:3] - cumf) * dt * jnp.exp2(tot[1:2, 0:HEADS])
    left = lax.dynamic_slice_in_dim(left, my * 16, 16, 1)
    whole = jnp.exp(cumf[2]) * jnp.exp2(tot[1, 0:HEADS])
    whole = lax.dynamic_slice_in_dim(whole, my * 16, 16, 0)
    sc3 = (left[:, :, None] * v0.reshape(3, 16, 64)).reshape(3, 1024)
    fin = fin + jnp.sum(sc3[:, :, None] * w0[:, None, :], axis=0)
    whole = jnp.broadcast_to(whole[:, None, None], (16, 64, 128)).reshape(1024, 128)
    new_states = place(out_a, out_b, fin, whole).reshape(SLOTS, 16, 64, 128)
    new_in = jnp.concatenate([out_a[:, 512:528], out_b[:, 512:520]], axis=1).reshape(SLOTS, 3, 1024)
    new_st = out_b[:, 520:522].reshape(SLOTS, 256)[:, :192].reshape(SLOTS, 3, 64)
    kept_in = kept[None, 0:3, 0:1024]
    kept_st = lax.dynamic_slice_in_dim(kept[3:6, 1024:1280], my * 64, 64, 1)[None]
    new_in = jnp.concatenate([kept_in, new_in[1:]], axis=0)
    new_st = jnp.concatenate([kept_st, new_st[1:]], axis=0)
    return (new_states, new_in, new_st, mixer_out)


def solution(mesh):
    return jax.shard_map(
        on_device,
        mesh=mesh,
        in_specs=(
            P("req", "seq", None, None), P("req", None, "seq"), P("req", None, "seq"), P("req", None), P("req"),
            P("req", "seq", None), P("req", "seq", None), P("req", "seq", None), P("req", "seq", None), P("req"),
            P(), P(), P(), P(), P(), P(),
        ),
        out_specs=(
            P("req", "seq", None, None), P("req", None, "seq"), P("req", None, "seq"), P("req", "seq", None),
        ),
        check_vma=False,
    )
```

```python
import functools

import jax
import jax.numpy as jnp
from jax import lax
from jax.experimental import pallas as pl
from jax.experimental.pallas import tpu as pltpu
from jax.sharding import PartitionSpec as P

MESH = pl.DeviceIdType.MESH
ANY = pl.BlockSpec(memory_space=pl.ANY)
VM = pl.BlockSpec(memory_space=pltpu.VMEM)
SM = pl.BlockSpec(memory_space=pltpu.SMEM)
F32 = jnp.float32
BF16 = jnp.bfloat16
I32 = jnp.int32

SLOTS = 13
HEADS = 64
INNER = 4096
SPAN = 512
CHUNK = 128
CHUNKS = SPAN // CHUNK
PAIRS = HEADS // 2
HALF = 528
GROUP = 2
LOG2E = 1.4426950408889634
EPSILON = 1e-05


def nn(a, b):
    return lax.dot_general(a, b, (((1,), (0,)), ((), ())), preferred_element_type=F32)


def nt(a, b):
    return lax.dot_general(a, b, (((1,), (1,)), ((), ())), preferred_element_type=F32)


def split3(v):
    hi = v.astype(BF16)
    rest = v - hi.astype(F32)
    mid = rest.astype(BF16)
    lo = (rest - mid.astype(F32)).astype(BF16)
    return hi, mid, lo


def silu(v):
    half = 0.5 * v
    return half + half * jnp.tanh(half)


def softplus(v):
    u = jnp.exp(-jnp.abs(v))
    series = u * (1.0 - u * (0.5 - u * (1.0 / 3.0 - u * (0.25 - u * 0.2))))
    return jnp.maximum(v, 0.0) + jnp.where(u < 0.02, series, jnp.log(1.0 + u))


def pick_lanes(copies, pair):
    row = lax.broadcasted_iota(I32, (64, 128), 0)
    lane = lax.broadcasted_iota(I32, (64, 128), 1)
    one = jnp.where(row == 2 * pair + (lane >= 64).astype(I32), 1.0, 0.0).astype(BF16)
    return jnp.concatenate([one] * copies, axis=0)


def pick_heads(copies, pair):
    row = lax.broadcasted_iota(I32, (64, 256), 0)
    lane = lax.broadcasted_iota(I32, (64, 256), 1)
    one = jnp.where(row == 2 * pair + (lane >= 128).astype(I32), 1.0, 0.0).astype(BF16)
    return jnp.concatenate([one] * copies, axis=0)


def conv_tile(x, taps, bias, rows):
    acc = bias + taps[3:4] * x[16 : 16 + rows]
    for k in range(3):
        acc = acc + taps[k : k + 1] * x[13 + k : 13 + k + rows]
    return silu(acc).astype(BF16)


def exchange_kernel(
    meta, lens, skip, tags, tags_b, pool, win, xin, xst, gate, step, conv_w, conv_b, step_b, decay, norm_w,
    moved, wout, fin_out, mix,
    stage, sbuf_a, sbuf_b, rel_a, rel_b, near_a, near_b, far_a, far_b, xbuf, xsbuf, gbuf, y_buf, read_buf, cum_buf, st_buf,
    lsend, lrecv, ssend, srecv, tbuf, tagbuf, rtag_a, rtag_b, tag_s, rtag_as, rtag_bs,
    cum3, cumt, dt2, sc_buf, wt_buf, base_buf, wtile, fin_buf, wstage, ffin, ffst, ffdt,
    small3, w0t, read0_buf, sc0_buf,
    pool_sem, in_sem, out_sem, one_send, one_recv, two_send, two_recv, tag_send, tag_recv, rt_send, rt_recv,
    halo_send, halo_recv, lend_send, lend_recv, win_send, win_recv, s0_send, s0_recv, f_send, f_recv,
):
    me = lax.axis_index("req")
    my = lax.axis_index("seq")
    mx, mz, mc = me // 8, (me // 2) % 4, me % 2

    def at(dx, dz, dc):
        return ((mx + dx) % 4) * 8 + ((mz + dz) % 4) * 2 + (mc + dc) % 2

    loads = []
    for k in range(SLOTS):
        cp = pltpu.make_async_copy(pool.at[k], stage.at[k], pool_sem.at[k])
        cp.start()
        loads.append(cp)
    ins = [
        pltpu.make_async_copy(xin, xbuf.at[pl.ds(16, SPAN)], in_sem.at[0]),
        pltpu.make_async_copy(xst, xsbuf.at[pl.ds(16, SPAN)], in_sem.at[1]),
    ]
    for cp in ins:
        cp.start()
    gate_load = pltpu.make_async_copy(gate, gbuf, in_sem.at[2])
    gate_load.start()

    barrier = pltpu.get_barrier_semaphore()
    for r in range(1, 32):
        peer = at(r // 8, (r // 2) % 4, r % 2)
        pl.semaphore_signal(barrier, inc=1, device_id=(peer, my), device_id_type=MESH)
    for r in range(1, 4):
        pl.semaphore_signal(barrier, inc=1, device_id=(me, (my + r) % 4), device_id_type=MESH)
    pl.semaphore_wait(barrier, 34)

    def send(src, dst, ssem, rsem, dev):
        cp = pltpu.make_async_remote_copy(
            src_ref=src, dst_ref=dst, send_sem=ssem, recv_sem=rsem, device_id=dev, device_id_type=MESH
        )
        cp.start()
        return cp

    halo = [
        send(xin.at[pl.ds(SPAN - 16, 16)], xbuf.at[pl.ds(0, 16)], halo_send.at[0], halo_recv.at[0], (me, (my + 1) % 4)),
        send(xst.at[pl.ds(SPAN - 16, 16)], xsbuf.at[pl.ds(0, 16)], halo_send.at[1], halo_recv.at[1], (me, (my + 1) % 4)),
    ]
    firsts = []
    for r in range(1, 4):
        dev = (me, (my + r) % 4)
        firsts.append(send(xin.at[pl.ds(0, 16)], ffin.at[my], f_send.at[r], f_recv.at[r], dev))
        firsts.append(send(xst.at[pl.ds(0, 16)], ffst.at[my], f_send.at[4 + r], f_recv.at[4 + r], dev))
        firsts.append(send(step.at[pl.ds(0, 16)], ffdt.at[my], f_send.at[8 + r], f_recv.at[8 + r], dev))

    for cp in loads:
        cp.wait()

    def fill(ref, lead, q, dest, half):
        slot = meta[dest, 0]
        keep = meta[dest, 1].astype(F32)
        ref[lead, q, pl.ds(0, 512), :] = (stage[slot, pl.ds(512 * half, 512), :] * keep).astype(BF16)
        ref[lead, q, pl.ds(512, 16), :] = (win[slot, pl.ds(16 * half, 16), :].astype(F32) * keep).astype(BF16)

    def fill_a(ref, lead, xd):
        def one(q, carry):
            fill(ref, lead, q, xd * 8 + q, 0)
            return carry

        lax.fori_loop(0, 8, one, 0)

    def fill_b(ref, lead, zd):
        def one(q, carry):
            fill(ref, lead, q, (q // 2) * 8 + zd * 2 + q % 2, 1)
            return carry

        lax.fori_loop(0, 8, one, 0)

    phase_a, phase_b, rtags = {}, {}, []
    for d in (2, 1, 3):
        xd, zd = (mx + d) % 4, (mz + d) % 4
        dev_a, dev_b = (at(d, 0, 0), my), (at(0, d, 0), my)
        fill_a(sbuf_a, xd, xd)
        phase_a[d] = send(sbuf_a.at[xd], rel_a.at[mx], one_send.at[d], one_recv.at[d], dev_a)
        fill_b(sbuf_b, zd, zd)
        phase_b[d] = send(sbuf_b.at[zd], rel_b.at[mz], one_send.at[4 + d], one_recv.at[4 + d], dev_b)
        rtags.append(send(tags.at[pl.ds(xd * 8, 8)], rtag_a.at[mx], rt_send.at[d], rt_recv.at[d], dev_a))
        rtags.append(send(tags_b.at[zd], rtag_b.at[mz], rt_send.at[4 + d], rt_recv.at[4 + d], dev_b))
    fill_a(rel_a, mx, mx)
    fill_b(rel_b, mz, mz)

    second = {}

    def row_a(p):
        return (near_a if p < 2 else far_a).at[(p % 2) * 8 + mz * 2 + mc]

    def row_b(p):
        return (near_b if p < 2 else far_b).at[(p % 2) * 8 + mx * 2 + mc]

    def forward(p, e, src_a, src_b):
        de, dc = e // 2, e % 2
        sem = p * 8 + e
        second[p, e, 0] = send(
            src_a, row_a(p), two_send.at[sem], two_recv.at[sem], (at(0, de, dc), my))
        second[p, e, 1] = send(
            src_b, row_b(p), two_send.at[32 + sem], two_recv.at[32 + sem], (at(de, 0, dc), my))

    def targets(e):
        de, dc = e // 2, e % 2
        ct = (mc + dc) % 2
        return ((mz + de) % 4) * 2 + ct, ((mx + de) % 4) * 2 + ct

    for e in range(1, 8):
        ta, tb = targets(e)
        forward(0, e, rel_a.at[mx, ta], rel_b.at[mz, tb])
    row_a(0)[...] = rel_a[mx, mz * 2 + mc]
    row_b(0)[...] = rel_b[mz, mx * 2 + mc]

    tag_copies = []
    for r in range(1, 32):
        peer = at(r // 8, (r // 2) % 4, r % 2)
        tag_copies.append(
            send(tags.at[peer], tagbuf.at[me], tag_send.at[r], tag_recv.at[r], (peer, my))
        )
    tagbuf[me] = tags[me]

    for cp in ins:
        cp.wait()
    for cp in halo:
        cp.wait()

    @pl.when(my == 0)
    def _():
        xbuf[pl.ds(0, 16), :] = jnp.zeros((16, INNER), BF16)
        xsbuf[pl.ds(0, 16), :] = jnp.zeros((16, 256), BF16)

    st_buf[...] = jnp.zeros_like(st_buf)
    base_buf[...] = jnp.zeros_like(base_buf)
    length = lens[0]

    def chunk_body(k, carry):
        r0 = pl.multiple_of(k * CHUNK, CHUNK)
        pos = my * SPAN + r0 + lax.broadcasted_iota(I32, (CHUNK, HEADS), 0)
        live = ((pos < length) & (pos >= 3)).astype(F32)
        dt = softplus(step[pl.ds(r0, CHUNK), :].astype(F32) + step_b[0:1, :]) * live
        rate = dt * (-LOG2E * jnp.exp(decay[0:1, :]))
        rows = lax.broadcasted_iota(I32, (CHUNK, CHUNK), 0)
        cols = lax.broadcasted_iota(I32, (CHUNK, CHUNK), 1)
        tri = jnp.where(rows >= cols, 1.0, 0.0).astype(BF16)
        hi, mid, lo = split3(rate)
        cum = nn(tri, hi) + nn(tri, mid) + nn(tri, lo)
        cum3[...] = jnp.concatenate(split3(cum), axis=1)
        cumt[...] = jnp.transpose(cum)
        dth = dt.astype(BF16)
        dt2[...] = jnp.concatenate([dth, (dt - dth.astype(F32)).astype(BF16)], axis=1)
        cum_buf[pl.ds(r0, CHUNK), :] = cum + base_buf[0:1, 0:HEADS]
        base_buf[0:1, 0:HEADS] = base_buf[0:1, 0:HEADS] + cum[CHUNK - 1 : CHUNK, :]
        xs_tile = xsbuf[pl.ds(r0, CHUNK + 16), :].astype(F32)
        mixed = conv_tile(xs_tile, conv_w[:, INNER : INNER + 256], conv_b[0:1, INNER : INNER + 256], CHUNK)
        write, read = mixed[:, 0:128], mixed[:, 128:256]
        read_buf[pl.ds(r0, CHUNK), :] = read
        sc_buf[...] = jnp.where(rows >= cols, nt(read, write), 0.0)
        wt_buf[...] = jnp.transpose(write.astype(F32)).astype(BF16)

        def group_body(j, inner):
            lanes = [pl.ds(pl.multiple_of(j * (GROUP * 128) + g * 128, 128), 128) for g in range(GROUP)]
            pairs = [j * GROUP + g for g in range(GROUP)]
            every = range(GROUP)
            low = lax.broadcasted_iota(I32, (CHUNK, 128), 1) < 64
            lane = lax.broadcasted_iota(I32, (1, 128), 1)
            x = [xbuf[pl.ds(r0, CHUNK + 16), lanes[g]].astype(F32) for g in every]
            state = [st_buf[:, lanes[g]] for g in every]
            both = [nn(cum3[...], pick_heads(3, pairs[g])) for g in every]
            dte = [nn(dt2[...], pick_lanes(2, pairs[g])) for g in every]
            carried = [nn(read_buf[pl.ds(r0, CHUNK), :], state[g].astype(BF16)) for g in every]
            value = [conv_tile(x[g], conv_w[:, lanes[g]], conv_b[0:1, lanes[g]], CHUNK).astype(F32) for g in every]
            ys, states = [], []
            for g in every:
                sc = sc_buf[...]
                c1, c2 = both[g][:, 0:128], both[g][:, 128:256]
                w1 = sc * jnp.exp2(jnp.minimum(c1 - cumt[pl.ds(2 * pairs[g], 1), :], 0.0))
                w2 = sc * jnp.exp2(jnp.minimum(c2 - cumt[pl.ds(2 * pairs[g] + 1, 1), :], 0.0))
                cp = jnp.where(low, c1, c2)
                vd = value[g] * dte[g]
                zero = jnp.zeros_like(vd)
                rhs = jnp.concatenate([jnp.where(low, vd, zero), jnp.where(low, zero, vd)], axis=0).astype(BF16)
                lhs = jnp.concatenate([w1.astype(BF16), w2.astype(BF16)], axis=1)
                last = cp[CHUNK - 1 : CHUNK, :]
                scaled = (jnp.exp2(last - cp) * vd).astype(BF16)
                skip_lane = jnp.where(lane < 64, skip[2 * pairs[g]], skip[2 * pairs[g] + 1])
                ys.append(nn(lhs, rhs) + carried[g] * jnp.exp2(cp) + skip_lane * value[g])
                states.append(jnp.exp2(last) * state[g] + nn(wt_buf[...], scaled))
            for g in every:
                y_buf[pl.ds(r0, CHUNK), lanes[g]] = ys[g].astype(BF16)
                st_buf[:, lanes[g]] = states[g]
            return inner

        lax.fori_loop(0, PAIRS // GROUP, group_body, 0)
        return carry

    lax.fori_loop(0, CHUNKS, chunk_body, 0)

    cols = lax.broadcasted_iota(I32, (16, SPAN), 1)
    rows = lax.broadcasted_iota(I32, (16, SPAN), 0)
    want = length - 3 - my * SPAN
    sel_in = jnp.where((cols == want + rows) & (rows < 3), 1.0, 0.0).astype(BF16)
    sel_st = jnp.where((cols == want + rows - 3) & (rows >= 3) & (rows < 6), 1.0, 0.0).astype(BF16)
    small3[0:16, :] = jnp.zeros((16, 192), BF16)
    lst = nn(sel_st, xsbuf[pl.ds(16, SPAN), :])

    def lend_body(i, carry):
        lanes = pl.ds(pl.multiple_of(i * 256, 256), 256)
        to = pl.ds(pl.multiple_of((i % 4) * 256, 256), 256)
        lsend[i // 4, pl.ds(0, 128), to] = st_buf[:, lanes].astype(BF16)
        first = jnp.where(i % 4 == 0, 1.0, 0.0)
        lsend[i // 4, pl.ds(128, 16), to] = (nn(sel_in, xbuf[pl.ds(16, SPAN), lanes]) + first * lst).astype(BF16)
        return carry

    lax.fori_loop(0, INNER // 256, lend_body, 0)
    tbuf[my] = base_buf[...]
    lrecv[my] = lsend[my]
    lends = []
    for r in range(1, 4):
        dev = (me, (my + r) % 4)
        lends.append(send(lsend.at[(my + r) % 4], lrecv.at[my], lend_send.at[r], lend_recv.at[r], dev))
        lends.append(send(tbuf.at[my], tbuf.at[my], lend_send.at[4 + r], lend_recv.at[4 + r], dev))

    for cp in rtags:
        cp.wait()
    tag_loads = [
        pltpu.make_async_copy(rtag_a, rtag_as, in_sem.at[3]),
        pltpu.make_async_copy(rtag_b, rtag_bs, in_sem.at[4]),
    ]
    for cp in tag_loads:
        cp.start()
    for d in (1, 3, 2):
        phase_a[d].wait()
        phase_b[d].wait()
    for cp in tag_loads:
        cp.wait()

    def swapped(first, p):
        if p == 1:
            return jnp.where(first >= 2, first, 1)
        return jnp.where(first == p, 1, p)

    for p in (1, 2, 3):
        for e in range(8):
            ta, tb = targets(e)
            first_a, first_b = jnp.int32(0), jnp.int32(0)
            for q in (1, 2, 3):
                first_a = first_a + jnp.where(rtag_as[(mx + 4 - q) % 4, ta, 0, 0] == 1, q, 0)
                first_b = first_b + jnp.where(rtag_bs[(mz + 4 - q) % 4, tb, 0, 0] == 1, q, 0)
            block_a = rel_a[(mx + 4 - swapped(first_a, p)) % 4, ta]
            block_b = rel_b[(mz + 4 - swapped(first_b, p)) % 4, tb]
            if e == 0:
                row_a(p)[...] = block_a
                row_b(p)[...] = block_b
            else:
                sbuf_a[p, e] = block_a
                sbuf_b[p, e] = block_b
                forward(p, e, sbuf_a.at[p, e], sbuf_b.at[p, e])

    for cp in tag_copies:
        cp.wait()
    tag_load = pltpu.make_async_copy(tagbuf, tag_s, in_sem.at[5])
    tag_load.start()
    tag_load.wait()

    def source_of(j):
        acc = jnp.int32(0)
        for s in range(32):
            acc = acc + jnp.where(tag_s[s, 0, 0] == j + 1, s, 0)
        return acc

    def split_source(src):
        xs, zs, cs = src // 8, (src // 2) % 4, src % 2
        return (mx + 4 - xs) % 4, zs * 2 + cs, (mz + 4 - zs) % 4, xs * 2 + cs

    hops0_a, relay0_a, hops0_b, relay0_b = split_source(source_of(0))
    loc0_a = jnp.where(hops0_a > 0, 8, 0) + relay0_a
    loc0_b = jnp.where(hops0_b > 0, 8, 0) + relay0_b

    def rank(hops, relay, hops0, relay0):
        moved_up = jnp.where(hops == hops0, 1, jnp.where(hops == 1, hops0, hops))
        place_in = jnp.where((relay == relay0) & (hops0 >= 2) & (hops > 0), moved_up, hops)
        return place_in * 8 + relay

    def places(j):
        hops_a, relay_a, hops_b, relay_b = split_source(source_of(j))
        return rank(hops_a, relay_a, hops0_a, relay0_a), rank(hops_b, relay_b, hops0_b, relay0_b)

    def fetch(near, far, loc):
        return jnp.where(loc < 16, near[jnp.minimum(loc, 15)], far[jnp.maximum(loc - 16, 0)])

    for cp in firsts:
        cp.wait()
    own_first = [
        pltpu.make_async_copy(xin.at[pl.ds(0, 16)], ffin.at[my], in_sem.at[6]),
        pltpu.make_async_copy(xst.at[pl.ds(0, 16)], ffst.at[my], in_sem.at[7]),
    ]
    for cp in own_first:
        cp.start()
    ffdt[my] = step[pl.ds(0, 16), :]
    for cp in own_first:
        cp.wait()
    for cp in lends:
        cp.wait()

    for p in (0, 1):
        for e in range(1, 8):
            second[p, e, 0].wait()
            second[p, e, 1].wait()

    wtile[my] = near_b[loc0_b, pl.ds(512, 16), :]
    wins = []
    for r in range(1, 4):
        wins.append(send(wtile.at[my], wtile.at[my], win_send.at[r], win_recv.at[r], (me, (my + r) % 4)))

    posf = lax.broadcasted_iota(I32, (16, HEADS), 0)
    livef = ((posf < length) & (posf < 3)).astype(F32)
    dtf0 = softplus(ffdt[0].astype(F32) + step_b[0:1, :]) * livef
    rate0 = dtf0 * (-LOG2E * jnp.exp(decay[0:1, :]))
    c0 = rate0[0:1]
    c1 = c0 + rate0[1:2]
    c2 = c1 + rate0[2:3]
    cumf = jnp.where(posf == 0, c0, jnp.where(posf == 1, c1, c2))
    totals = jnp.where(posf == 0, tbuf[0][0:1, 0:HEADS], jnp.where(
        posf == 1, tbuf[1][0:1, 0:HEADS], jnp.where(posf == 2, tbuf[2][0:1, 0:HEADS], tbuf[3][0:1, 0:HEADS])))
    small3[0:16, :] = jnp.concatenate(split3(cumf), axis=1)
    small3[16:32, :] = jnp.concatenate(split3(dtf0), axis=1)
    small3[32:48, :] = jnp.concatenate(split3(totals), axis=1)

    for cp in wins:
        cp.wait()
    w_low = wtile[0].astype(F32) + wtile[1].astype(F32)
    w_high = wtile[2].astype(F32) + wtile[3].astype(F32)
    e_st = jnp.concatenate([jnp.concatenate([w_low, w_high], axis=1), ffst[0].astype(F32)], axis=0)
    mixed0 = conv_tile(e_st, conv_w[:, INNER : INNER + 256], conv_b[0:1, INNER : INNER + 256], 16)
    write0, read0 = mixed0[:, 0:128], mixed0[:, 128:256]
    read0_buf[...] = read0
    sc0_buf[...] = nt(read0, write0)
    w0t[...] = jnp.transpose(
        jnp.concatenate([write0.astype(F32), jnp.zeros((112, 128), F32)], axis=0)).astype(BF16)

    row16 = lax.broadcasted_iota(I32, (16, 128), 0)
    lane1 = lax.broadcasted_iota(I32, (1, 128), 1)
    for q in range(8):
        i = my * 8 + q
        lanes = pl.ds(pl.multiple_of(my * 1024 + q * 128, 128), 128)
        own = pl.ds(q * 128, 128)
        if q < 4:
            s0 = near_a[loc0_a, pl.ds(q * 128, 128), :]
        else:
            s0 = near_b[loc0_b, pl.ds((q - 4) * 128, 128), :]
        s0t = jnp.transpose(s0.astype(F32))
        wa = near_a[loc0_a, pl.ds(512, 16), :].astype(F32)
        wb = near_b[loc0_b, pl.ds(512, 16), :].astype(F32)
        wq = jnp.where(row16 == 13, wa[q : q + 1], jnp.where(row16 == 14, wa[8 + q : 9 + q], wb[q : q + 1]))
        x0 = jnp.concatenate([wq, ffin[0, :, lanes].astype(F32)], axis=0)
        small = nn(small3[...], pick_lanes(3, i))
        cf, dtf, totl = small[0:16], small[16:32], small[32:48]
        v0 = conv_tile(x0, conv_w[:, lanes], conv_b[0:1, lanes], 16).astype(F32)
        vd = v0 * dtf
        scaled = jnp.concatenate([jnp.exp2(cf[2:3] - cf) * vd, jnp.zeros((112, 128), F32)], axis=0).astype(BF16)
        carry = jnp.exp2(cf[2:3]) * s0t + nn(w0t[...], scaled)
        y0 = nt(read0_buf[...], s0) * jnp.exp2(cf)
        y0 = y0 + jnp.where(lane1 < 64, skip[2 * i], skip[2 * i + 1]) * v0
        for s in range(3):
            term = sc0_buf[:, s : s + 1] * jnp.exp2(jnp.minimum(cf - cf[s : s + 1], 0.0)) * vd[s : s + 1]
            y0 = y0 + jnp.where(row16 >= s, term, 0.0)
        kept = jnp.zeros((16, 128), F32)
        for c in range(4):
            ssend[c, pl.ds(0, 128), own] = carry.astype(BF16)
            ssend[c, pl.ds(128, 16), own] = y0.astype(BF16)
            carry = jnp.exp2(totl[c : c + 1]) * carry + lrecv[c, pl.ds(0, 128), own].astype(F32)
            kept = kept + lrecv[c, pl.ds(128, 16), own].astype(F32)
        fin_buf[pl.ds(q * 128, 128), :] = jnp.transpose(carry)
        for r in range(3):
            wstage[0, pl.ds(r * 8 + q, 1), :] = kept[r : r + 1]
        if q < 2:
            wstage[1 + q, pl.ds(0, 16), :] = kept

    sins = []
    for r in range(1, 4):
        other = (my + r) % 4
        sins.append(send(ssend.at[other], srecv.at[my], s0_send.at[r], s0_recv.at[r], (me, other)))
    srecv[my] = ssend[my]

    outs = []

    def put_out(src, dst, i):
        cp = pltpu.make_async_copy(src, dst, out_sem.at[i])
        cp.start()
        outs.append(cp)

    put_out(fin_buf, fin_out, 30)
    gate_load.wait()
    for cp in sins:
        cp.wait()

    @pl.when(my == 0)
    def _():
        rowc = lax.broadcasted_iota(I32, (16, HEADS), 0)
        cum_buf[pl.ds(0, 16), :] = jnp.where(rowc < 3, -1.0e6, cum_buf[pl.ds(0, 16), :])

        def patch(i, carry):
            lanes = pl.ds(pl.multiple_of(i * 256, 256), 256)
            new = srecv[i // 4, pl.ds(128, 16), pl.ds(pl.multiple_of((i % 4) * 256, 256), 256)].astype(F32)
            old = y_buf[pl.ds(0, 16), lanes].astype(F32)
            rowy = lax.broadcasted_iota(I32, (16, 256), 0)
            y_buf[pl.ds(0, 16), lanes] = jnp.where(rowy < 3, new, old).astype(BF16)
            return carry

        lax.fori_loop(0, INNER // 256, patch, 0)

    def tail_body(k, carry):
        r0 = pl.multiple_of(k * CHUNK, CHUNK)
        cum3[...] = jnp.concatenate(split3(cum_buf[pl.ds(r0, CHUNK), :]), axis=1)
        rowpos = my * SPAN + r0 + lax.broadcasted_iota(I32, (CHUNK, 128), 0)

        def group_body(j, total):
            lanes = [pl.ds(pl.multiple_of(j * 256 + g * 128, 128), 128) for g in range(2)]
            owner = j // 4
            valid = (rowpos < length).astype(F32)
            read = read_buf[pl.ds(r0, CHUNK), :]
            own = [pl.ds(pl.multiple_of((j % 4) * 256 + g * 128, 128), 128) for g in range(2)]
            ce = [nn(cum3[...], pick_lanes(3, 2 * j + g)) for g in range(2)]
            part = [nn(read, srecv[owner, pl.ds(0, 128), own[g]]) for g in range(2)]
            old = [y_buf[pl.ds(r0, CHUNK), lanes[g]].astype(F32) for g in range(2)]
            gates = [silu(gbuf[pl.ds(r0, CHUNK), lanes[g]].astype(F32)) for g in range(2)]
            new = []
            for g in range(2):
                y = (old[g] + jnp.exp2(ce[g]) * part[g]) * valid
                new.append(y.astype(BF16).astype(F32) * gates[g])
            for g in range(2):
                st_buf[:, lanes[g]] = new[g]
                total = total + new[g] * new[g]
            return total

        total = lax.fori_loop(0, PAIRS // 2, group_body, jnp.zeros((CHUNK, 128), F32))
        sc_buf[...] = jnp.broadcast_to(
            lax.rsqrt(jnp.sum(total, axis=1, keepdims=True) * (1.0 / INNER) + EPSILON), (CHUNK, CHUNK))

        def norm_body(i, inner):
            lanes = pl.ds(pl.multiple_of(i * 128, 128), 128)
            y_buf[pl.ds(r0, CHUNK), lanes] = (st_buf[:, lanes] * sc_buf[...] * norm_w[0:1, lanes]).astype(BF16)
            return inner

        lax.fori_loop(0, PAIRS, norm_body, 0)
        return carry

    lax.fori_loop(0, CHUNKS, tail_body, 0)
    put_out(y_buf, mix, 31)

    spots = [places(j) for j in range(SLOTS)]
    for p in (2, 3):
        for e in range(1, 8):
            second[p, e, 0].wait()
            second[p, e, 1].wait()
    for j in range(1, SLOTS):
        loc_a, loc_b = spots[j]
        sbuf_a[j // 8, j % 8] = fetch(near_a, far_a, loc_a)
        sbuf_b[j // 8, j % 8] = fetch(near_b, far_b, loc_b)
        put_out(sbuf_a.at[j // 8, j % 8, pl.ds(0, 512)], moved.at[j, pl.ds(0, 512)], 2 * j)
        put_out(sbuf_b.at[j // 8, j % 8, pl.ds(0, 512)], moved.at[j, pl.ds(512, 512)], 2 * j + 1)
        wstage[2 + j, pl.ds(0, 16), :] = sbuf_a[j // 8, j % 8, pl.ds(512, 16), :].astype(F32)
        wstage[2 + j, pl.ds(16, 16), :] = sbuf_b[j // 8, j % 8, pl.ds(512, 16), :].astype(F32)
    put_out(wstage, wout, 0)
    for cp in outs:
        cp.wait()


def exchange(meta, lens, skip, tags, tags_b, pool, win, xin, xst, gate, step, conv_w, conv_b, step_b, decay, norm_w):
    dma = pltpu.SemaphoreType.DMA
    shape = jax.ShapeDtypeStruct
    out_shape = (
        shape((SLOTS, 1024, 128), BF16),
        shape((SLOTS + 2, 32, 128), F32),
        shape((1024, 128), F32),
        shape((SPAN, INNER), BF16),
    )
    scratch = [
        pltpu.VMEM((SLOTS, 1024, 128), F32),
        pltpu.VMEM((4, 8, HALF, 128), BF16),
        pltpu.VMEM((4, 8, HALF, 128), BF16),
        pltpu.VMEM((4, 8, HALF, 128), BF16),
        pltpu.VMEM((4, 8, HALF, 128), BF16),
        pltpu.VMEM((16, HALF, 128), BF16),
        pltpu.VMEM((16, HALF, 128), BF16),
        pltpu.VMEM((16, HALF, 128), BF16),
        pltpu.VMEM((16, HALF, 128), BF16),
        pltpu.VMEM((SPAN + 16, INNER), BF16),
        pltpu.VMEM((SPAN + 16, 256), BF16),
        pltpu.VMEM((SPAN, INNER), BF16),
        pltpu.VMEM((SPAN, INNER), BF16),
        pltpu.VMEM((SPAN, 128), BF16),
        pltpu.VMEM((SPAN, HEADS), F32),
        pltpu.VMEM((128, INNER), F32),
        pltpu.VMEM((4, 144, 1024), BF16),
        pltpu.VMEM((4, 144, 1024), BF16),
        pltpu.VMEM((4, 144, 1024), BF16),
        pltpu.VMEM((4, 144, 1024), BF16),
        pltpu.VMEM((4, 8, 128), F32),
        pltpu.VMEM((32, 1, 128), I32),
        pltpu.VMEM((4, 8, 1, 128), I32),
        pltpu.VMEM((4, 8, 1, 128), I32),
        pltpu.SMEM((32, 1, 128), I32),
        pltpu.SMEM((4, 8, 1, 128), I32),
        pltpu.SMEM((4, 8, 1, 128), I32),
        pltpu.VMEM((CHUNK, 192), BF16),
        pltpu.VMEM((HEADS, CHUNK), F32),
        pltpu.VMEM((CHUNK, 128), BF16),
        pltpu.VMEM((CHUNK, CHUNK), F32),
        pltpu.VMEM((CHUNK, CHUNK), BF16),
        pltpu.VMEM((8, 128), F32),
        pltpu.VMEM((4, 16, 128), BF16),
        pltpu.VMEM((1024, 128), F32),
        pltpu.VMEM((SLOTS + 2, 32, 128), F32),
        pltpu.VMEM((4, 16, INNER), BF16),
        pltpu.VMEM((4, 16, 256), BF16),
        pltpu.VMEM((4, 16, HEADS), BF16),
        pltpu.VMEM((48, 192), BF16),
        pltpu.VMEM((128, 128), BF16),
        pltpu.VMEM((16, 128), BF16),
        pltpu.VMEM((16, 16), F32),
        dma((SLOTS,)), dma((8,)), dma((32,)),
        dma((8,)), dma((8,)), dma((64,)), dma((64,)), dma((32,)), dma((32,)), dma((8,)), dma((8,)),
        dma((2,)), dma((2,)), dma((8,)), dma((8,)), dma((4,)), dma((4,)), dma((4,)), dma((4,)), dma((12,)), dma((12,)),
    ]
    return pl.pallas_call(
        exchange_kernel,
        out_shape=out_shape,
        in_specs=[SM, SM, SM, VM, VM, ANY, VM, ANY, ANY, ANY, VM, VM, VM, VM, VM, VM],
        out_specs=[ANY] * len(out_shape),
        scratch_shapes=scratch,
        compiler_params=pltpu.CompilerParams(
            collective_id=1, has_side_effects=True, vmem_limit_bytes=67043328
        ),
        name="exchange",
    )(meta, lens, skip, tags, tags_b, pool, win, xin, xst, gate, step, conv_w, conv_b, step_b, decay, norm_w)


PLACE_ROWS = SLOTS * 256


def place_kernel(moved, fin, states):
    states[...] = moved[...].astype(F32)

    @pl.when(pl.program_id(0) == 0)
    def _():
        states[pl.ds(0, 1024), :] = fin[...]


def place(moved, fin):
    return pl.pallas_call(
        place_kernel,
        grid=(4,),
        out_shape=jax.ShapeDtypeStruct((SLOTS * 1024, 128), F32),
        in_specs=[pl.BlockSpec((PLACE_ROWS, 128), lambda j: (j, 0)), VM],
        out_specs=pl.BlockSpec((PLACE_ROWS, 128), lambda j: (j, 0)),
        name="place",
    )(moved, fin)


def on_device(
    pool_states, inner_window, state_window, move_plan, active_mask, inputs_inner, inputs_state, gate_rows,
    step_raw, lengths, conv_weight, conv_bias, step_bias, decay_log, skip_weight, norm_weight,
):
    my = lax.axis_index("seq")
    match = (move_plan[None, :, 0] == jnp.arange(32, dtype=I32)[:, None]).astype(I32)
    slot = jnp.sum(match * jnp.arange(SLOTS, dtype=I32)[None, :], axis=1)
    keep = jnp.sum(match * active_mask[None, :], axis=1)
    tag = jnp.sum(match * (move_plan[None, :, 1] + 1), axis=1)
    meta = jnp.stack([slot, keep], axis=1)
    tags = jnp.broadcast_to(tag[:, None, None], (32, 1, 128))
    tag_b = jnp.moveaxis(tag.reshape(4, 4, 2), 1, 0).reshape(4, 8)
    tags_b = jnp.broadcast_to(tag_b[:, :, None, None], (4, 8, 1, 128))
    blank = jnp.zeros((SLOTS, 3, 64), BF16)
    odd = (my % 2) == 1
    lane_window = jnp.concatenate(
        [jnp.where(odd, blank, state_window), jnp.where(odd, state_window, blank)], axis=2)
    win = jnp.concatenate(
        [inner_window.reshape(SLOTS, 24, 128), jnp.zeros((SLOTS, 5, 128), BF16), lane_window], axis=1)
    moved, wout, fin, mix = exchange(
        meta, lengths, skip_weight, tags, tags_b, pool_states.reshape(SLOTS, 1024, 128), win,
        inputs_inner[0], inputs_state[0], gate_rows[0], step_raw[0],
        conv_weight, conv_bias[None], step_bias[None], decay_log[None], norm_weight[None],
    )
    new_states = place(moved.reshape(SLOTS * 1024, 128), fin).reshape(SLOTS, 16, 64, 128)
    kept_st = jnp.concatenate([wout[1, 3:6], wout[2, 3:6]], axis=1)
    kept_st = lax.dynamic_slice_in_dim(kept_st, my * 64, 64, 1)[None]
    rows = jnp.concatenate([wout[0:1], wout[3:]], axis=0)
    new_in = rows[:, 0:24].reshape(SLOTS, 3, 1024).astype(BF16)
    moved_st = wout[3:, 29:32]
    moved_st = jnp.where(odd, moved_st[:, :, 64:], moved_st[:, :, :64])
    new_st = jnp.concatenate([kept_st, moved_st], axis=0).astype(BF16)
    return (new_states, new_in, new_st, mix[None])


def solution(mesh):
    return jax.shard_map(
        on_device,
        mesh=mesh,
        in_specs=(
            P("req", "seq", None, None), P("req", None, "seq"), P("req", None, "seq"), P("req", None), P("req"),
            P("req", "seq", None), P("req", "seq", None), P("req", "seq", None), P("req", "seq", None), P("req"),
            P(), P(), P(), P(), P(), P(),
        ),
        out_specs=(
            P("req", "seq", None, None), P("req", None, "seq"), P("req", None, "seq"), P("req", "seq", None),
        ),
        check_vma=False,
    )
```

```python
import functools

import jax
import jax.numpy as jnp
from jax import lax
from jax.experimental import pallas as pl
from jax.experimental.pallas import tpu as pltpu
from jax.sharding import PartitionSpec as P

MESH = pl.DeviceIdType.MESH
ANY = pl.BlockSpec(memory_space=pl.ANY)
VM = pl.BlockSpec(memory_space=pltpu.VMEM)
SM = pl.BlockSpec(memory_space=pltpu.SMEM)
F32 = jnp.float32
BF16 = jnp.bfloat16
I32 = jnp.int32

SLOTS = 13
HEADS = 64
INNER = 4096
SPAN = 512
CHUNK = 128
CHUNKS = SPAN // CHUNK
PAIRS = HEADS // 2
HALF = 528
GROUP = 2
LOG2E = 1.4426950408889634
EPSILON = 1e-05


def nn(a, b):
    return lax.dot_general(a, b, (((1,), (0,)), ((), ())), preferred_element_type=F32)


def nt(a, b):
    return lax.dot_general(a, b, (((1,), (1,)), ((), ())), preferred_element_type=F32)


def split3(v):
    hi = v.astype(BF16)
    rest = v - hi.astype(F32)
    mid = rest.astype(BF16)
    lo = (rest - mid.astype(F32)).astype(BF16)
    return hi, mid, lo


def silu(v):
    half = 0.5 * v
    return half + half * jnp.tanh(half)


def softplus(v):
    u = jnp.exp(-jnp.abs(v))
    series = u * (1.0 - u * (0.5 - u * (1.0 / 3.0 - u * (0.25 - u * 0.2))))
    return jnp.maximum(v, 0.0) + jnp.where(u < 0.02, series, jnp.log(1.0 + u))


def pick_lanes(copies, pair):
    row = lax.broadcasted_iota(I32, (64, 128), 0)
    lane = lax.broadcasted_iota(I32, (64, 128), 1)
    one = jnp.where(row == 2 * pair + (lane >= 64).astype(I32), 1.0, 0.0).astype(BF16)
    return jnp.concatenate([one] * copies, axis=0)


def pick_heads(copies, pair):
    row = lax.broadcasted_iota(I32, (64, 256), 0)
    lane = lax.broadcasted_iota(I32, (64, 256), 1)
    one = jnp.where(row == 2 * pair + (lane >= 128).astype(I32), 1.0, 0.0).astype(BF16)
    return jnp.concatenate([one] * copies, axis=0)


def conv_tile(x, taps, bias, rows):
    acc = bias + taps[3:4] * x[16 : 16 + rows]
    for k in range(3):
        acc = acc + taps[k : k + 1] * x[13 + k : 13 + k + rows]
    return silu(acc).astype(BF16)


def exchange_kernel(
    plan, mask, lens, skip, pool, iw, sw, xin, xst, gate, step, conv_w, conv_b, step_b, decay,
    moved, wout, fin_out, mix, scale_out,
    meta, tags, tags_b, win, tot_buf,
    stage, sbuf_a, sbuf_b, rel_a, rel_b, near_a, near_b, far_a, far_b, xbuf, xsbuf, gbuf, y_buf, read_buf, cum_buf, st_buf,
    lsend, lrecv, ssend, srecv, tbuf, tagbuf, rtag_a, rtag_b, tag_s, rtag_as, rtag_bs,
    cum3, cumt, dt2, sc_buf, wt_buf, base_buf, wtile, fin_buf, wstage, ffin, ffst, ffdt,
    small3, w0t, read0_buf, sc0_buf,
    pool_sem, in_sem, out_sem, one_send, one_recv, two_send, two_recv, tag_send, tag_recv, rt_send, rt_recv,
    halo_send, halo_recv, lend_send, lend_recv, win_send, win_recv, s0_send, s0_recv, f_send, f_recv,
):
    me = lax.axis_index("req")
    my = lax.axis_index("seq")
    mx, mz, mc = me // 8, (me // 2) % 4, me % 2

    def at(dx, dz, dc):
        return ((mx + dx) % 4) * 8 + ((mz + dz) % 4) * 2 + (mc + dc) % 2

    loads = []
    for k in range(SLOTS):
        cp = pltpu.make_async_copy(pool.at[k], stage.at[k], pool_sem.at[k])
        cp.start()
        loads.append(cp)
    ins = [
        pltpu.make_async_copy(xin, xbuf.at[pl.ds(16, SPAN)], in_sem.at[0]),
        pltpu.make_async_copy(xst, xsbuf.at[pl.ds(16, SPAN)], in_sem.at[1]),
    ]
    for cp in ins:
        cp.start()
    gate_load = pltpu.make_async_copy(gate, gbuf, in_sem.at[2])
    gate_load.start()

    barrier = pltpu.get_barrier_semaphore()
    for r in range(1, 32):
        peer = at(r // 8, (r // 2) % 4, r % 2)
        pl.semaphore_signal(barrier, inc=1, device_id=(peer, my), device_id_type=MESH)
    for r in range(1, 4):
        pl.semaphore_signal(barrier, inc=1, device_id=(me, (my + r) % 4), device_id_type=MESH)

    def table_body(d, carry):
        slot, keep, tag = jnp.int32(0), jnp.int32(0), jnp.int32(0)
        for k in range(SLOTS):
            hit = plan[k, 0] == d
            slot = jnp.where(hit, k, slot)
            keep = jnp.where(hit, mask[k], keep)
            tag = jnp.where(hit, plan[k, 1] + 1, tag)
        meta[0, d] = slot
        meta[1, d] = keep
        row = jnp.full((1, 128), tag, I32)
        tags[d] = row
        tags_b[(d // 2) % 4, (d // 8) * 2 + d % 2] = row
        return carry

    lax.fori_loop(0, 32, table_body, 0)

    def window_body(k, carry):
        rows3 = iw[k].astype(F32)
        for i in range(3):
            for q in range(8):
                win[k, pl.ds(i * 8 + q, 1), :] = rows3[i : i + 1, q * 128 : (q + 1) * 128]
        win[k, pl.ds(24, 8), :] = jnp.zeros((8, 128), F32)
        own = sw[k].astype(F32)
        blank = jnp.zeros((3, 64), F32)
        win[k, pl.ds(29, 3), :] = jnp.where(
            my % 2 == 1, jnp.concatenate([blank, own], axis=1), jnp.concatenate([own, blank], axis=1))
        return carry

    lax.fori_loop(0, SLOTS, window_body, 0)
    pl.semaphore_wait(barrier, 34)

    def send(src, dst, ssem, rsem, dev):
        cp = pltpu.make_async_remote_copy(
            src_ref=src, dst_ref=dst, send_sem=ssem, recv_sem=rsem, device_id=dev, device_id_type=MESH
        )
        cp.start()
        return cp

    halo = [
        send(xin.at[pl.ds(SPAN - 16, 16)], xbuf.at[pl.ds(0, 16)], halo_send.at[0], halo_recv.at[0], (me, (my + 1) % 4)),
        send(xst.at[pl.ds(SPAN - 16, 16)], xsbuf.at[pl.ds(0, 16)], halo_send.at[1], halo_recv.at[1], (me, (my + 1) % 4)),
    ]
    firsts = []
    for r in range(1, 4):
        dev = (me, (my + r) % 4)
        firsts.append(send(xin.at[pl.ds(0, 16)], ffin.at[my], f_send.at[r], f_recv.at[r], dev))
        firsts.append(send(xst.at[pl.ds(0, 16)], ffst.at[my], f_send.at[4 + r], f_recv.at[4 + r], dev))
        firsts.append(send(step.at[pl.ds(0, 16)], ffdt.at[my], f_send.at[8 + r], f_recv.at[8 + r], dev))

    for cp in loads:
        cp.wait()

    def fill(ref, lead, q, dest, half):
        slot = meta[0, dest]
        keep = meta[1, dest].astype(F32)
        ref[lead, q, pl.ds(0, 512), :] = (stage[slot, pl.ds(512 * half, 512), :] * keep).astype(BF16)
        ref[lead, q, pl.ds(512, 16), :] = (win[slot, pl.ds(16 * half, 16), :] * keep).astype(BF16)

    def fill_a(ref, lead, xd):
        def one(q, carry):
            fill(ref, lead, q, xd * 8 + q, 0)
            return carry

        lax.fori_loop(0, 8, one, 0)

    def fill_b(ref, lead, zd):
        def one(q, carry):
            fill(ref, lead, q, (q // 2) * 8 + zd * 2 + q % 2, 1)
            return carry

        lax.fori_loop(0, 8, one, 0)

    phase_a, phase_b, rtags = {}, {}, []
    for d in (2, 1, 3):
        xd, zd = (mx + d) % 4, (mz + d) % 4
        dev_a, dev_b = (at(d, 0, 0), my), (at(0, d, 0), my)
        fill_a(sbuf_a, xd, xd)
        phase_a[d] = send(sbuf_a.at[xd], rel_a.at[mx], one_send.at[d], one_recv.at[d], dev_a)
        fill_b(sbuf_b, zd, zd)
        phase_b[d] = send(sbuf_b.at[zd], rel_b.at[mz], one_send.at[4 + d], one_recv.at[4 + d], dev_b)
        rtags.append(send(tags.at[pl.ds(xd * 8, 8)], rtag_a.at[mx], rt_send.at[d], rt_recv.at[d], dev_a))
        rtags.append(send(tags_b.at[zd], rtag_b.at[mz], rt_send.at[4 + d], rt_recv.at[4 + d], dev_b))
    fill_a(rel_a, mx, mx)
    fill_b(rel_b, mz, mz)

    second = {}

    def row_a(p):
        return (near_a if p < 2 else far_a).at[(p % 2) * 8 + mz * 2 + mc]

    def row_b(p):
        return (near_b if p < 2 else far_b).at[(p % 2) * 8 + mx * 2 + mc]

    def forward(p, e, src_a, src_b):
        de, dc = e // 2, e % 2
        sem = p * 8 + e
        second[p, e, 0] = send(
            src_a, row_a(p), two_send.at[sem], two_recv.at[sem], (at(0, de, dc), my))
        second[p, e, 1] = send(
            src_b, row_b(p), two_send.at[32 + sem], two_recv.at[32 + sem], (at(de, 0, dc), my))

    def targets(e):
        de, dc = e // 2, e % 2
        ct = (mc + dc) % 2
        return ((mz + de) % 4) * 2 + ct, ((mx + de) % 4) * 2 + ct

    for e in range(1, 8):
        ta, tb = targets(e)
        forward(0, e, rel_a.at[mx, ta], rel_b.at[mz, tb])
    row_a(0)[...] = rel_a[mx, mz * 2 + mc]
    row_b(0)[...] = rel_b[mz, mx * 2 + mc]

    tag_copies = []
    for r in range(1, 32):
        peer = at(r // 8, (r // 2) % 4, r % 2)
        tag_copies.append(
            send(tags.at[peer], tagbuf.at[me], tag_send.at[r], tag_recv.at[r], (peer, my))
        )
    tagbuf[me] = tags[me]

    for cp in ins:
        cp.wait()
    for cp in halo:
        cp.wait()

    @pl.when(my == 0)
    def _():
        xbuf[pl.ds(0, 16), :] = jnp.zeros((16, INNER), BF16)
        xsbuf[pl.ds(0, 16), :] = jnp.zeros((16, 256), BF16)

    st_buf[...] = jnp.zeros_like(st_buf)
    base_buf[...] = jnp.zeros_like(base_buf)
    length = lens[0]

    def chunk_body(k, carry):
        r0 = pl.multiple_of(k * CHUNK, CHUNK)
        pos = my * SPAN + r0 + lax.broadcasted_iota(I32, (CHUNK, HEADS), 0)
        live = ((pos < length) & (pos >= 3)).astype(F32)
        dt = softplus(step[pl.ds(r0, CHUNK), :].astype(F32) + step_b[0:1, :]) * live
        rate = dt * (-LOG2E * jnp.exp(decay[0:1, :]))
        rows = lax.broadcasted_iota(I32, (CHUNK, CHUNK), 0)
        cols = lax.broadcasted_iota(I32, (CHUNK, CHUNK), 1)
        tri = jnp.where(rows >= cols, 1.0, 0.0).astype(BF16)
        hi, mid, lo = split3(rate)
        cum = nn(tri, hi) + nn(tri, mid) + nn(tri, lo)
        cum3[...] = jnp.concatenate(split3(cum), axis=1)
        cumt[...] = jnp.transpose(cum)
        dth = dt.astype(BF16)
        dt2[...] = jnp.concatenate([dth, (dt - dth.astype(F32)).astype(BF16)], axis=1)
        cum_buf[pl.ds(r0, CHUNK), :] = cum + base_buf[0:1, 0:HEADS]
        base_buf[0:1, 0:HEADS] = base_buf[0:1, 0:HEADS] + cum[CHUNK - 1 : CHUNK, :]
        xs_tile = xsbuf[pl.ds(r0, CHUNK + 16), :].astype(F32)
        mixed = conv_tile(xs_tile, conv_w[:, INNER : INNER + 256], conv_b[0:1, INNER : INNER + 256], CHUNK)
        write, read = mixed[:, 0:128], mixed[:, 128:256]
        read_buf[pl.ds(r0, CHUNK), :] = read
        sc_buf[...] = jnp.where(rows >= cols, nt(read, write), 0.0)
        wt_buf[...] = jnp.transpose(write.astype(F32)).astype(BF16)

        def group_body(j, inner):
            lanes = [pl.ds(pl.multiple_of(j * (GROUP * 128) + g * 128, 128), 128) for g in range(GROUP)]
            pairs = [j * GROUP + g for g in range(GROUP)]
            every = range(GROUP)
            low = lax.broadcasted_iota(I32, (CHUNK, 128), 1) < 64
            lane = lax.broadcasted_iota(I32, (1, 128), 1)
            x = [xbuf[pl.ds(r0, CHUNK + 16), lanes[g]].astype(F32) for g in every]
            state = [st_buf[:, lanes[g]] for g in every]
            both = [nn(cum3[...], pick_heads(3, pairs[g])) for g in every]
            dte = [nn(dt2[...], pick_lanes(2, pairs[g])) for g in every]
            carried = [nn(read_buf[pl.ds(r0, CHUNK), :], state[g].astype(BF16)) for g in every]
            value = [conv_tile(x[g], conv_w[:, lanes[g]], conv_b[0:1, lanes[g]], CHUNK).astype(F32) for g in every]
            ys, states = [], []
            for g in every:
                sc = sc_buf[...]
                c1, c2 = both[g][:, 0:128], both[g][:, 128:256]
                w1 = sc * jnp.exp2(jnp.minimum(c1 - cumt[pl.ds(2 * pairs[g], 1), :], 0.0))
                w2 = sc * jnp.exp2(jnp.minimum(c2 - cumt[pl.ds(2 * pairs[g] + 1, 1), :], 0.0))
                cp = jnp.where(low, c1, c2)
                vd = value[g] * dte[g]
                zero = jnp.zeros_like(vd)
                rhs = jnp.concatenate([jnp.where(low, vd, zero), jnp.where(low, zero, vd)], axis=0).astype(BF16)
                lhs = jnp.concatenate([w1.astype(BF16), w2.astype(BF16)], axis=1)
                last = cp[CHUNK - 1 : CHUNK, :]
                scaled = (jnp.exp2(last - cp) * vd).astype(BF16)
                skip_lane = jnp.where(lane < 64, skip[2 * pairs[g]], skip[2 * pairs[g] + 1])
                ys.append(nn(lhs, rhs) + carried[g] * jnp.exp2(cp) + skip_lane * value[g])
                states.append(jnp.exp2(last) * state[g] + nn(wt_buf[...], scaled))
            for g in every:
                y_buf[pl.ds(r0, CHUNK), lanes[g]] = ys[g].astype(BF16)
                st_buf[:, lanes[g]] = states[g]
            return inner

        lax.fori_loop(0, PAIRS // GROUP, group_body, 0)
        return carry

    lax.fori_loop(0, CHUNKS, chunk_body, 0)

    cols = lax.broadcasted_iota(I32, (16, SPAN), 1)
    rows = lax.broadcasted_iota(I32, (16, SPAN), 0)
    want = length - 3 - my * SPAN
    sel_in = jnp.where((cols == want + rows) & (rows < 3), 1.0, 0.0).astype(BF16)
    sel_st = jnp.where((cols == want + rows - 3) & (rows >= 3) & (rows < 6), 1.0, 0.0).astype(BF16)
    small3[0:16, :] = jnp.zeros((16, 192), BF16)
    lst = nn(sel_st, xsbuf[pl.ds(16, SPAN), :])

    def lend_body(i, carry):
        lanes = pl.ds(pl.multiple_of(i * 256, 256), 256)
        to = pl.ds(pl.multiple_of((i % 4) * 256, 256), 256)
        lsend[i // 4, pl.ds(0, 128), to] = st_buf[:, lanes].astype(BF16)
        first = jnp.where(i % 4 == 0, 1.0, 0.0)
        lsend[i // 4, pl.ds(128, 16), to] = (nn(sel_in, xbuf[pl.ds(16, SPAN), lanes]) + first * lst).astype(BF16)
        return carry

    lax.fori_loop(0, INNER // 256, lend_body, 0)
    tbuf[my] = base_buf[...]
    lrecv[my] = lsend[my]
    lends = []
    for r in range(1, 4):
        dev = (me, (my + r) % 4)
        lends.append(send(lsend.at[(my + r) % 4], lrecv.at[my], lend_send.at[r], lend_recv.at[r], dev))
        lends.append(send(tbuf.at[my], tbuf.at[my], lend_send.at[4 + r], lend_recv.at[4 + r], dev))

    @pl.when(my == 0)
    def _():
        rowc = lax.broadcasted_iota(I32, (16, HEADS), 0)
        cum_buf[pl.ds(0, 16), :] = jnp.where(rowc < 3, -1.0e6, cum_buf[pl.ds(0, 16), :])

    gate_load.wait()

    def ready_body(k, carry):
        r0 = pl.multiple_of(k * CHUNK, CHUNK)
        cum3[...] = jnp.concatenate(split3(cum_buf[pl.ds(r0, CHUNK), :]), axis=1)
        rowpos = my * SPAN + r0 + lax.broadcasted_iota(I32, (CHUNK, 128), 0)

        def group_body(j, inner):
            lanes = [pl.ds(pl.multiple_of(j * 256 + g * 128, 128), 128) for g in range(2)]
            valid = (rowpos < length).astype(F32)
            ce = [nn(cum3[...], pick_lanes(3, 2 * j + g)) for g in range(2)]
            gates = [silu(gbuf[pl.ds(r0, CHUNK), lanes[g]].astype(F32)) * valid for g in range(2)]
            for g in range(2):
                xbuf[pl.ds(r0, CHUNK), lanes[g]] = jnp.exp2(ce[g]).astype(BF16)
                gbuf[pl.ds(r0, CHUNK), lanes[g]] = gates[g].astype(BF16)
            return inner

        lax.fori_loop(0, PAIRS // 2, group_body, 0)
        return carry

    lax.fori_loop(0, CHUNKS, ready_body, 0)
    tot_buf[...] = jnp.zeros_like(tot_buf)

    for cp in rtags:
        cp.wait()
    tag_loads = [
        pltpu.make_async_copy(rtag_a, rtag_as, in_sem.at[3]),
        pltpu.make_async_copy(rtag_b, rtag_bs, in_sem.at[4]),
    ]
    for cp in tag_loads:
        cp.start()
    for d in (1, 3, 2):
        phase_a[d].wait()
        phase_b[d].wait()
    for cp in tag_loads:
        cp.wait()

    def swapped(first, p):
        if p == 1:
            return jnp.where(first >= 2, first, 1)
        return jnp.where(first == p, 1, p)

    for p in (1, 2, 3):
        for e in range(8):
            ta, tb = targets(e)
            first_a, first_b = jnp.int32(0), jnp.int32(0)
            for q in (1, 2, 3):
                first_a = jnp.where(rtag_as[(mx + 4 - q) % 4, ta, 0, 0] == 1, q, first_a)
                first_b = jnp.where(rtag_bs[(mz + 4 - q) % 4, tb, 0, 0] == 1, q, first_b)
            block_a = rel_a[(mx + 4 - swapped(first_a, p)) % 4, ta]
            block_b = rel_b[(mz + 4 - swapped(first_b, p)) % 4, tb]
            if e == 0:
                row_a(p)[...] = block_a
                row_b(p)[...] = block_b
            else:
                sbuf_a[p, e] = block_a
                sbuf_b[p, e] = block_b
                forward(p, e, sbuf_a.at[p, e], sbuf_b.at[p, e])

    for cp in tag_copies:
        cp.wait()
    tag_load = pltpu.make_async_copy(tagbuf, tag_s, in_sem.at[5])
    tag_load.start()
    tag_load.wait()

    def source_of(j):
        acc = jnp.int32(0)
        for s in range(32):
            acc = jnp.where(tag_s[s, 0, 0] == j + 1, s, acc)
        return acc

    def split_source(src):
        xs, zs, cs = src // 8, (src // 2) % 4, src % 2
        return (mx + 4 - xs) % 4, zs * 2 + cs, (mz + 4 - zs) % 4, xs * 2 + cs

    hops0_a, relay0_a, hops0_b, relay0_b = split_source(source_of(0))
    loc0_a = jnp.where(hops0_a > 0, 8, 0) + relay0_a
    loc0_b = jnp.where(hops0_b > 0, 8, 0) + relay0_b

    def rank(hops, relay, hops0, relay0):
        moved_up = jnp.where(hops == hops0, 1, jnp.where(hops == 1, hops0, hops))
        place_in = jnp.where((relay == relay0) & (hops0 >= 2) & (hops > 0), moved_up, hops)
        return place_in * 8 + relay

    def places(j):
        hops_a, relay_a, hops_b, relay_b = split_source(source_of(j))
        return rank(hops_a, relay_a, hops0_a, relay0_a), rank(hops_b, relay_b, hops0_b, relay0_b)

    def fetch(near, far, loc):
        return jnp.where(loc < 16, near[jnp.minimum(loc, 15)], far[jnp.maximum(loc - 16, 0)])

    for cp in firsts:
        cp.wait()
    own_first = [
        pltpu.make_async_copy(xin.at[pl.ds(0, 16)], ffin.at[my], in_sem.at[6]),
        pltpu.make_async_copy(xst.at[pl.ds(0, 16)], ffst.at[my], in_sem.at[7]),
    ]
    for cp in own_first:
        cp.start()
    ffdt[my] = step[pl.ds(0, 16), :]
    for cp in own_first:
        cp.wait()
    for cp in lends:
        cp.wait()

    for p in (0, 1):
        for e in range(1, 8):
            second[p, e, 0].wait()
            second[p, e, 1].wait()

    wtile[my] = near_b[loc0_b, pl.ds(512, 16), :]
    wins = []
    for r in range(1, 4):
        wins.append(send(wtile.at[my], wtile.at[my], win_send.at[r], win_recv.at[r], (me, (my + r) % 4)))

    posf = lax.broadcasted_iota(I32, (16, HEADS), 0)
    livef = ((posf < length) & (posf < 3)).astype(F32)
    dtf0 = softplus(ffdt[0].astype(F32) + step_b[0:1, :]) * livef
    rate0 = dtf0 * (-LOG2E * jnp.exp(decay[0:1, :]))
    c0 = rate0[0:1]
    c1 = c0 + rate0[1:2]
    c2 = c1 + rate0[2:3]
    cumf = jnp.where(posf == 0, c0, jnp.where(posf == 1, c1, c2))
    totals = jnp.where(posf == 0, tbuf[0][0:1, 0:HEADS], jnp.where(
        posf == 1, tbuf[1][0:1, 0:HEADS], jnp.where(posf == 2, tbuf[2][0:1, 0:HEADS], tbuf[3][0:1, 0:HEADS])))
    small3[0:16, :] = jnp.concatenate(split3(cumf), axis=1)
    small3[16:32, :] = jnp.concatenate(split3(dtf0), axis=1)
    small3[32:48, :] = jnp.concatenate(split3(totals), axis=1)

    for cp in wins:
        cp.wait()
    w_low = wtile[0].astype(F32) + wtile[1].astype(F32)
    w_high = wtile[2].astype(F32) + wtile[3].astype(F32)
    e_st = jnp.concatenate([jnp.concatenate([w_low, w_high], axis=1), ffst[0].astype(F32)], axis=0)
    mixed0 = conv_tile(e_st, conv_w[:, INNER : INNER + 256], conv_b[0:1, INNER : INNER + 256], 16)
    write0, read0 = mixed0[:, 0:128], mixed0[:, 128:256]
    read0_buf[...] = read0
    sc0_buf[...] = nt(read0, write0)
    w0t[...] = jnp.transpose(
        jnp.concatenate([write0.astype(F32), jnp.zeros((112, 128), F32)], axis=0)).astype(BF16)

    row16 = lax.broadcasted_iota(I32, (16, 128), 0)
    lane1 = lax.broadcasted_iota(I32, (1, 128), 1)
    for q in range(8):
        i = my * 8 + q
        lanes = pl.ds(pl.multiple_of(my * 1024 + q * 128, 128), 128)
        own = pl.ds(q * 128, 128)
        if q < 4:
            s0 = near_a[loc0_a, pl.ds(q * 128, 128), :]
        else:
            s0 = near_b[loc0_b, pl.ds((q - 4) * 128, 128), :]
        s0t = jnp.transpose(s0.astype(F32))
        wa = near_a[loc0_a, pl.ds(512, 16), :].astype(F32)
        wb = near_b[loc0_b, pl.ds(512, 16), :].astype(F32)
        wq = jnp.where(row16 == 13, wa[q : q + 1], jnp.where(row16 == 14, wa[8 + q : 9 + q], wb[q : q + 1]))
        x0 = jnp.concatenate([wq, ffin[0, :, lanes].astype(F32)], axis=0)
        small = nn(small3[...], pick_lanes(3, i))
        cf, dtf, totl = small[0:16], small[16:32], small[32:48]
        v0 = conv_tile(x0, conv_w[:, lanes], conv_b[0:1, lanes], 16).astype(F32)
        vd = v0 * dtf
        scaled = jnp.concatenate([jnp.exp2(cf[2:3] - cf) * vd, jnp.zeros((112, 128), F32)], axis=0).astype(BF16)
        carry = jnp.exp2(cf[2:3]) * s0t + nn(w0t[...], scaled)
        y0 = nt(read0_buf[...], s0) * jnp.exp2(cf)
        y0 = y0 + jnp.where(lane1 < 64, skip[2 * i], skip[2 * i + 1]) * v0
        for s in range(3):
            term = sc0_buf[:, s : s + 1] * jnp.exp2(jnp.minimum(cf - cf[s : s + 1], 0.0)) * vd[s : s + 1]
            y0 = y0 + jnp.where(row16 >= s, term, 0.0)
        kept = jnp.zeros((16, 128), F32)
        for c in range(4):
            ssend[c, pl.ds(0, 128), own] = carry.astype(BF16)
            ssend[c, pl.ds(128, 16), own] = y0.astype(BF16)
            carry = jnp.exp2(totl[c : c + 1]) * carry + lrecv[c, pl.ds(0, 128), own].astype(F32)
            kept = kept + lrecv[c, pl.ds(128, 16), own].astype(F32)
        fin_buf[pl.ds(q * 128, 128), :] = jnp.transpose(carry)
        for r in range(3):
            wstage[0, pl.ds(r * 8 + q, 1), :] = kept[r : r + 1]
        if q < 2:
            wstage[1 + q, pl.ds(0, 16), :] = kept

    sins = []
    for r in range(1, 4):
        other = (my + r) % 4
        sins.append(send(ssend.at[other], srecv.at[my], s0_send.at[r], s0_recv.at[r], (me, other)))
    srecv[my] = ssend[my]

    outs = []

    def put_out(src, dst, i):
        cp = pltpu.make_async_copy(src, dst, out_sem.at[i])
        cp.start()
        outs.append(cp)

    put_out(fin_buf, fin_out, 30)
    def quarter(owner):
        base = owner * 1024

        @pl.when(my == 0)
        def _():
            for j in range(4):
                lanes = pl.ds(pl.multiple_of(base + j * 256, 128), 256)
                new = srecv[owner, pl.ds(128, 16), pl.ds(j * 256, 256)].astype(F32)
                old = y_buf[pl.ds(0, 16), lanes].astype(F32)
                rowy = lax.broadcasted_iota(I32, (16, 256), 0)
                y_buf[pl.ds(0, 16), lanes] = jnp.where(rowy < 3, new, old).astype(BF16)

        def group_body(j, carry):
            lanes = pl.ds(pl.multiple_of(base + j * 256, 128), 256)
            state = srecv[owner, pl.ds(0, 128), pl.ds(pl.multiple_of(j * 256, 256), 256)]
            spans = [pl.ds(r * CHUNK, CHUNK) for r in range(CHUNKS)]
            parts = [nn(read_buf[span, :], state) for span in spans]
            new, squares = [], []
            for span, part in zip(spans, parts):
                y = y_buf[span, lanes].astype(F32) + xbuf[span, lanes].astype(F32) * part
                v = y.astype(BF16).astype(F32) * gbuf[span, lanes].astype(F32)
                new.append(v.astype(BF16))
                squares.append(tot_buf[span, :] + v[:, 0:128] * v[:, 0:128] + v[:, 128:256] * v[:, 128:256])
            for span, v, square in zip(spans, new, squares):
                y_buf[span, lanes] = v
                tot_buf[span, :] = square
            return carry

        lax.fori_loop(0, 4, group_body, 0)

    quarter(my)
    for r in (1, 3, 2):
        sins[r - 1].wait()
        quarter((my + 4 - r) % 4)
    put_out(y_buf, mix, 31)
    tot_buf[...] = jnp.broadcast_to(
        lax.rsqrt(jnp.sum(tot_buf[...], axis=1, keepdims=True) * (1.0 / INNER) + EPSILON), (SPAN, 128))
    put_out(tot_buf, scale_out, 29)

    spots = [places(j) for j in range(SLOTS)]
    for p in (2, 3):
        for e in range(1, 8):
            second[p, e, 0].wait()
            second[p, e, 1].wait()
    for j in range(1, SLOTS):
        loc_a, loc_b = spots[j]
        sbuf_a[j // 8, j % 8] = fetch(near_a, far_a, loc_a)
        sbuf_b[j // 8, j % 8] = fetch(near_b, far_b, loc_b)
        put_out(sbuf_a.at[j // 8, j % 8, pl.ds(0, 512)], moved.at[j, pl.ds(0, 512)], 2 * j)
        put_out(sbuf_b.at[j // 8, j % 8, pl.ds(0, 512)], moved.at[j, pl.ds(512, 512)], 2 * j + 1)
        wstage[2 + j, pl.ds(0, 16), :] = sbuf_a[j // 8, j % 8, pl.ds(512, 16), :].astype(F32)
        wstage[2 + j, pl.ds(16, 16), :] = sbuf_b[j // 8, j % 8, pl.ds(512, 16), :].astype(F32)
    put_out(wstage, wout, 0)
    for cp in outs:
        cp.wait()


def exchange(*operands):
    dma = pltpu.SemaphoreType.DMA
    shape = jax.ShapeDtypeStruct
    out_shape = (
        shape((SLOTS, 1024, 128), BF16),
        shape((SLOTS + 2, 32, 128), F32),
        shape((1024, 128), F32),
        shape((SPAN, INNER), BF16),
        shape((SPAN, 128), F32),
    )
    scratch = [
        pltpu.SMEM((2, 32), I32),
        pltpu.VMEM((32, 1, 128), I32),
        pltpu.VMEM((4, 8, 1, 128), I32),
        pltpu.VMEM((SLOTS, 32, 128), F32),
        pltpu.VMEM((SPAN, 128), F32),
        pltpu.VMEM((SLOTS, 1024, 128), F32),
        pltpu.VMEM((4, 8, HALF, 128), BF16),
        pltpu.VMEM((4, 8, HALF, 128), BF16),
        pltpu.VMEM((4, 8, HALF, 128), BF16),
        pltpu.VMEM((4, 8, HALF, 128), BF16),
        pltpu.VMEM((16, HALF, 128), BF16),
        pltpu.VMEM((16, HALF, 128), BF16),
        pltpu.VMEM((16, HALF, 128), BF16),
        pltpu.VMEM((16, HALF, 128), BF16),
        pltpu.VMEM((SPAN + 16, INNER), BF16),
        pltpu.VMEM((SPAN + 16, 256), BF16),
        pltpu.VMEM((SPAN, INNER), BF16),
        pltpu.VMEM((SPAN, INNER), BF16),
        pltpu.VMEM((SPAN, 128), BF16),
        pltpu.VMEM((SPAN, HEADS), F32),
        pltpu.VMEM((128, INNER), F32),
        pltpu.VMEM((4, 144, 1024), BF16),
        pltpu.VMEM((4, 144, 1024), BF16),
        pltpu.VMEM((4, 144, 1024), BF16),
        pltpu.VMEM((4, 144, 1024), BF16),
        pltpu.VMEM((4, 8, 128), F32),
        pltpu.VMEM((32, 1, 128), I32),
        pltpu.VMEM((4, 8, 1, 128), I32),
        pltpu.VMEM((4, 8, 1, 128), I32),
        pltpu.SMEM((32, 1, 128), I32),
        pltpu.SMEM((4, 8, 1, 128), I32),
        pltpu.SMEM((4, 8, 1, 128), I32),
        pltpu.VMEM((CHUNK, 192), BF16),
        pltpu.VMEM((HEADS, CHUNK), F32),
        pltpu.VMEM((CHUNK, 128), BF16),
        pltpu.VMEM((CHUNK, CHUNK), F32),
        pltpu.VMEM((CHUNK, CHUNK), BF16),
        pltpu.VMEM((8, 128), F32),
        pltpu.VMEM((4, 16, 128), BF16),
        pltpu.VMEM((1024, 128), F32),
        pltpu.VMEM((SLOTS + 2, 32, 128), F32),
        pltpu.VMEM((4, 16, INNER), BF16),
        pltpu.VMEM((4, 16, 256), BF16),
        pltpu.VMEM((4, 16, HEADS), BF16),
        pltpu.VMEM((48, 192), BF16),
        pltpu.VMEM((128, 128), BF16),
        pltpu.VMEM((16, 128), BF16),
        pltpu.VMEM((16, 16), F32),
        dma((SLOTS,)), dma((8,)), dma((32,)),
        dma((8,)), dma((8,)), dma((64,)), dma((64,)), dma((32,)), dma((32,)), dma((8,)), dma((8,)),
        dma((2,)), dma((2,)), dma((8,)), dma((8,)), dma((4,)), dma((4,)), dma((4,)), dma((4,)), dma((12,)), dma((12,)),
    ]
    return pl.pallas_call(
        exchange_kernel,
        out_shape=out_shape,
        in_specs=[SM, SM, SM, SM, ANY, VM, VM, ANY, ANY, ANY, VM, VM, VM, VM, VM],
        out_specs=[ANY] * len(out_shape),
        scratch_shapes=scratch,
        compiler_params=pltpu.CompilerParams(
            collective_id=1, has_side_effects=True, vmem_limit_bytes=67043328
        ),
        name="exchange",
    )(*operands)


PLACE_ROWS = SLOTS * 256


def place_kernel(moved, fin, gated, scale, norm_w, states, mixed):
    states[...] = moved[...].astype(F32)

    @pl.when(pl.program_id(0) == 0)
    def _():
        states[pl.ds(0, 1024), :] = fin[...]

    def norm_body(i, carry):
        lanes = pl.ds(pl.multiple_of(i * 128, 128), 128)
        mixed[:, lanes] = (gated[:, lanes].astype(F32) * scale[...] * norm_w[0:1, lanes]).astype(BF16)
        return carry

    lax.fori_loop(0, PAIRS, norm_body, 0)


def place(moved, fin, gated, scale, norm_w):
    rows = lambda count, lanes: pl.BlockSpec((count, lanes), lambda j: (j, 0))
    return pl.pallas_call(
        place_kernel,
        grid=(4,),
        out_shape=(
            jax.ShapeDtypeStruct((SLOTS * 1024, 128), F32),
            jax.ShapeDtypeStruct((SPAN, INNER), BF16),
        ),
        in_specs=[rows(PLACE_ROWS, 128), VM, rows(CHUNK, INNER), rows(CHUNK, 128), VM],
        out_specs=[rows(PLACE_ROWS, 128), rows(CHUNK, INNER)],
        name="place",
    )(moved, fin, gated, scale, norm_w)


def on_device(
    pool_states, inner_window, state_window, move_plan, active_mask, inputs_inner, inputs_state, gate_rows,
    step_raw, lengths, conv_weight, conv_bias, step_bias, decay_log, skip_weight, norm_weight,
):
    my = lax.axis_index("seq")
    odd = (my % 2) == 1
    moved, wout, fin, gated, scale = exchange(
        move_plan, active_mask, lengths, skip_weight, pool_states.reshape(SLOTS, 1024, 128), inner_window, state_window,
        inputs_inner[0], inputs_state[0], gate_rows[0], step_raw[0],
        conv_weight, conv_bias[None], step_bias[None], decay_log[None],
    )
    new_states, mix = place(moved.reshape(SLOTS * 1024, 128), fin, gated, scale, norm_weight[None])
    new_states = new_states.reshape(SLOTS, 16, 64, 128)
    kept_st = jnp.concatenate([wout[1, 3:6], wout[2, 3:6]], axis=1)
    kept_st = lax.dynamic_slice_in_dim(kept_st, my * 64, 64, 1)[None]
    rows = jnp.concatenate([wout[0:1], wout[3:]], axis=0)
    new_in = rows[:, 0:24].reshape(SLOTS, 3, 1024).astype(BF16)
    moved_st = wout[3:, 29:32]
    moved_st = jnp.where(odd, moved_st[:, :, 64:], moved_st[:, :, :64])
    new_st = jnp.concatenate([kept_st, moved_st], axis=0).astype(BF16)
    return (new_states, new_in, new_st, mix[None])


def solution(mesh):
    return jax.shard_map(
        on_device,
        mesh=mesh,
        in_specs=(
            P("req", "seq", None, None), P("req", None, "seq"), P("req", None, "seq"), P("req", None), P("req"),
            P("req", "seq", None), P("req", "seq", None), P("req", "seq", None), P("req", "seq", None), P("req"),
            P(), P(), P(), P(), P(), P(),
        ),
        out_specs=(
            P("req", "seq", None, None), P("req", None, "seq"), P("req", None, "seq"), P("req", "seq", None),
        ),
        check_vma=False,
    )
```

```python
import functools

import jax
import jax.numpy as jnp
from jax import lax
from jax.experimental import pallas as pl
from jax.experimental.pallas import tpu as pltpu
from jax.sharding import PartitionSpec as P

MESH = pl.DeviceIdType.MESH
ANY = pl.BlockSpec(memory_space=pl.ANY)
VM = pl.BlockSpec(memory_space=pltpu.VMEM)
SM = pl.BlockSpec(memory_space=pltpu.SMEM)
F32 = jnp.float32
BF16 = jnp.bfloat16
I32 = jnp.int32

SLOTS = 13
HEADS = 64
INNER = 4096
SPAN = 512
CHUNK = 128
CHUNKS = SPAN // CHUNK
PAIRS = HEADS // 2
HALF = 528
GROUP = 2
LOG2E = 1.4426950408889634
EPSILON = 1e-05


def nn(a, b):
    return lax.dot_general(a, b, (((1,), (0,)), ((), ())), preferred_element_type=F32)


def nt(a, b):
    return lax.dot_general(a, b, (((1,), (1,)), ((), ())), preferred_element_type=F32)


def split3(v):
    hi = v.astype(BF16)
    rest = v - hi.astype(F32)
    mid = rest.astype(BF16)
    lo = (rest - mid.astype(F32)).astype(BF16)
    return hi, mid, lo


def silu(v):
    half = 0.5 * v
    return half + half * jnp.tanh(half)


def softplus(v):
    u = jnp.exp(-jnp.abs(v))
    series = u * (1.0 - u * (0.5 - u * (1.0 / 3.0 - u * (0.25 - u * 0.2))))
    return jnp.maximum(v, 0.0) + jnp.where(u < 0.02, series, jnp.log(1.0 + u))


def pick_lanes(copies, pair):
    row = lax.broadcasted_iota(I32, (64, 128), 0)
    lane = lax.broadcasted_iota(I32, (64, 128), 1)
    one = jnp.where(row == 2 * pair + (lane >= 64).astype(I32), 1.0, 0.0).astype(BF16)
    return jnp.concatenate([one] * copies, axis=0)


def pick_heads(copies, pair):
    row = lax.broadcasted_iota(I32, (64, 256), 0)
    lane = lax.broadcasted_iota(I32, (64, 256), 1)
    one = jnp.where(row == 2 * pair + (lane >= 128).astype(I32), 1.0, 0.0).astype(BF16)
    return jnp.concatenate([one] * copies, axis=0)


def conv_tile(x, taps, bias, rows):
    acc = bias + taps[3:4] * x[16 : 16 + rows]
    for k in range(3):
        acc = acc + taps[k : k + 1] * x[13 + k : 13 + k + rows]
    return silu(acc).astype(BF16)


def exchange_kernel(
    plan, mask, lens, skip, pool, iw, sw, xin, xst, gate, step, conv_w, conv_b, step_b, decay,
    moved, wout, fin_out, mix, scale_out,
    meta, tags, tags_b, win, tot_buf,
    stage, sbuf_a, sbuf_b, rel_a, rel_b, near_a, near_b, far_a, far_b, xbuf, xsbuf, gbuf, y_buf, read_buf, cum_buf, st_buf,
    lsend, lrecv, ssend, srecv, tbuf, tagbuf, rtag_a, rtag_b, tag_s, rtag_as, rtag_bs,
    cum3, cumt, dt2, sc_buf, wt_buf, base_buf, wtile, fin_buf, wstage, ffin, ffst, ffdt,
    small3, w0t, read0_buf, sc0_buf,
    pool_sem, in_sem, out_sem, one_send, one_recv, two_send, two_recv, tag_send, tag_recv, rt_send, rt_recv,
    halo_send, halo_recv, lend_send, lend_recv, win_send, win_recv, s0_send, s0_recv, f_send, f_recv,
):
    me = lax.axis_index("req")
    my = lax.axis_index("seq")
    mx, mz, mc = me // 8, (me // 2) % 4, me % 2

    def at(dx, dz, dc):
        return ((mx + dx) % 4) * 8 + ((mz + dz) % 4) * 2 + (mc + dc) % 2

    loads = []
    for k in range(SLOTS):
        cp = pltpu.make_async_copy(pool.at[k], stage.at[k], pool_sem.at[k])
        cp.start()
        loads.append(cp)
    ins = [
        pltpu.make_async_copy(xin, xbuf.at[pl.ds(16, SPAN)], in_sem.at[0]),
        pltpu.make_async_copy(xst, xsbuf.at[pl.ds(16, SPAN)], in_sem.at[1]),
    ]
    for cp in ins:
        cp.start()
    gate_load = pltpu.make_async_copy(gate, gbuf, in_sem.at[2])
    gate_load.start()

    barrier = pltpu.get_barrier_semaphore()
    for r in range(1, 32):
        peer = at(r // 8, (r // 2) % 4, r % 2)
        pl.semaphore_signal(barrier, inc=1, device_id=(peer, my), device_id_type=MESH)
    for r in range(1, 4):
        pl.semaphore_signal(barrier, inc=1, device_id=(me, (my + r) % 4), device_id_type=MESH)

    def table_body(d, carry):
        slot, keep, tag = jnp.int32(0), jnp.int32(0), jnp.int32(0)
        for k in range(SLOTS):
            hit = plan[0, k] == d
            slot = jnp.where(hit, k, slot)
            keep = jnp.where(hit, mask[k], keep)
            tag = jnp.where(hit, plan[1, k] + 1, tag)
        meta[0, d] = slot
        meta[1, d] = keep
        row = jnp.full((1, 128), tag, I32)
        tags[d] = row
        tags_b[(d // 2) % 4, (d // 8) * 2 + d % 2] = row
        return carry

    lax.fori_loop(0, 32, table_body, 0)

    for k in range(SLOTS):
        win[k, pl.ds(24, 8), :] = jnp.zeros((8, 128), F32)
    for i in range(3):
        block = iw[i].astype(F32)
        own = sw[i].astype(F32)
        blank = jnp.zeros((SLOTS, 64), F32)
        wide = jnp.where(
            my % 2 == 1, jnp.concatenate([blank, own], axis=1), jnp.concatenate([own, blank], axis=1))
        for k in range(SLOTS):
            for q in range(8):
                win[k, pl.ds(i * 8 + q, 1), :] = block[k : k + 1, q * 128 : (q + 1) * 128]
            win[k, pl.ds(29 + i, 1), :] = wide[k : k + 1]
    pl.semaphore_wait(barrier, 34)

    def send(src, dst, ssem, rsem, dev):
        cp = pltpu.make_async_remote_copy(
            src_ref=src, dst_ref=dst, send_sem=ssem, recv_sem=rsem, device_id=dev, device_id_type=MESH
        )
        cp.start()
        return cp

    halo = [
        send(xin.at[pl.ds(SPAN - 16, 16)], xbuf.at[pl.ds(0, 16)], halo_send.at[0], halo_recv.at[0], (me, (my + 1) % 4)),
        send(xst.at[pl.ds(SPAN - 16, 16)], xsbuf.at[pl.ds(0, 16)], halo_send.at[1], halo_recv.at[1], (me, (my + 1) % 4)),
    ]
    firsts = []
    for r in range(1, 4):
        dev = (me, (my + r) % 4)
        firsts.append(send(xin.at[pl.ds(0, 16)], ffin.at[my], f_send.at[r], f_recv.at[r], dev))
        firsts.append(send(xst.at[pl.ds(0, 16)], ffst.at[my], f_send.at[4 + r], f_recv.at[4 + r], dev))
        firsts.append(send(step.at[:, pl.ds(0, 128)], ffdt.at[my], f_send.at[8 + r], f_recv.at[8 + r], dev))

    for cp in loads:
        cp.wait()

    def fill(ref, lead, q, dest, half):
        slot = meta[0, dest]
        keep = meta[1, dest].astype(F32)
        ref[lead, q, pl.ds(0, 512), :] = (stage[slot, pl.ds(512 * half, 512), :] * keep).astype(BF16)
        ref[lead, q, pl.ds(512, 16), :] = (win[slot, pl.ds(16 * half, 16), :] * keep).astype(BF16)

    def fill_a(ref, lead, xd):
        def one(q, carry):
            fill(ref, lead, q, xd * 8 + q, 0)
            return carry

        lax.fori_loop(0, 8, one, 0)

    def fill_b(ref, lead, zd):
        def one(q, carry):
            fill(ref, lead, q, (q // 2) * 8 + zd * 2 + q % 2, 1)
            return carry

        lax.fori_loop(0, 8, one, 0)

    phase_a, phase_b, rtags = {}, {}, []
    for d in (1, 3, 2):
        xd, zd = (mx + d) % 4, (mz + d) % 4
        dev_a, dev_b = (at(d, 0, 0), my), (at(0, d, 0), my)
        fill_a(sbuf_a, xd, xd)
        phase_a[d] = send(sbuf_a.at[xd], rel_a.at[mx], one_send.at[d], one_recv.at[d], dev_a)
        fill_b(sbuf_b, zd, zd)
        phase_b[d] = send(sbuf_b.at[zd], rel_b.at[mz], one_send.at[4 + d], one_recv.at[4 + d], dev_b)
        rtags.append(send(tags.at[pl.ds(xd * 8, 8)], rtag_a.at[mx], rt_send.at[d], rt_recv.at[d], dev_a))
        rtags.append(send(tags_b.at[zd], rtag_b.at[mz], rt_send.at[4 + d], rt_recv.at[4 + d], dev_b))
    fill_a(rel_a, mx, mx)
    fill_b(rel_b, mz, mz)

    second = {}

    def row_a(p):
        return (near_a if p < 2 else far_a).at[(p % 2) * 8 + mz * 2 + mc]

    def row_b(p):
        return (near_b if p < 2 else far_b).at[(p % 2) * 8 + mx * 2 + mc]

    def forward(p, e, src_a, src_b):
        de, dc = e // 2, e % 2
        sem = p * 8 + e
        second[p, e, 0] = send(
            src_a, row_a(p), two_send.at[sem], two_recv.at[sem], (at(0, de, dc), my))
        second[p, e, 1] = send(
            src_b, row_b(p), two_send.at[32 + sem], two_recv.at[32 + sem], (at(de, 0, dc), my))

    def targets(e):
        de, dc = e // 2, e % 2
        ct = (mc + dc) % 2
        return ((mz + de) % 4) * 2 + ct, ((mx + de) % 4) * 2 + ct

    for e in (2, 6, 3, 7, 1, 4, 5):
        ta, tb = targets(e)
        forward(0, e, rel_a.at[mx, ta], rel_b.at[mz, tb])
    row_a(0)[...] = rel_a[mx, mz * 2 + mc]
    row_b(0)[...] = rel_b[mz, mx * 2 + mc]

    tag_copies = []
    for r in range(1, 32):
        peer = at(r // 8, (r // 2) % 4, r % 2)
        tag_copies.append(
            send(tags.at[peer], tagbuf.at[me], tag_send.at[r], tag_recv.at[r], (peer, my))
        )
    tagbuf[me] = tags[me]

    for cp in ins:
        cp.wait()
    for cp in halo:
        cp.wait()

    @pl.when(my == 0)
    def _():
        xbuf[pl.ds(0, 16), :] = jnp.zeros((16, INNER), BF16)
        xsbuf[pl.ds(0, 16), :] = jnp.zeros((16, 256), BF16)

    st_buf[...] = jnp.zeros_like(st_buf)
    base_buf[...] = jnp.zeros_like(base_buf)
    length = lens[0]

    def chunk_body(k, carry):
        r0 = pl.multiple_of(k * CHUNK, CHUNK)
        pos = my * SPAN + r0 + lax.broadcasted_iota(I32, (CHUNK, HEADS), 0)
        live = ((pos < length) & (pos >= 3)).astype(F32)
        dt = softplus(jnp.transpose(step[:, pl.ds(r0, CHUNK)].astype(F32)) + step_b[0:1, :]) * live
        rate = dt * (-LOG2E * jnp.exp(decay[0:1, :]))
        rows = lax.broadcasted_iota(I32, (CHUNK, CHUNK), 0)
        cols = lax.broadcasted_iota(I32, (CHUNK, CHUNK), 1)
        tri = jnp.where(rows >= cols, 1.0, 0.0).astype(BF16)
        hi, mid, lo = split3(rate)
        cum = nn(tri, hi) + nn(tri, mid) + nn(tri, lo)
        cum3[...] = jnp.concatenate(split3(cum), axis=1)
        cumt[...] = jnp.transpose(cum)
        dth = dt.astype(BF16)
        dt2[...] = jnp.concatenate([dth, (dt - dth.astype(F32)).astype(BF16)], axis=1)
        cum_buf[pl.ds(r0, CHUNK), :] = cum + base_buf[0:1, 0:HEADS]
        base_buf[0:1, 0:HEADS] = base_buf[0:1, 0:HEADS] + cum[CHUNK - 1 : CHUNK, :]
        xs_tile = xsbuf[pl.ds(r0, CHUNK + 16), :].astype(F32)
        mixed = conv_tile(xs_tile, conv_w[:, INNER : INNER + 256], jnp.concatenate([conv_b[32:33, :], conv_b[33:34, :]], axis=1), CHUNK)
        write, read = mixed[:, 0:128], mixed[:, 128:256]
        read_buf[pl.ds(r0, CHUNK), :] = read
        sc_buf[...] = jnp.where(rows >= cols, nt(read, write), 0.0)
        wt_buf[...] = jnp.transpose(write.astype(F32)).astype(BF16)

        def group_body(j, inner):
            lanes = [pl.ds(pl.multiple_of(j * (GROUP * 128) + g * 128, 128), 128) for g in range(GROUP)]
            pairs = [j * GROUP + g for g in range(GROUP)]
            every = range(GROUP)
            low = lax.broadcasted_iota(I32, (CHUNK, 128), 1) < 64
            lane = lax.broadcasted_iota(I32, (1, 128), 1)
            x = [xbuf[pl.ds(r0, CHUNK + 16), lanes[g]].astype(F32) for g in every]
            state = [st_buf[:, lanes[g]] for g in every]
            both = [nn(cum3[...], pick_heads(3, pairs[g])) for g in every]
            dte = [nn(dt2[...], pick_lanes(2, pairs[g])) for g in every]
            carried = [nn(read_buf[pl.ds(r0, CHUNK), :], state[g].astype(BF16)) for g in every]
            value = [conv_tile(x[g], conv_w[:, lanes[g]], conv_b[pl.ds(pairs[g], 1), :], CHUNK).astype(F32) for g in every]
            ys, states = [], []
            for g in every:
                sc = sc_buf[...]
                c1, c2 = both[g][:, 0:128], both[g][:, 128:256]
                w1 = sc * jnp.exp2(jnp.minimum(c1 - cumt[pl.ds(2 * pairs[g], 1), :], 0.0))
                w2 = sc * jnp.exp2(jnp.minimum(c2 - cumt[pl.ds(2 * pairs[g] + 1, 1), :], 0.0))
                cp = jnp.where(low, c1, c2)
                vd = value[g] * dte[g]
                zero = jnp.zeros_like(vd)
                rhs = jnp.concatenate([jnp.where(low, vd, zero), jnp.where(low, zero, vd)], axis=0).astype(BF16)
                lhs = jnp.concatenate([w1.astype(BF16), w2.astype(BF16)], axis=1)
                last = cp[CHUNK - 1 : CHUNK, :]
                scaled = (jnp.exp2(last - cp) * vd).astype(BF16)
                skip_lane = jnp.where(lane < 64, skip[2 * pairs[g]], skip[2 * pairs[g] + 1])
                ys.append(nn(lhs, rhs) + carried[g] * jnp.exp2(cp) + skip_lane * value[g])
                states.append(jnp.exp2(last) * state[g] + nn(wt_buf[...], scaled))
            for g in every:
                y_buf[pl.ds(r0, CHUNK), lanes[g]] = ys[g].astype(BF16)
                st_buf[:, lanes[g]] = states[g]
            return inner

        lax.fori_loop(0, PAIRS // GROUP, group_body, 0)
        return carry

    lax.fori_loop(0, CHUNKS, chunk_body, 0)

    cols = lax.broadcasted_iota(I32, (16, SPAN), 1)
    rows = lax.broadcasted_iota(I32, (16, SPAN), 0)
    want = length - 3 - my * SPAN
    sel_in = jnp.where((cols == want + rows) & (rows < 3), 1.0, 0.0).astype(BF16)
    sel_st = jnp.where((cols == want + rows - 3) & (rows >= 3) & (rows < 6), 1.0, 0.0).astype(BF16)
    small3[0:16, :] = jnp.zeros((16, 192), BF16)
    lst = nn(sel_st, xsbuf[pl.ds(16, SPAN), :])

    def lend_body(i, carry):
        lanes = pl.ds(pl.multiple_of(i * 256, 256), 256)
        to = pl.ds(pl.multiple_of((i % 4) * 256, 256), 256)
        lsend[i // 4, pl.ds(0, 128), to] = st_buf[:, lanes].astype(BF16)
        first = jnp.where(i % 4 == 0, 1.0, 0.0)
        lsend[i // 4, pl.ds(128, 16), to] = (nn(sel_in, xbuf[pl.ds(16, SPAN), lanes]) + first * lst).astype(BF16)
        return carry

    lax.fori_loop(0, INNER // 256, lend_body, 0)
    tbuf[my] = base_buf[...]
    lrecv[my] = lsend[my]
    lends = []
    for r in range(1, 4):
        dev = (me, (my + r) % 4)
        lends.append(send(lsend.at[(my + r) % 4], lrecv.at[my], lend_send.at[r], lend_recv.at[r], dev))
        lends.append(send(tbuf.at[my], tbuf.at[my], lend_send.at[4 + r], lend_recv.at[4 + r], dev))

    @pl.when(my == 0)
    def _():
        rowc = lax.broadcasted_iota(I32, (16, HEADS), 0)
        cum_buf[pl.ds(0, 16), :] = jnp.where(rowc < 3, -1.0e6, cum_buf[pl.ds(0, 16), :])

    gate_load.wait()

    def ready_body(k, carry):
        r0 = pl.multiple_of(k * CHUNK, CHUNK)
        cum3[...] = jnp.concatenate(split3(cum_buf[pl.ds(r0, CHUNK), :]), axis=1)
        rowpos = my * SPAN + r0 + lax.broadcasted_iota(I32, (CHUNK, 128), 0)

        def group_body(j, inner):
            lanes = [pl.ds(pl.multiple_of(j * 256 + g * 128, 128), 128) for g in range(2)]
            valid = (rowpos < length).astype(F32)
            ce = [nn(cum3[...], pick_lanes(3, 2 * j + g)) for g in range(2)]
            gates = [silu(gbuf[pl.ds(r0, CHUNK), lanes[g]].astype(F32)) * valid for g in range(2)]
            for g in range(2):
                xbuf[pl.ds(r0, CHUNK), lanes[g]] = jnp.exp2(ce[g]).astype(BF16)
                gbuf[pl.ds(r0, CHUNK), lanes[g]] = gates[g].astype(BF16)
            return inner

        lax.fori_loop(0, PAIRS // 2, group_body, 0)
        return carry

    lax.fori_loop(0, CHUNKS, ready_body, 0)
    tot_buf[...] = jnp.zeros_like(tot_buf)

    for cp in rtags:
        cp.wait()
    tag_loads = [
        pltpu.make_async_copy(rtag_a, rtag_as, in_sem.at[3]),
        pltpu.make_async_copy(rtag_b, rtag_bs, in_sem.at[4]),
    ]
    for cp in tag_loads:
        cp.start()
    for d in (1, 3, 2):
        phase_a[d].wait()
        phase_b[d].wait()
    for cp in tag_loads:
        cp.wait()

    def swapped(first, p):
        if p == 1:
            return jnp.where(first >= 2, first, 1)
        return jnp.where(first == p, 1, p)

    for p in (1, 2, 3):
        for e in (2, 6, 3, 7, 0, 1, 4, 5):
            ta, tb = targets(e)
            first_a, first_b = jnp.int32(0), jnp.int32(0)
            for q in (1, 2, 3):
                first_a = jnp.where(rtag_as[(mx + 4 - q) % 4, ta, 0, 0] == 1, q, first_a)
                first_b = jnp.where(rtag_bs[(mz + 4 - q) % 4, tb, 0, 0] == 1, q, first_b)
            block_a = rel_a[(mx + 4 - swapped(first_a, p)) % 4, ta]
            block_b = rel_b[(mz + 4 - swapped(first_b, p)) % 4, tb]
            if e == 0:
                row_a(p)[...] = block_a
                row_b(p)[...] = block_b
            else:
                sbuf_a[p, e] = block_a
                sbuf_b[p, e] = block_b
                forward(p, e, sbuf_a.at[p, e], sbuf_b.at[p, e])

    for cp in tag_copies:
        cp.wait()
    tag_load = pltpu.make_async_copy(tagbuf, tag_s, in_sem.at[5])
    tag_load.start()
    tag_load.wait()

    def source_of(j):
        acc = jnp.int32(0)
        for s in range(32):
            acc = jnp.where(tag_s[s, 0, 0] == j + 1, s, acc)
        return acc

    def split_source(src):
        xs, zs, cs = src // 8, (src // 2) % 4, src % 2
        return (mx + 4 - xs) % 4, zs * 2 + cs, (mz + 4 - zs) % 4, xs * 2 + cs

    hops0_a, relay0_a, hops0_b, relay0_b = split_source(source_of(0))
    loc0_a = jnp.where(hops0_a > 0, 8, 0) + relay0_a
    loc0_b = jnp.where(hops0_b > 0, 8, 0) + relay0_b

    def rank(hops, relay, hops0, relay0):
        moved_up = jnp.where(hops == hops0, 1, jnp.where(hops == 1, hops0, hops))
        place_in = jnp.where((relay == relay0) & (hops0 >= 2) & (hops > 0), moved_up, hops)
        return place_in * 8 + relay

    def places(j):
        hops_a, relay_a, hops_b, relay_b = split_source(source_of(j))
        return rank(hops_a, relay_a, hops0_a, relay0_a), rank(hops_b, relay_b, hops0_b, relay0_b)

    def fetch(near, far, loc):
        return jnp.where(loc < 16, near[jnp.minimum(loc, 15)], far[jnp.maximum(loc - 16, 0)])

    for cp in firsts:
        cp.wait()
    own_first = [
        pltpu.make_async_copy(xin.at[pl.ds(0, 16)], ffin.at[my], in_sem.at[6]),
        pltpu.make_async_copy(xst.at[pl.ds(0, 16)], ffst.at[my], in_sem.at[7]),
    ]
    for cp in own_first:
        cp.start()
    ffdt[my] = step[:, 0:128]
    for cp in own_first:
        cp.wait()
    for cp in lends:
        cp.wait()

    for p in (0, 1):
        for e in range(1, 8):
            second[p, e, 0].wait()
            second[p, e, 1].wait()

    wtile[my] = near_b[loc0_b, pl.ds(512, 16), :]
    wins = []
    for r in range(1, 4):
        wins.append(send(wtile.at[my], wtile.at[my], win_send.at[r], win_recv.at[r], (me, (my + r) % 4)))

    posf = lax.broadcasted_iota(I32, (16, HEADS), 0)
    livef = ((posf < length) & (posf < 3)).astype(F32)
    dtf0 = softplus(jnp.transpose(ffdt[0].astype(F32))[0:16] + step_b[0:1, :]) * livef
    rate0 = dtf0 * (-LOG2E * jnp.exp(decay[0:1, :]))
    c0 = rate0[0:1]
    c1 = c0 + rate0[1:2]
    c2 = c1 + rate0[2:3]
    cumf = jnp.where(posf == 0, c0, jnp.where(posf == 1, c1, c2))
    totals = jnp.where(posf == 0, tbuf[0][0:1, 0:HEADS], jnp.where(
        posf == 1, tbuf[1][0:1, 0:HEADS], jnp.where(posf == 2, tbuf[2][0:1, 0:HEADS], tbuf[3][0:1, 0:HEADS])))
    small3[0:16, :] = jnp.concatenate(split3(cumf), axis=1)
    small3[16:32, :] = jnp.concatenate(split3(dtf0), axis=1)
    small3[32:48, :] = jnp.concatenate(split3(totals), axis=1)

    for cp in wins:
        cp.wait()
    w_low = wtile[0].astype(F32) + wtile[1].astype(F32)
    w_high = wtile[2].astype(F32) + wtile[3].astype(F32)
    e_st = jnp.concatenate([jnp.concatenate([w_low, w_high], axis=1), ffst[0].astype(F32)], axis=0)
    mixed0 = conv_tile(e_st, conv_w[:, INNER : INNER + 256], jnp.concatenate([conv_b[32:33, :], conv_b[33:34, :]], axis=1), 16)
    write0, read0 = mixed0[:, 0:128], mixed0[:, 128:256]
    read0_buf[...] = read0
    sc0_buf[...] = nt(read0, write0)
    w0t[...] = jnp.transpose(
        jnp.concatenate([write0.astype(F32), jnp.zeros((112, 128), F32)], axis=0)).astype(BF16)

    row16 = lax.broadcasted_iota(I32, (16, 128), 0)
    lane1 = lax.broadcasted_iota(I32, (1, 128), 1)
    for q in range(8):
        i = my * 8 + q
        lanes = pl.ds(pl.multiple_of(my * 1024 + q * 128, 128), 128)
        own = pl.ds(q * 128, 128)
        if q < 4:
            s0 = near_a[loc0_a, pl.ds(q * 128, 128), :]
        else:
            s0 = near_b[loc0_b, pl.ds((q - 4) * 128, 128), :]
        s0t = jnp.transpose(s0.astype(F32))
        wa = near_a[loc0_a, pl.ds(512, 16), :].astype(F32)
        wb = near_b[loc0_b, pl.ds(512, 16), :].astype(F32)
        wq = jnp.where(row16 == 13, wa[q : q + 1], jnp.where(row16 == 14, wa[8 + q : 9 + q], wb[q : q + 1]))
        x0 = jnp.concatenate([wq, ffin[0, :, lanes].astype(F32)], axis=0)
        small = nn(small3[...], pick_lanes(3, i))
        cf, dtf, totl = small[0:16], small[16:32], small[32:48]
        v0 = conv_tile(x0, conv_w[:, lanes], conv_b[pl.ds(i, 1), :], 16).astype(F32)
        vd = v0 * dtf
        scaled = jnp.concatenate([jnp.exp2(cf[2:3] - cf) * vd, jnp.zeros((112, 128), F32)], axis=0).astype(BF16)
        carry = jnp.exp2(cf[2:3]) * s0t + nn(w0t[...], scaled)
        y0 = nt(read0_buf[...], s0) * jnp.exp2(cf)
        y0 = y0 + jnp.where(lane1 < 64, skip[2 * i], skip[2 * i + 1]) * v0
        for s in range(3):
            term = sc0_buf[:, s : s + 1] * jnp.exp2(jnp.minimum(cf - cf[s : s + 1], 0.0)) * vd[s : s + 1]
            y0 = y0 + jnp.where(row16 >= s, term, 0.0)
        kept = jnp.zeros((16, 128), F32)
        for c in range(4):
            ssend[c, pl.ds(0, 128), own] = carry.astype(BF16)
            ssend[c, pl.ds(128, 16), own] = y0.astype(BF16)
            carry = jnp.exp2(totl[c : c + 1]) * carry + lrecv[c, pl.ds(0, 128), own].astype(F32)
            kept = kept + lrecv[c, pl.ds(128, 16), own].astype(F32)
        fin_buf[pl.ds(q * 128, 128), :] = jnp.transpose(carry)
        for r in range(3):
            wstage[0, pl.ds(r * 8 + q, 1), :] = kept[r : r + 1]
        if q < 2:
            wstage[1 + q, pl.ds(0, 16), :] = kept

    sins = []
    for r in range(1, 4):
        other = (my + r) % 4
        sins.append(send(ssend.at[other], srecv.at[my], s0_send.at[r], s0_recv.at[r], (me, other)))
    srecv[my] = ssend[my]

    outs = []

    def put_out(src, dst, i):
        cp = pltpu.make_async_copy(src, dst, out_sem.at[i])
        cp.start()
        outs.append(cp)

    put_out(fin_buf, fin_out, 30)
    def quarter(owner):
        base = owner * 1024

        @pl.when(my == 0)
        def _():
            for j in range(4):
                lanes = pl.ds(pl.multiple_of(base + j * 256, 128), 256)
                new = srecv[owner, pl.ds(128, 16), pl.ds(j * 256, 256)].astype(F32)
                old = y_buf[pl.ds(0, 16), lanes].astype(F32)
                rowy = lax.broadcasted_iota(I32, (16, 256), 0)
                y_buf[pl.ds(0, 16), lanes] = jnp.where(rowy < 3, new, old).astype(BF16)

        def group_body(j, carry):
            lanes = pl.ds(pl.multiple_of(base + j * 256, 128), 256)
            state = srecv[owner, pl.ds(0, 128), pl.ds(pl.multiple_of(j * 256, 256), 256)]
            spans = [pl.ds(r * CHUNK, CHUNK) for r in range(CHUNKS)]
            parts = [nn(read_buf[span, :], state) for span in spans]
            new, squares = [], []
            for span, part in zip(spans, parts):
                y = y_buf[span, lanes].astype(F32) + xbuf[span, lanes].astype(F32) * part
                v = y.astype(BF16).astype(F32) * gbuf[span, lanes].astype(F32)
                new.append(v.astype(BF16))
                squares.append(tot_buf[span, :] + v[:, 0:128] * v[:, 0:128] + v[:, 128:256] * v[:, 128:256])
            for span, v, square in zip(spans, new, squares):
                y_buf[span, lanes] = v
                tot_buf[span, :] = square
            return carry

        lax.fori_loop(0, 4, group_body, 0)

    quarter(my)
    for r in (1, 3, 2):
        sins[r - 1].wait()
        quarter((my + 4 - r) % 4)
    put_out(y_buf, mix, 31)
    tot_buf[...] = jnp.broadcast_to(
        lax.rsqrt(jnp.sum(tot_buf[...], axis=1, keepdims=True) * (1.0 / INNER) + EPSILON), (SPAN, 128))
    put_out(tot_buf, scale_out, 29)

    spots = [places(j) for j in range(SLOTS)]
    for p in (2, 3):
        for e in range(1, 8):
            second[p, e, 0].wait()
            second[p, e, 1].wait()
    for j in range(1, SLOTS):
        loc_a, loc_b = spots[j]
        sbuf_a[j // 8, j % 8] = fetch(near_a, far_a, loc_a)
        sbuf_b[j // 8, j % 8] = fetch(near_b, far_b, loc_b)
        put_out(sbuf_a.at[j // 8, j % 8, pl.ds(0, 512)], moved.at[j, pl.ds(0, 512)], 2 * j)
        put_out(sbuf_b.at[j // 8, j % 8, pl.ds(0, 512)], moved.at[j, pl.ds(512, 512)], 2 * j + 1)
        wstage[2 + j, pl.ds(0, 16), :] = sbuf_a[j // 8, j % 8, pl.ds(512, 16), :].astype(F32)
        wstage[2 + j, pl.ds(16, 16), :] = sbuf_b[j // 8, j % 8, pl.ds(512, 16), :].astype(F32)
    put_out(wstage, wout, 0)
    for cp in outs:
        cp.wait()


def exchange(*operands):
    dma = pltpu.SemaphoreType.DMA
    shape = jax.ShapeDtypeStruct
    out_shape = (
        shape((SLOTS, 1024, 128), BF16),
        shape((SLOTS + 2, 32, 128), F32),
        shape((1024, 128), F32),
        shape((SPAN, INNER), BF16),
        shape((SPAN, 128), F32),
    )
    scratch = [
        pltpu.SMEM((2, 32), I32),
        pltpu.VMEM((32, 1, 128), I32),
        pltpu.VMEM((4, 8, 1, 128), I32),
        pltpu.VMEM((SLOTS, 32, 128), F32),
        pltpu.VMEM((SPAN, 128), F32),
        pltpu.VMEM((SLOTS, 1024, 128), F32),
        pltpu.VMEM((4, 8, HALF, 128), BF16),
        pltpu.VMEM((4, 8, HALF, 128), BF16),
        pltpu.VMEM((4, 8, HALF, 128), BF16),
        pltpu.VMEM((4, 8, HALF, 128), BF16),
        pltpu.VMEM((16, HALF, 128), BF16),
        pltpu.VMEM((16, HALF, 128), BF16),
        pltpu.VMEM((16, HALF, 128), BF16),
        pltpu.VMEM((16, HALF, 128), BF16),
        pltpu.VMEM((SPAN + 16, INNER), BF16),
        pltpu.VMEM((SPAN + 16, 256), BF16),
        pltpu.VMEM((SPAN, INNER), BF16),
        pltpu.VMEM((SPAN, INNER), BF16),
        pltpu.VMEM((SPAN, 128), BF16),
        pltpu.VMEM((SPAN, HEADS), F32),
        pltpu.VMEM((128, INNER), F32),
        pltpu.VMEM((4, 144, 1024), BF16),
        pltpu.VMEM((4, 144, 1024), BF16),
        pltpu.VMEM((4, 144, 1024), BF16),
        pltpu.VMEM((4, 144, 1024), BF16),
        pltpu.VMEM((4, 8, 128), F32),
        pltpu.VMEM((32, 1, 128), I32),
        pltpu.VMEM((4, 8, 1, 128), I32),
        pltpu.VMEM((4, 8, 1, 128), I32),
        pltpu.SMEM((32, 1, 128), I32),
        pltpu.SMEM((4, 8, 1, 128), I32),
        pltpu.SMEM((4, 8, 1, 128), I32),
        pltpu.VMEM((CHUNK, 192), BF16),
        pltpu.VMEM((HEADS, CHUNK), F32),
        pltpu.VMEM((CHUNK, 128), BF16),
        pltpu.VMEM((CHUNK, CHUNK), F32),
        pltpu.VMEM((CHUNK, CHUNK), BF16),
        pltpu.VMEM((8, 128), F32),
        pltpu.VMEM((4, 16, 128), BF16),
        pltpu.VMEM((1024, 128), F32),
        pltpu.VMEM((SLOTS + 2, 32, 128), F32),
        pltpu.VMEM((4, 16, INNER), BF16),
        pltpu.VMEM((4, 16, 256), BF16),
        pltpu.VMEM((4, HEADS, 128), BF16),
        pltpu.VMEM((48, 192), BF16),
        pltpu.VMEM((128, 128), BF16),
        pltpu.VMEM((16, 128), BF16),
        pltpu.VMEM((16, 16), F32),
        dma((SLOTS,)), dma((8,)), dma((32,)),
        dma((8,)), dma((8,)), dma((64,)), dma((64,)), dma((32,)), dma((32,)), dma((8,)), dma((8,)),
        dma((2,)), dma((2,)), dma((8,)), dma((8,)), dma((4,)), dma((4,)), dma((4,)), dma((4,)), dma((12,)), dma((12,)),
    ]
    return pl.pallas_call(
        exchange_kernel,
        out_shape=out_shape,
        in_specs=[SM, SM, SM, SM, ANY, VM, VM, ANY, ANY, ANY, VM, VM, VM, VM, VM],
        out_specs=[ANY] * len(out_shape),
        scratch_shapes=scratch,
        compiler_params=pltpu.CompilerParams(
            collective_id=1, has_side_effects=True, vmem_limit_bytes=67043328
        ),
        name="exchange",
    )(*operands)


STEPS = 8
PLACE_ROWS = SLOTS * 1024 // STEPS
MIX_ROWS = SPAN // STEPS


def place_kernel(moved, fin, gated, scale, norm_w, wout, states, mixed, win_in, win_st, acc_in, acc_st):
    my = lax.axis_index("seq")
    states[...] = moved[...].astype(F32)

    @pl.when(pl.program_id(0) == 0)
    def _():
        states[pl.ds(0, 1024), :] = fin[...]
        for j in range(SLOTS):
            src = 0 if j == 0 else 2 + j
            for i in range(3):
                for q in range(8):
                    acc_in[i, pl.ds(j, 1), pl.ds(q * 128, 128)] = wout[src, pl.ds(i * 8 + q, 1), :]
                if j == 0:
                    acc_st[i, pl.ds(0, 1), :] = jnp.where(my >= 2, wout[2, pl.ds(3 + i, 1), :], wout[1, pl.ds(3 + i, 1), :])
                else:
                    acc_st[i, pl.ds(j, 1), :] = wout[src, pl.ds(29 + i, 1), :]
        for i in range(3):
            win_in[i] = acc_in[i].astype(BF16)
            rows = acc_st[i]
            win_st[i] = jnp.where(my % 2 == 1, rows[:, 64:128], rows[:, 0:64]).astype(BF16)

    def norm_body(i, carry):
        lanes = pl.ds(pl.multiple_of(i * 128, 128), 128)
        mixed[:, lanes] = (gated[:, lanes].astype(F32) * scale[...] * norm_w[pl.ds(i, 1), :]).astype(BF16)
        return carry

    lax.fori_loop(0, PAIRS, norm_body, 0, unroll=4)


def place(moved, fin, gated, scale, norm_w, wout):
    rows = lambda count, lanes: pl.BlockSpec((count, lanes), lambda j: (j, 0))
    whole = lambda lanes: pl.BlockSpec((3, SLOTS, lanes), lambda j: (0, 0, 0))
    return pl.pallas_call(
        place_kernel,
        grid=(STEPS,),
        out_shape=(
            jax.ShapeDtypeStruct((SLOTS * 1024, 128), F32),
            jax.ShapeDtypeStruct((SPAN, INNER), BF16),
            jax.ShapeDtypeStruct((3, SLOTS, 1024), BF16),
            jax.ShapeDtypeStruct((3, SLOTS, 64), BF16),
        ),
        in_specs=[rows(PLACE_ROWS, 128), VM, rows(MIX_ROWS, INNER), rows(MIX_ROWS, 128), VM, VM],
        out_specs=[rows(PLACE_ROWS, 128), rows(MIX_ROWS, INNER), whole(1024), whole(64)],
        scratch_shapes=[pltpu.VMEM((3, SLOTS, 1024), F32), pltpu.VMEM((3, SLOTS, 128), F32)],
        name="place",
    )(moved, fin, gated, scale, norm_w, wout)


def on_device(
    pool_states, inner_window, state_window, move_plan, active_mask, inputs_inner, inputs_state, gate_rows,
    step_raw, lengths, conv_weight, conv_bias, step_bias, decay_log, skip_weight, norm_weight,
):
    moved, wout, fin, gated, scale = exchange(
        move_plan.T, active_mask, lengths, skip_weight, pool_states.reshape(SLOTS, 1024, 128),
        jnp.transpose(inner_window, (1, 0, 2)), jnp.transpose(state_window, (1, 0, 2)),
        inputs_inner[0], inputs_state[0], gate_rows[0], step_raw[0].T,
        conv_weight, conv_bias.reshape(34, 128), step_bias[None], decay_log[None],
    )
    new_states, mix, new_in, new_st = place(
        moved.reshape(SLOTS * 1024, 128), fin, gated, scale, norm_weight.reshape(32, 128), wout)
    return (
        new_states.reshape(SLOTS, 16, 64, 128), jnp.transpose(new_in, (1, 0, 2)), jnp.transpose(new_st, (1, 0, 2)),
        mix[None],
    )


def solution(mesh):
    return jax.shard_map(
        on_device,
        mesh=mesh,
        in_specs=(
            P("req", "seq", None, None), P("req", None, "seq"), P("req", None, "seq"), P("req", None), P("req"),
            P("req", "seq", None), P("req", "seq", None), P("req", "seq", None), P("req", "seq", None), P("req"),
            P(), P(), P(), P(), P(), P(),
        ),
        out_specs=(
            P("req", "seq", None, None), P("req", None, "seq"), P("req", None, "seq"), P("req", "seq", None),
        ),
        check_vma=False,
    )
```

```python
import functools

import jax
import jax.numpy as jnp
from jax import lax
from jax.experimental import pallas as pl
from jax.experimental.pallas import tpu as pltpu
from jax.sharding import PartitionSpec as P

MESH = pl.DeviceIdType.MESH
ANY = pl.BlockSpec(memory_space=pl.ANY)
VM = pl.BlockSpec(memory_space=pltpu.VMEM)
SM = pl.BlockSpec(memory_space=pltpu.SMEM)
F32 = jnp.float32
BF16 = jnp.bfloat16
I32 = jnp.int32

SLOTS = 13
HEADS = 64
INNER = 4096
SPAN = 512
CHUNK = 128
CHUNKS = SPAN // CHUNK
PAIRS = HEADS // 2
HALF = 528
GROUP = 2
LOG2E = 1.4426950408889634
EPSILON = 1e-05


def nn(a, b):
    return lax.dot_general(a, b, (((1,), (0,)), ((), ())), preferred_element_type=F32)


def nt(a, b):
    return lax.dot_general(a, b, (((1,), (1,)), ((), ())), preferred_element_type=F32)


def split3(v):
    hi = v.astype(BF16)
    rest = v - hi.astype(F32)
    mid = rest.astype(BF16)
    lo = (rest - mid.astype(F32)).astype(BF16)
    return hi, mid, lo


def silu(v):
    half = 0.5 * v
    return half + half * jnp.tanh(half)


def softplus(v):
    u = jnp.exp(-jnp.abs(v))
    series = u * (1.0 - u * (0.5 - u * (1.0 / 3.0 - u * (0.25 - u * 0.2))))
    return jnp.maximum(v, 0.0) + jnp.where(u < 0.02, series, jnp.log(1.0 + u))


def pick_lanes(copies, pair):
    row = lax.broadcasted_iota(I32, (64, 128), 0)
    lane = lax.broadcasted_iota(I32, (64, 128), 1)
    one = jnp.where(row == 2 * pair + (lane >= 64).astype(I32), 1.0, 0.0).astype(BF16)
    return jnp.concatenate([one] * copies, axis=0)


def pick_heads(copies, pair):
    row = lax.broadcasted_iota(I32, (64, 256), 0)
    lane = lax.broadcasted_iota(I32, (64, 256), 1)
    one = jnp.where(row == 2 * pair + (lane >= 128).astype(I32), 1.0, 0.0).astype(BF16)
    return jnp.concatenate([one] * copies, axis=0)


def conv_tile(x, taps, bias, rows):
    acc = bias + taps[3:4] * x[16 : 16 + rows]
    for k in range(3):
        acc = acc + taps[k : k + 1] * x[13 + k : 13 + k + rows]
    return silu(acc).astype(BF16)


def exchange_kernel(
    plan, mask, lens, skip, pool, iw, sw, xin, xst, gate, step, conv_w, conv_b, step_b, decay,
    moved, wout, fin_out, mix, scale_out,
    meta, tags, tags_b, win, tot_buf,
    stage, sbuf_a, sbuf_b, rel_a, rel_b, near_a, near_b, far_a, far_b, xbuf, xsbuf, gbuf, y_buf, read_buf, cum_buf, st_buf,
    lsend, lrecv, ssend, srecv, tbuf, tagbuf, rtag_a, rtag_b, tag_s, rtag_as, rtag_bs,
    cum3, cumt, dt2, sc_buf, wt_buf, base_buf, wtile, fin_buf, wstage, ffin, ffst, ffdt,
    small3, w0t, read0_buf, sc0_buf,
    pool_sem, in_sem, out_sem, one_send, one_recv, two_send, two_recv, tag_send, tag_recv, rt_send, rt_recv,
    halo_send, halo_recv, lend_send, lend_recv, win_send, win_recv, s0_send, s0_recv, f_send, f_recv,
):
    me = lax.axis_index("req")
    my = lax.axis_index("seq")
    mx, mz, mc = me // 8, (me // 2) % 4, me % 2

    def at(dx, dz, dc):
        return ((mx + dx) % 4) * 8 + ((mz + dz) % 4) * 2 + (mc + dc) % 2

    loads = []
    for k in range(SLOTS):
        cp = pltpu.make_async_copy(pool.at[k], stage.at[k], pool_sem.at[k])
        cp.start()
        loads.append(cp)
    ins = [
        pltpu.make_async_copy(xin, xbuf.at[pl.ds(16, SPAN)], in_sem.at[0]),
        pltpu.make_async_copy(xst, xsbuf.at[pl.ds(16, SPAN)], in_sem.at[1]),
    ]
    for cp in ins:
        cp.start()
    gate_load = pltpu.make_async_copy(gate, gbuf, in_sem.at[2])
    gate_load.start()

    barrier = pltpu.get_barrier_semaphore()
    for r in range(1, 32):
        peer = at(r // 8, (r // 2) % 4, r % 2)
        pl.semaphore_signal(barrier, inc=1, device_id=(peer, my), device_id_type=MESH)
    for r in range(1, 4):
        pl.semaphore_signal(barrier, inc=1, device_id=(me, (my + r) % 4), device_id_type=MESH)

    def table_body(d, carry):
        slot, keep, tag = jnp.int32(0), jnp.int32(0), jnp.int32(0)
        for k in range(SLOTS):
            hit = plan[0, k] == d
            slot = jnp.where(hit, k, slot)
            keep = jnp.where(hit, mask[k], keep)
            tag = jnp.where(hit, plan[1, k] + 1, tag)
        meta[0, d] = slot
        meta[1, d] = keep
        row = jnp.full((1, 128), tag, I32)
        tags[d] = row
        tags_b[(d // 2) % 4, (d // 8) * 2 + d % 2] = row
        return carry

    lax.fori_loop(0, 32, table_body, 0)

    for k in range(SLOTS):
        win[k, pl.ds(24, 8), :] = jnp.zeros((8, 128), F32)
    for i in range(3):
        block = iw[i].astype(F32)
        own = sw[i].astype(F32)
        blank = jnp.zeros((SLOTS, 64), F32)
        wide = jnp.where(
            my % 2 == 1, jnp.concatenate([blank, own], axis=1), jnp.concatenate([own, blank], axis=1))
        for k in range(SLOTS):
            for q in range(8):
                win[k, pl.ds(i * 8 + q, 1), :] = block[k : k + 1, q * 128 : (q + 1) * 128]
            win[k, pl.ds(29 + i, 1), :] = wide[k : k + 1]
    pl.semaphore_wait(barrier, 34)

    def send(src, dst, ssem, rsem, dev):
        cp = pltpu.make_async_remote_copy(
            src_ref=src, dst_ref=dst, send_sem=ssem, recv_sem=rsem, device_id=dev, device_id_type=MESH
        )
        cp.start()
        return cp

    halo = [
        send(xin.at[pl.ds(SPAN - 16, 16)], xbuf.at[pl.ds(0, 16)], halo_send.at[0], halo_recv.at[0], (me, (my + 1) % 4)),
        send(xst.at[pl.ds(SPAN - 16, 16)], xsbuf.at[pl.ds(0, 16)], halo_send.at[1], halo_recv.at[1], (me, (my + 1) % 4)),
    ]
    firsts = []
    for r in range(1, 4):
        dev = (me, (my + r) % 4)
        firsts.append(send(xin.at[pl.ds(0, 16)], ffin.at[my], f_send.at[r], f_recv.at[r], dev))
        firsts.append(send(xst.at[pl.ds(0, 16)], ffst.at[my], f_send.at[4 + r], f_recv.at[4 + r], dev))
        firsts.append(send(step.at[:, pl.ds(0, 128)], ffdt.at[my], f_send.at[8 + r], f_recv.at[8 + r], dev))

    for cp in loads:
        cp.wait()

    def fill(ref, lead, q, dest, half):
        slot = meta[0, dest]
        keep = meta[1, dest].astype(F32)
        ref[lead, q, pl.ds(0, 512), :] = (stage[slot, pl.ds(512 * half, 512), :] * keep).astype(BF16)
        ref[lead, q, pl.ds(512, 16), :] = (win[slot, pl.ds(16 * half, 16), :] * keep).astype(BF16)

    def fill_a(ref, lead, xd):
        def one(q, carry):
            fill(ref, lead, q, xd * 8 + q, 0)
            return carry

        lax.fori_loop(0, 8, one, 0)

    def fill_b(ref, lead, zd):
        def one(q, carry):
            fill(ref, lead, q, (q // 2) * 8 + zd * 2 + q % 2, 1)
            return carry

        lax.fori_loop(0, 8, one, 0)

    phase_a, phase_b, rtags = {}, {}, []
    for d in (1, 3, 2):
        xd, zd = (mx + d) % 4, (mz + d) % 4
        dev_a, dev_b = (at(d, 0, 0), my), (at(0, d, 0), my)
        fill_a(sbuf_a, xd, xd)
        phase_a[d] = send(sbuf_a.at[xd], rel_a.at[mx], one_send.at[d], one_recv.at[d], dev_a)
        fill_b(sbuf_b, zd, zd)
        phase_b[d] = send(sbuf_b.at[zd], rel_b.at[mz], one_send.at[4 + d], one_recv.at[4 + d], dev_b)
        rtags.append(send(tags.at[pl.ds(xd * 8, 8)], rtag_a.at[mx], rt_send.at[d], rt_recv.at[d], dev_a))
        rtags.append(send(tags_b.at[zd], rtag_b.at[mz], rt_send.at[4 + d], rt_recv.at[4 + d], dev_b))
    fill_a(rel_a, mx, mx)
    fill_b(rel_b, mz, mz)

    second = {}

    def row_a(p):
        return (near_a if p < 2 else far_a).at[(p % 2) * 8 + mz * 2 + mc]

    def row_b(p):
        return (near_b if p < 2 else far_b).at[(p % 2) * 8 + mx * 2 + mc]

    def forward(p, e, src_a, src_b):
        de, dc = e // 2, e % 2
        sem = p * 8 + e
        second[p, e, 0] = send(
            src_a, row_a(p), two_send.at[sem], two_recv.at[sem], (at(0, de, dc), my))
        second[p, e, 1] = send(
            src_b, row_b(p), two_send.at[32 + sem], two_recv.at[32 + sem], (at(de, 0, dc), my))

    def targets(e):
        de, dc = e // 2, e % 2
        ct = (mc + dc) % 2
        return ((mz + de) % 4) * 2 + ct, ((mx + de) % 4) * 2 + ct

    for e in (2, 6, 3, 7, 1, 4, 5):
        ta, tb = targets(e)
        forward(0, e, rel_a.at[mx, ta], rel_b.at[mz, tb])
    row_a(0)[...] = rel_a[mx, mz * 2 + mc]
    row_b(0)[...] = rel_b[mz, mx * 2 + mc]

    tag_copies = []
    for r in range(1, 32):
        peer = at(r // 8, (r // 2) % 4, r % 2)
        tag_copies.append(
            send(tags.at[peer], tagbuf.at[me], tag_send.at[r], tag_recv.at[r], (peer, my))
        )
    tagbuf[me] = tags[me]

    for cp in ins:
        cp.wait()
    for cp in halo:
        cp.wait()

    @pl.when(my == 0)
    def _():
        xbuf[pl.ds(0, 16), :] = jnp.zeros((16, INNER), BF16)
        xsbuf[pl.ds(0, 16), :] = jnp.zeros((16, 256), BF16)

    st_buf[...] = jnp.zeros_like(st_buf)
    base_buf[...] = jnp.zeros_like(base_buf)
    length = lens[0]

    def chunk_body(k, carry):
        r0 = pl.multiple_of(k * CHUNK, CHUNK)
        pos = my * SPAN + r0 + lax.broadcasted_iota(I32, (CHUNK, HEADS), 0)
        live = ((pos < length) & (pos >= 3)).astype(F32)
        dt = softplus(jnp.transpose(step[:, pl.ds(r0, CHUNK)].astype(F32)) + step_b[0:1, :]) * live
        rate = dt * (-LOG2E * jnp.exp(decay[0:1, :]))
        rows = lax.broadcasted_iota(I32, (CHUNK, CHUNK), 0)
        cols = lax.broadcasted_iota(I32, (CHUNK, CHUNK), 1)
        tri = jnp.where(rows >= cols, 1.0, 0.0).astype(BF16)
        hi, mid, lo = split3(rate)
        cum = nn(tri, hi) + nn(tri, mid) + nn(tri, lo)
        cum3[...] = jnp.concatenate(split3(cum), axis=1)
        cumt[...] = jnp.transpose(cum)
        dth = dt.astype(BF16)
        dt2[...] = jnp.concatenate([dth, (dt - dth.astype(F32)).astype(BF16)], axis=1)
        cum_buf[pl.ds(r0, CHUNK), :] = cum + base_buf[0:1, 0:HEADS]
        base_buf[0:1, 0:HEADS] = base_buf[0:1, 0:HEADS] + cum[CHUNK - 1 : CHUNK, :]
        xs_tile = xsbuf[pl.ds(r0, CHUNK + 16), :].astype(F32)
        mixed = conv_tile(xs_tile, conv_w[:, INNER : INNER + 256], jnp.concatenate([conv_b[32:33, :], conv_b[33:34, :]], axis=1), CHUNK)
        write, read = mixed[:, 0:128], mixed[:, 128:256]
        read_buf[pl.ds(r0, CHUNK), :] = read
        sc_buf[...] = jnp.where(rows >= cols, nt(read, write), 0.0)
        wt_buf[...] = jnp.transpose(write.astype(F32)).astype(BF16)

        def group_body(j, inner):
            lanes = [pl.ds(pl.multiple_of(j * (GROUP * 128) + g * 128, 128), 128) for g in range(GROUP)]
            pairs = [j * GROUP + g for g in range(GROUP)]
            every = range(GROUP)
            low = lax.broadcasted_iota(I32, (CHUNK, 128), 1) < 64
            lane = lax.broadcasted_iota(I32, (1, 128), 1)
            x = [xbuf[pl.ds(r0, CHUNK + 16), lanes[g]].astype(F32) for g in every]
            state = [st_buf[:, lanes[g]] for g in every]
            both = [nn(cum3[...], pick_heads(3, pairs[g])) for g in every]
            dte = [nn(dt2[...], pick_lanes(2, pairs[g])) for g in every]
            carried = [nn(read_buf[pl.ds(r0, CHUNK), :], state[g].astype(BF16)) for g in every]
            value = [conv_tile(x[g], conv_w[:, lanes[g]], conv_b[pl.ds(pairs[g], 1), :], CHUNK).astype(F32) for g in every]
            ys, states = [], []
            for g in every:
                sc = sc_buf[...]
                c1, c2 = both[g][:, 0:128], both[g][:, 128:256]
                w1 = sc * jnp.exp2(jnp.minimum(c1 - cumt[pl.ds(2 * pairs[g], 1), :], 0.0))
                w2 = sc * jnp.exp2(jnp.minimum(c2 - cumt[pl.ds(2 * pairs[g] + 1, 1), :], 0.0))
                cp = jnp.where(low, c1, c2)
                vd = value[g] * dte[g]
                zero = jnp.zeros_like(vd)
                rhs = jnp.concatenate([jnp.where(low, vd, zero), jnp.where(low, zero, vd)], axis=0).astype(BF16)
                lhs = jnp.concatenate([w1.astype(BF16), w2.astype(BF16)], axis=1)
                last = cp[CHUNK - 1 : CHUNK, :]
                scaled = (jnp.exp2(last - cp) * vd).astype(BF16)
                skip_lane = jnp.where(lane < 64, skip[2 * pairs[g]], skip[2 * pairs[g] + 1])
                ys.append(nn(lhs, rhs) + carried[g] * jnp.exp2(cp) + skip_lane * value[g])
                states.append(jnp.exp2(last) * state[g] + nn(wt_buf[...], scaled))
            for g in every:
                y_buf[pl.ds(r0, CHUNK), lanes[g]] = ys[g].astype(BF16)
                st_buf[:, lanes[g]] = states[g]
            return inner

        lax.fori_loop(0, PAIRS // GROUP, group_body, 0)
        return carry

    lax.fori_loop(0, CHUNKS, chunk_body, 0)

    cols = lax.broadcasted_iota(I32, (16, SPAN), 1)
    rows = lax.broadcasted_iota(I32, (16, SPAN), 0)
    want = length - 3 - my * SPAN
    sel_in = jnp.where((cols == want + rows) & (rows < 3), 1.0, 0.0).astype(BF16)
    sel_st = jnp.where((cols == want + rows - 3) & (rows >= 3) & (rows < 6), 1.0, 0.0).astype(BF16)
    small3[0:16, :] = jnp.zeros((16, 192), BF16)
    lst = nn(sel_st, xsbuf[pl.ds(16, SPAN), :])

    def lend_body(i, carry):
        lanes = pl.ds(pl.multiple_of(i * 256, 256), 256)
        to = pl.ds(pl.multiple_of((i % 4) * 256, 256), 256)
        lsend[i // 4, pl.ds(0, 128), to] = st_buf[:, lanes].astype(BF16)
        first = jnp.where(i % 4 == 0, 1.0, 0.0)
        lsend[i // 4, pl.ds(128, 16), to] = (nn(sel_in, xbuf[pl.ds(16, SPAN), lanes]) + first * lst).astype(BF16)
        return carry

    lax.fori_loop(0, INNER // 256, lend_body, 0)
    tbuf[my] = base_buf[...]
    lrecv[my] = lsend[my]
    lends = []
    for r in range(1, 4):
        dev = (me, (my + r) % 4)
        lends.append(send(lsend.at[(my + r) % 4], lrecv.at[my], lend_send.at[r], lend_recv.at[r], dev))
        lends.append(send(tbuf.at[my], tbuf.at[my], lend_send.at[4 + r], lend_recv.at[4 + r], dev))

    @pl.when(my == 0)
    def _():
        rowc = lax.broadcasted_iota(I32, (16, HEADS), 0)
        cum_buf[pl.ds(0, 16), :] = jnp.where(rowc < 3, -1.0e6, cum_buf[pl.ds(0, 16), :])

    gate_load.wait()

    def ready_body(k, carry):
        r0 = pl.multiple_of(k * CHUNK, CHUNK)
        cum3[...] = jnp.concatenate(split3(cum_buf[pl.ds(r0, CHUNK), :]), axis=1)
        rowpos = my * SPAN + r0 + lax.broadcasted_iota(I32, (CHUNK, 128), 0)

        def group_body(j, inner):
            lanes = [pl.ds(pl.multiple_of(j * 256 + g * 128, 128), 128) for g in range(2)]
            valid = (rowpos < length).astype(F32)
            ce = [nn(cum3[...], pick_lanes(3, 2 * j + g)) for g in range(2)]
            gates = [silu(gbuf[pl.ds(r0, CHUNK), lanes[g]].astype(F32)) * valid for g in range(2)]
            for g in range(2):
                xbuf[pl.ds(r0, CHUNK), lanes[g]] = jnp.exp2(ce[g]).astype(BF16)
                gbuf[pl.ds(r0, CHUNK), lanes[g]] = gates[g].astype(BF16)
            return inner

        lax.fori_loop(0, PAIRS // 2, group_body, 0)
        return carry

    lax.fori_loop(0, CHUNKS, ready_body, 0)
    tot_buf[...] = jnp.zeros_like(tot_buf)

    for cp in rtags:
        cp.wait()
    tag_loads = [
        pltpu.make_async_copy(rtag_a, rtag_as, in_sem.at[3]),
        pltpu.make_async_copy(rtag_b, rtag_bs, in_sem.at[4]),
    ]
    for cp in tag_loads:
        cp.start()
    for d in (1, 3, 2):
        phase_a[d].wait()
        phase_b[d].wait()
    for cp in tag_loads:
        cp.wait()

    def swapped(first, p):
        if p == 1:
            return jnp.where(first >= 2, first, 1)
        return jnp.where(first == p, 1, p)

    for p in (1, 2, 3):
        for e in (2, 6, 3, 7, 0, 1, 4, 5):
            ta, tb = targets(e)
            first_a, first_b = jnp.int32(0), jnp.int32(0)
            for q in (1, 2, 3):
                first_a = jnp.where(rtag_as[(mx + 4 - q) % 4, ta, 0, 0] == 1, q, first_a)
                first_b = jnp.where(rtag_bs[(mz + 4 - q) % 4, tb, 0, 0] == 1, q, first_b)
            block_a = rel_a[(mx + 4 - swapped(first_a, p)) % 4, ta]
            block_b = rel_b[(mz + 4 - swapped(first_b, p)) % 4, tb]
            if e == 0:
                row_a(p)[...] = block_a
                row_b(p)[...] = block_b
            else:
                sbuf_a[p, e] = block_a
                sbuf_b[p, e] = block_b
                forward(p, e, sbuf_a.at[p, e], sbuf_b.at[p, e])

    for cp in tag_copies:
        cp.wait()
    tag_load = pltpu.make_async_copy(tagbuf, tag_s, in_sem.at[5])
    tag_load.start()
    tag_load.wait()

    def source_of(j):
        acc = jnp.int32(0)
        for s in range(32):
            acc = jnp.where(tag_s[s, 0, 0] == j + 1, s, acc)
        return acc

    def split_source(src):
        xs, zs, cs = src // 8, (src // 2) % 4, src % 2
        return (mx + 4 - xs) % 4, zs * 2 + cs, (mz + 4 - zs) % 4, xs * 2 + cs

    hops0_a, relay0_a, hops0_b, relay0_b = split_source(source_of(0))
    loc0_a = jnp.where(hops0_a > 0, 8, 0) + relay0_a
    loc0_b = jnp.where(hops0_b > 0, 8, 0) + relay0_b

    def rank(hops, relay, hops0, relay0):
        moved_up = jnp.where(hops == hops0, 1, jnp.where(hops == 1, hops0, hops))
        place_in = jnp.where((relay == relay0) & (hops0 >= 2) & (hops > 0), moved_up, hops)
        return place_in * 8 + relay

    def places(j):
        hops_a, relay_a, hops_b, relay_b = split_source(source_of(j))
        return rank(hops_a, relay_a, hops0_a, relay0_a), rank(hops_b, relay_b, hops0_b, relay0_b)

    def fetch(near, far, loc):
        return jnp.where(loc < 16, near[jnp.minimum(loc, 15)], far[jnp.maximum(loc - 16, 0)])

    for cp in firsts:
        cp.wait()
    own_first = [
        pltpu.make_async_copy(xin.at[pl.ds(0, 16)], ffin.at[my], in_sem.at[6]),
        pltpu.make_async_copy(xst.at[pl.ds(0, 16)], ffst.at[my], in_sem.at[7]),
    ]
    for cp in own_first:
        cp.start()
    ffdt[my] = step[:, 0:128]
    for cp in own_first:
        cp.wait()
    for cp in lends:
        cp.wait()

    for p in (0, 1):
        for e in range(1, 8):
            second[p, e, 0].wait()
            second[p, e, 1].wait()

    wtile[my] = near_b[loc0_b, pl.ds(512, 16), :]
    wins = []
    for r in range(1, 4):
        wins.append(send(wtile.at[my], wtile.at[my], win_send.at[r], win_recv.at[r], (me, (my + r) % 4)))

    posf = lax.broadcasted_iota(I32, (16, HEADS), 0)
    livef = ((posf < length) & (posf < 3)).astype(F32)
    dtf0 = softplus(jnp.transpose(ffdt[0].astype(F32))[0:16] + step_b[0:1, :]) * livef
    rate0 = dtf0 * (-LOG2E * jnp.exp(decay[0:1, :]))
    c0 = rate0[0:1]
    c1 = c0 + rate0[1:2]
    c2 = c1 + rate0[2:3]
    cumf = jnp.where(posf == 0, c0, jnp.where(posf == 1, c1, c2))
    totals = jnp.where(posf == 0, tbuf[0][0:1, 0:HEADS], jnp.where(
        posf == 1, tbuf[1][0:1, 0:HEADS], jnp.where(posf == 2, tbuf[2][0:1, 0:HEADS], tbuf[3][0:1, 0:HEADS])))
    small3[0:16, :] = jnp.concatenate(split3(cumf), axis=1)
    small3[16:32, :] = jnp.concatenate(split3(dtf0), axis=1)
    small3[32:48, :] = jnp.concatenate(split3(totals), axis=1)

    for cp in wins:
        cp.wait()
    w_low = wtile[0].astype(F32) + wtile[1].astype(F32)
    w_high = wtile[2].astype(F32) + wtile[3].astype(F32)
    e_st = jnp.concatenate([jnp.concatenate([w_low, w_high], axis=1), ffst[0].astype(F32)], axis=0)
    mixed0 = conv_tile(e_st, conv_w[:, INNER : INNER + 256], jnp.concatenate([conv_b[32:33, :], conv_b[33:34, :]], axis=1), 16)
    write0, read0 = mixed0[:, 0:128], mixed0[:, 128:256]
    read0_buf[...] = read0
    sc0_buf[...] = nt(read0, write0)
    w0t[...] = jnp.transpose(
        jnp.concatenate([write0.astype(F32), jnp.zeros((112, 128), F32)], axis=0)).astype(BF16)

    row16 = lax.broadcasted_iota(I32, (16, 128), 0)
    lane1 = lax.broadcasted_iota(I32, (1, 128), 1)
    for q in range(8):
        i = my * 8 + q
        lanes = pl.ds(pl.multiple_of(my * 1024 + q * 128, 128), 128)
        own = pl.ds(q * 128, 128)
        if q < 4:
            s0 = near_a[loc0_a, pl.ds(q * 128, 128), :]
        else:
            s0 = near_b[loc0_b, pl.ds((q - 4) * 128, 128), :]
        s0t = jnp.transpose(s0.astype(F32))
        wa = near_a[loc0_a, pl.ds(512, 16), :].astype(F32)
        wb = near_b[loc0_b, pl.ds(512, 16), :].astype(F32)
        wq = jnp.where(row16 == 13, wa[q : q + 1], jnp.where(row16 == 14, wa[8 + q : 9 + q], wb[q : q + 1]))
        x0 = jnp.concatenate([wq, ffin[0, :, lanes].astype(F32)], axis=0)
        small = nn(small3[...], pick_lanes(3, i))
        cf, dtf, totl = small[0:16], small[16:32], small[32:48]
        v0 = conv_tile(x0, conv_w[:, lanes], conv_b[pl.ds(i, 1), :], 16).astype(F32)
        vd = v0 * dtf
        scaled = jnp.concatenate([jnp.exp2(cf[2:3] - cf) * vd, jnp.zeros((112, 128), F32)], axis=0).astype(BF16)
        carry = jnp.exp2(cf[2:3]) * s0t + nn(w0t[...], scaled)
        y0 = nt(read0_buf[...], s0) * jnp.exp2(cf)
        y0 = y0 + jnp.where(lane1 < 64, skip[2 * i], skip[2 * i + 1]) * v0
        for s in range(3):
            term = sc0_buf[:, s : s + 1] * jnp.exp2(jnp.minimum(cf - cf[s : s + 1], 0.0)) * vd[s : s + 1]
            y0 = y0 + jnp.where(row16 >= s, term, 0.0)
        kept = jnp.zeros((16, 128), F32)
        for c in range(4):
            ssend[c, pl.ds(0, 128), own] = carry.astype(BF16)
            ssend[c, pl.ds(128, 16), own] = y0.astype(BF16)
            carry = jnp.exp2(totl[c : c + 1]) * carry + lrecv[c, pl.ds(0, 128), own].astype(F32)
            kept = kept + lrecv[c, pl.ds(128, 16), own].astype(F32)
        fin_buf[pl.ds(q * 128, 128), :] = jnp.transpose(carry)
        for r in range(3):
            wstage[0, pl.ds(r * 8 + q, 1), :] = kept[r : r + 1]
        if q < 2:
            wstage[1 + q, pl.ds(0, 16), :] = kept

    sins = []
    for r in range(1, 4):
        other = (my + r) % 4
        sins.append(send(ssend.at[other], srecv.at[my], s0_send.at[r], s0_recv.at[r], (me, other)))
    srecv[my] = ssend[my]

    outs = []

    def put_out(src, dst, i):
        cp = pltpu.make_async_copy(src, dst, out_sem.at[i])
        cp.start()
        outs.append(cp)

    put_out(fin_buf, fin_out, 30)
    def quarter(owner):
        base = owner * 1024

        @pl.when(my == 0)
        def _():
            for j in range(4):
                lanes = pl.ds(pl.multiple_of(base + j * 256, 128), 256)
                new = srecv[owner, pl.ds(128, 16), pl.ds(j * 256, 256)].astype(F32)
                old = y_buf[pl.ds(0, 16), lanes].astype(F32)
                rowy = lax.broadcasted_iota(I32, (16, 256), 0)
                y_buf[pl.ds(0, 16), lanes] = jnp.where(rowy < 3, new, old).astype(BF16)

        def group_body(j, carry):
            lanes = pl.ds(pl.multiple_of(base + j * 256, 128), 256)
            state = srecv[owner, pl.ds(0, 128), pl.ds(pl.multiple_of(j * 256, 256), 256)]
            spans = [pl.ds(r * CHUNK, CHUNK) for r in range(CHUNKS)]
            parts = [nn(read_buf[span, :], state) for span in spans]
            new, squares = [], []
            for span, part in zip(spans, parts):
                y = y_buf[span, lanes].astype(F32) + xbuf[span, lanes].astype(F32) * part
                v = y.astype(BF16).astype(F32) * gbuf[span, lanes].astype(F32)
                new.append(v.astype(BF16))
                squares.append(tot_buf[span, :] + v[:, 0:128] * v[:, 0:128] + v[:, 128:256] * v[:, 128:256])
            for span, v, square in zip(spans, new, squares):
                y_buf[span, lanes] = v
                tot_buf[span, :] = square
            return carry

        lax.fori_loop(0, 4, group_body, 0)

    quarter(my)
    for r in (1, 3, 2):
        sins[r - 1].wait()
        quarter((my + 4 - r) % 4)
    put_out(y_buf, mix, 31)
    tot_buf[...] = jnp.broadcast_to(
        lax.rsqrt(jnp.sum(tot_buf[...], axis=1, keepdims=True) * (1.0 / INNER) + EPSILON), (SPAN, 128))
    put_out(tot_buf, scale_out, 29)

    spots = [places(j) for j in range(SLOTS)]
    for p in (2, 3):
        for e in range(1, 8):
            second[p, e, 0].wait()
            second[p, e, 1].wait()
    for j in range(1, SLOTS):
        loc_a, loc_b = spots[j]
        sbuf_a[j // 8, j % 8] = fetch(near_a, far_a, loc_a)
        sbuf_b[j // 8, j % 8] = fetch(near_b, far_b, loc_b)
        put_out(sbuf_a.at[j // 8, j % 8, pl.ds(0, 512)], moved.at[j, pl.ds(0, 512)], 2 * j)
        put_out(sbuf_b.at[j // 8, j % 8, pl.ds(0, 512)], moved.at[j, pl.ds(512, 512)], 2 * j + 1)
        wstage[2 + j, pl.ds(0, 16), :] = sbuf_a[j // 8, j % 8, pl.ds(512, 16), :].astype(F32)
        wstage[2 + j, pl.ds(16, 16), :] = sbuf_b[j // 8, j % 8, pl.ds(512, 16), :].astype(F32)
    put_out(wstage, wout, 0)
    for cp in outs:
        cp.wait()


def exchange(*operands):
    dma = pltpu.SemaphoreType.DMA
    shape = jax.ShapeDtypeStruct
    out_shape = (
        shape((SLOTS, 1024, 128), BF16),
        shape((SLOTS + 2, 32, 128), F32),
        shape((1024, 128), F32),
        shape((SPAN, INNER), BF16),
        shape((SPAN, 128), F32),
    )
    scratch = [
        pltpu.SMEM((2, 32), I32),
        pltpu.VMEM((32, 1, 128), I32),
        pltpu.VMEM((4, 8, 1, 128), I32),
        pltpu.VMEM((SLOTS, 32, 128), F32),
        pltpu.VMEM((SPAN, 128), F32),
        pltpu.VMEM((SLOTS, 1024, 128), F32),
        pltpu.VMEM((4, 8, HALF, 128), BF16),
        pltpu.VMEM((4, 8, HALF, 128), BF16),
        pltpu.VMEM((4, 8, HALF, 128), BF16),
        pltpu.VMEM((4, 8, HALF, 128), BF16),
        pltpu.VMEM((16, HALF, 128), BF16),
        pltpu.VMEM((16, HALF, 128), BF16),
        pltpu.VMEM((16, HALF, 128), BF16),
        pltpu.VMEM((16, HALF, 128), BF16),
        pltpu.VMEM((SPAN + 16, INNER), BF16),
        pltpu.VMEM((SPAN + 16, 256), BF16),
        pltpu.VMEM((SPAN, INNER), BF16),
        pltpu.VMEM((SPAN, INNER), BF16),
        pltpu.VMEM((SPAN, 128), BF16),
        pltpu.VMEM((SPAN, HEADS), F32),
        pltpu.VMEM((128, INNER), F32),
        pltpu.VMEM((4, 144, 1024), BF16),
        pltpu.VMEM((4, 144, 1024), BF16),
        pltpu.VMEM((4, 144, 1024), BF16),
        pltpu.VMEM((4, 144, 1024), BF16),
        pltpu.VMEM((4, 8, 128), F32),
        pltpu.VMEM((32, 1, 128), I32),
        pltpu.VMEM((4, 8, 1, 128), I32),
        pltpu.VMEM((4, 8, 1, 128), I32),
        pltpu.SMEM((32, 1, 128), I32),
        pltpu.SMEM((4, 8, 1, 128), I32),
        pltpu.SMEM((4, 8, 1, 128), I32),
        pltpu.VMEM((CHUNK, 192), BF16),
        pltpu.VMEM((HEADS, CHUNK), F32),
        pltpu.VMEM((CHUNK, 128), BF16),
        pltpu.VMEM((CHUNK, CHUNK), F32),
        pltpu.VMEM((CHUNK, CHUNK), BF16),
        pltpu.VMEM((8, 128), F32),
        pltpu.VMEM((4, 16, 128), BF16),
        pltpu.VMEM((1024, 128), F32),
        pltpu.VMEM((SLOTS + 2, 32, 128), F32),
        pltpu.VMEM((4, 16, INNER), BF16),
        pltpu.VMEM((4, 16, 256), BF16),
        pltpu.VMEM((4, HEADS, 128), BF16),
        pltpu.VMEM((48, 192), BF16),
        pltpu.VMEM((128, 128), BF16),
        pltpu.VMEM((16, 128), BF16),
        pltpu.VMEM((16, 16), F32),
        dma((SLOTS,)), dma((8,)), dma((32,)),
        dma((8,)), dma((8,)), dma((64,)), dma((64,)), dma((32,)), dma((32,)), dma((8,)), dma((8,)),
        dma((2,)), dma((2,)), dma((8,)), dma((8,)), dma((4,)), dma((4,)), dma((4,)), dma((4,)), dma((12,)), dma((12,)),
    ]
    return pl.pallas_call(
        exchange_kernel,
        out_shape=out_shape,
        in_specs=[SM, SM, SM, SM, ANY, VM, VM, ANY, ANY, ANY, VM, VM, VM, VM, VM],
        out_specs=[ANY] * len(out_shape),
        scratch_shapes=scratch,
        compiler_params=pltpu.CompilerParams(
            collective_id=1, has_side_effects=True, vmem_limit_bytes=67043328
        ),
        name="exchange",
    )(*operands)


STEPS = 4
PLACE_ROWS = SLOTS * 1024 // STEPS
MIX_ROWS = SPAN // STEPS


def place_kernel(moved, fin, gated, scale, norm_w, wout, states, mixed, win_in, win_st, acc_in, acc_st):
    my = lax.axis_index("seq")
    step = pl.program_id(0)
    states[...] = moved[...].astype(F32)

    @pl.when(step == 0)
    def _():
        states[pl.ds(0, 1024), :] = fin[...]

    @pl.when(step < 3)
    def _():
        for j in range(SLOTS):
            src = 0 if j == 0 else 2 + j
            for q in range(8):
                acc_in[pl.ds(j, 1), pl.ds(q * 128, 128)] = wout[src, pl.ds(step * 8 + q, 1), :]
            if j == 0:
                row = pl.ds(3 + step, 1)
                acc_st[pl.ds(0, 1), :] = jnp.where(my >= 2, wout[2, row, :], wout[1, row, :])
            else:
                acc_st[pl.ds(j, 1), :] = wout[src, pl.ds(29 + step, 1), :]
        win_in[step] = acc_in[...].astype(BF16)
        rows = acc_st[...]
        win_st[step] = jnp.where(my % 2 == 1, rows[:, 64:128], rows[:, 0:64]).astype(BF16)

    def norm_body(i, carry):
        span = pl.ds(pl.multiple_of(i * 16, 16), 16)
        wide = jnp.concatenate([scale[span, :]] * PAIRS, axis=1)
        mixed[span, :] = (gated[span, :].astype(F32) * wide * norm_w[0:1, :]).astype(BF16)
        return carry

    lax.fori_loop(0, MIX_ROWS // 16, norm_body, 0)


def place(moved, fin, gated, scale, norm_w, wout):
    rows = lambda count, lanes: pl.BlockSpec((count, lanes), lambda j: (j, 0))
    whole = lambda lanes: pl.BlockSpec((3, SLOTS, lanes), lambda j: (0, 0, 0))
    return pl.pallas_call(
        place_kernel,
        grid=(STEPS,),
        out_shape=(
            jax.ShapeDtypeStruct((SLOTS * 1024, 128), F32),
            jax.ShapeDtypeStruct((SPAN, INNER), BF16),
            jax.ShapeDtypeStruct((3, SLOTS, 1024), BF16),
            jax.ShapeDtypeStruct((3, SLOTS, 64), BF16),
        ),
        in_specs=[rows(PLACE_ROWS, 128), VM, rows(MIX_ROWS, INNER), rows(MIX_ROWS, 128), VM, VM],
        out_specs=[rows(PLACE_ROWS, 128), rows(MIX_ROWS, INNER), whole(1024), whole(64)],
        scratch_shapes=[pltpu.VMEM((SLOTS, 1024), F32), pltpu.VMEM((SLOTS, 128), F32)],
        name="place",
    )(moved, fin, gated, scale, norm_w, wout)


def on_device(
    pool_states, inner_window, state_window, move_plan, active_mask, inputs_inner, inputs_state, gate_rows,
    step_raw, lengths, conv_weight, conv_bias, step_bias, decay_log, skip_weight, norm_weight,
):
    moved, wout, fin, gated, scale = exchange(
        move_plan.T, active_mask, lengths, skip_weight, pool_states.reshape(SLOTS, 1024, 128),
        jnp.transpose(inner_window, (1, 0, 2)), jnp.transpose(state_window, (1, 0, 2)),
        inputs_inner[0], inputs_state[0], gate_rows[0], step_raw[0].T,
        conv_weight, conv_bias.reshape(34, 128), step_bias[None], decay_log[None],
    )
    new_states, mix, new_in, new_st = place(
        moved.reshape(SLOTS * 1024, 128), fin, gated, scale, norm_weight[None], wout)
    return (
        new_states.reshape(SLOTS, 16, 64, 128), jnp.transpose(new_in, (1, 0, 2)), jnp.transpose(new_st, (1, 0, 2)),
        mix[None],
    )


def solution(mesh):
    return jax.shard_map(
        on_device,
        mesh=mesh,
        in_specs=(
            P("req", "seq", None, None), P("req", None, "seq"), P("req", None, "seq"), P("req", None), P("req"),
            P("req", "seq", None), P("req", "seq", None), P("req", "seq", None), P("req", "seq", None), P("req"),
            P(), P(), P(), P(), P(), P(),
        ),
        out_specs=(
            P("req", "seq", None, None), P("req", None, "seq"), P("req", None, "seq"), P("req", "seq", None),
        ),
        check_vma=False,
    )
```
